32 devices in a mesh: gx: 4 (over z), gy: 8 (over y, x, core).
Axes of the slice: x: 2, y: 2, z: 4, core: 2. Of those that a mesh axis runs over, the one named last changes fastest.
Arguments:
- atm_members: float32 [4, 8, 80, 12, 128], P('gx', 'gy'), may hold values from -6 to 6
- ocean_members: bfloat16 [4, 8, 80, 1024], P('gx', 'gy'), may hold values from -6 to 6
- remap_weights: bfloat16 [4, 8, 4, 1024, 128], P('gx', 'gy'), may hold values from -0.09375 to 0.09375
- pair_src: int32 [4, 8, 4], P('gx', 'gy'), may hold values from 0 to 31, as said below
- obs_cell: int32 [4, 8, 64], P('gx', 'gy'), may hold values from 0 to 127
- obs_value: float32 [4, 8, 64], P('gx', 'gy'), may hold values from -8 to 8
- obs_error: float32 [4, 8, 64], P('gx', 'gy'), may hold values from 2 to 16
- obs_live: int32 [4, 8, 64], P('gx', 'gy'), may hold values from 0 to 1, as said below
- obs_order: int32 [4, 8, 64], P('gx', 'gy'), may hold values from 0 to 63, each once within a row
Outputs:
- post_mean: float32 [4, 8, 13, 128], P('gx', 'gy')
- post_anom: float32 [4, 8, 80, 13, 128], P('gx', 'gy')
The draws below stay inside these ranges and needn't reach their ends.
Inputs may be any that keep to these rules, and one draw needn't show every extreme that they name: `pair_src`: for atmosphere tile (i, j) the 4 numbers are distinct, each a * 8 + b with |a - i| <= 1 and |b - j| <= 1. `obs_live`: the live slots of a tile are its first ones, between 8 and 64 of them; some tile has all slots live. `obs_order`: each tile's last dimension is a permutation of its slots.
All inputs are finite; a program needn't handle non-finite values.
Results may differ from the reference program's by a relative error of at most 0.0003.
Values may be sent and summed in bfloat16 or wider, within the bound.
A program may use at most 64 MiB of HBM per device.

```python
import math
import jax
import jax.numpy as jnp
from jax import lax

MEM = 80
AX = 8
AY = 16
OCN_DEV = 1024
OB = 32
NB = 2
K = 4
FIELDS = 12
COMP = 13
CELLS = 128
RAD = 2
OBS_DEV = 64
TILES_X = 4
TILES_Y = 8


def draw_pair_src(key, part):
    tile_x = jnp.arange(TILES_X, dtype=jnp.int32)[:, None, None]
    tile_y = jnp.arange(TILES_Y, dtype=jnp.int32)[None, :, None]
    candidate = jnp.arange(9, dtype=jnp.int32)[None, None, :]
    source_x = tile_x + candidate // 3 - 1
    source_y = tile_y + candidate % 3 - 1
    scores = jax.random.randint(jax.random.fold_in(key, 11), (TILES_X, TILES_Y, 9), 0, 1 << 20)
    scores = scores * 9 + candidate
    outside = (source_x < 0) | (source_x >= TILES_X) | (source_y < 0) | (source_y >= TILES_Y)
    scores = jnp.where(outside, scores + (1 << 29), scores)
    ranking = jnp.argsort(scores, axis=-1)[..., :K]
    linear = source_x * TILES_Y + source_y
    return jnp.take_along_axis(linear, ranking, axis=-1).astype(jnp.int32)


def draw_obs_live(key, part):
    threshold = jax.random.randint(jax.random.fold_in(key, 21), (TILES_X, TILES_Y), OBS_DEV // 8, OBS_DEV + 1)
    chosen_tile = jax.random.randint(jax.random.fold_in(key, 22), (), 0, TILES_X * TILES_Y)
    tile_number = jnp.arange(TILES_X * TILES_Y, dtype=jnp.int32).reshape(TILES_X, TILES_Y)
    threshold = jnp.where(tile_number == chosen_tile, OBS_DEV, threshold)
    slot_number = jnp.arange(OBS_DEV, dtype=jnp.int32)
    return (slot_number[None, None, :] < threshold[:, :, None]).astype(jnp.int32)


def plant(values, rng, smallest, top_value):
    longest = values.shape.index(max(values.shape))
    spots = []
    for shift in (0, 1):
        where = [jax.random.randint(jax.random.fold_in(rng, axis), (), 0, length) for axis, length in enumerate(values.shape)]
        where[longest] = (where[longest] + shift) % values.shape[longest]
        spots.append(tuple(where))
    return values.at[spots[0]].set(smallest).at[spots[1]].set(top_value)


def levels(key, shape, pieces, smallest, high):
    level, own = 1.0, jax.random.fold_in(key, 6)
    for axis_at, shards_of in pieces:
        heights = jnp.exp(jax.random.uniform(jax.random.fold_in(own, axis_at), (shards_of,), jnp.float32, smallest / len(pieces), high / len(pieces)))
        level = level * jnp.repeat(heights, shape[axis_at] // shards_of).reshape([-1 if axis == axis_at else 1 for axis in range(len(shape))])
    return level


def centred(rng, shape, spread, limit, pieces=(), held_as=jnp.bfloat16):
    values = spread * jax.random.normal(rng, shape, jnp.float32)
    if pieces:
        values = values * levels(rng, shape, pieces, -0.22, 0.18)
    return jnp.clip(values, -limit, limit).astype(held_as)


def setup_inputs(seed: int = 0) -> dict:
    splits = jax.random.split(jax.random.key(seed), 10)
    atm_members = centred(splits[0], (TILES_X, TILES_Y, MEM, FIELDS, CELLS), 1.0, 6.0, ((0, 4), (1, 8)), jnp.float32)
    ocean_members = centred(splits[1], (TILES_X, TILES_Y, MEM, OCN_DEV), 1.0, 6.0, ((0, 4), (1, 8)))
    remap_weights = centred(splits[2], (TILES_X, TILES_Y, K, OCN_DEV, CELLS), (K * OCN_DEV) ** -0.5, 0.09375, ((0, 4), (1, 8)))
    pair_src = draw_pair_src(jax.random.fold_in(splits[9], 71), 0)
    obs_cell = plant(jax.random.randint(splits[4], (TILES_X, TILES_Y, OBS_DEV), 0, CELLS), jax.random.fold_in(splits[4], 1), 0, CELLS - 1).astype(jnp.int32)
    obs_value = centred(splits[5], (TILES_X, TILES_Y, OBS_DEV), 1.5, 8.0, ((0, 4), (1, 8)), jnp.float32)
    obs_error = jnp.clip(jnp.exp(math.log(16.0) - 2.0794415 * jax.random.uniform(splits[6], (TILES_X, TILES_Y, OBS_DEV), jnp.float32) ** levels(splits[6], (TILES_X, TILES_Y, OBS_DEV), ((0, 4), (1, 8)), -0.2, 0.2)), 2.0, 16.0)
    obs_live = draw_obs_live(jax.random.fold_in(splits[9], 71), 0)
    obs_order = jax.vmap(lambda own: jax.random.permutation(own, OBS_DEV))(jax.random.split(splits[8], TILES_X * TILES_Y)).reshape((TILES_X, TILES_Y, OBS_DEV)).astype(jnp.int32)
    return {"atm_members": atm_members, "ocean_members": ocean_members, "remap_weights": remap_weights, "pair_src": pair_src, "obs_cell": obs_cell, "obs_value": obs_value, "obs_error": obs_error, "obs_live": obs_live, "obs_order": obs_order}


exact_mode = lax.Precision.HIGHEST

def update_group(packets, anomaly, ens_mean, base_x, base_y):
    members = anomaly.shape[0]
    components = anomaly.shape[1]
    cell_count = anomaly.shape[2]
    observed = jnp.transpose(packets[:, :members, :], (1, 0, 2)).reshape(members, -1)
    innovation = packets[:, members, :].reshape(-1)
    errors = packets[:, members + 1, :].reshape(-1)
    obs_x = packets[:, members + 2, :].reshape(-1)
    obs_y = packets[:, members + 3, :].reshape(-1)
    live = packets[:, members + 4, :].reshape(-1)
    variance = lax.optimization_barrier(jnp.sum(observed * observed, axis=0)) / (members - 1)
    denominator = variance + errors + (1.0 - live)
    weighting = live / denominator
    damping = 1.0 / (1.0 + jnp.sqrt(errors / denominator))
    cell_index = jnp.arange(cell_count, dtype=jnp.int32)
    cell_x = (base_x + cell_index // AY).astype(jnp.float32)
    cell_y = (base_y + cell_index % AY).astype(jnp.float32)
    distance = (obs_x[:, None] - cell_x[None, :]) ** 2 + (obs_y[:, None] - cell_y[None, :]) ** 2
    taper = jnp.maximum(1.0 - distance / float(RAD * RAD), 0.0) ** 2
    flat_anomaly = anomaly.reshape(members, components * cell_count)
    covariance = jnp.dot(observed.T, flat_anomaly, precision=exact_mode, preferred_element_type=jnp.float32) / (members - 1)
    gain = covariance.reshape(-1, components, cell_count) * (taper * weighting[:, None])[:, None, :]
    gain = gain.reshape(-1, components * cell_count)
    mean_step = jnp.dot(innovation[None, :], gain, precision=exact_mode, preferred_element_type=jnp.float32)
    anomaly_step = jnp.dot(observed * damping[None, :], gain, precision=exact_mode, preferred_element_type=jnp.float32)
    return (mean_step.reshape(components, cell_count), anomaly_step.reshape(members, components, cell_count))

def reference(atm_members, ocean_members, remap_weights, pair_src, obs_cell, obs_value, obs_error, obs_live, obs_order):
    tiles = TILES_X * TILES_Y
    ocean_flat = ocean_members.reshape(tiles, MEM, OCN_DEV)

    def remap_one(inputs):
        weights, sources = inputs
        chosen = ocean_flat[sources]
        stacked = jnp.transpose(chosen, (1, 0, 2)).reshape(MEM, K * OCN_DEV)
        return jnp.dot(stacked, weights.reshape(K * OCN_DEV, CELLS), preferred_element_type=jnp.float32)
    surface = lax.map(remap_one, (remap_weights.reshape(tiles, K, OCN_DEV, CELLS), pair_src.reshape(tiles, K).astype(jnp.int32)))
    state = jnp.concatenate([atm_members.reshape(tiles, MEM, FIELDS, CELLS), surface[:, :, None, :]], axis=2)
    ens_mean = lax.optimization_barrier(jnp.sum(state, axis=1)) / MEM
    anomaly = state - ens_mean[:, None]
    ens_mean = ens_mean.reshape(TILES_X, TILES_Y, COMP, CELLS)
    anomaly = anomaly.reshape(TILES_X, TILES_Y, MEM, COMP, CELLS)
    tile_x = jnp.broadcast_to(jnp.arange(TILES_X, dtype=jnp.int32)[:, None], (TILES_X, TILES_Y))
    tile_y = jnp.broadcast_to(jnp.arange(TILES_Y, dtype=jnp.int32)[None, :], (TILES_X, TILES_Y))
    base_x = tile_x * AX
    base_y = tile_y * AY
    for batch_index in range(NB):
        obs_slots = obs_order[:, :, batch_index * OB:(batch_index + 1) * OB].astype(jnp.int32)
        obs_cells = jnp.take_along_axis(obs_cell.astype(jnp.int32), obs_slots, axis=2)
        values = jnp.take_along_axis(obs_value, obs_slots, axis=2)
        errors = jnp.take_along_axis(obs_error, obs_slots, axis=2)
        live = jnp.take_along_axis(obs_live, obs_slots, axis=2).astype(jnp.float32)
        observed = jnp.take_along_axis(anomaly[:, :, :, FIELDS, :], obs_cells[:, :, None, :], axis=3)
        predicted = jnp.take_along_axis(ens_mean[:, :, FIELDS, :], obs_cells, axis=2)
        pos_x = (base_x[:, :, None] + obs_cells // AY).astype(jnp.float32)
        pos_y = (base_y[:, :, None] + obs_cells % AY).astype(jnp.float32)
        extras = jnp.stack([values - predicted, errors, pos_x, pos_y, live], axis=2)
        packet = jnp.concatenate([observed, extras], axis=2)
        padded = jnp.pad(packet, ((1, 1), (1, 1), (0, 0), (0, 0)))
        beside_all = jnp.stack([padded[row_shift:row_shift + TILES_X, col_shift:col_shift + TILES_Y] for row_shift in range(3) for col_shift in range(3)], axis=2)

        def one_tile(inputs):
            packets, tile_anomaly, tile_mean, anchor_x, anchor_y = inputs
            mean_step, anomaly_step = update_group(packets, tile_anomaly, tile_mean, anchor_x, anchor_y)
            return (tile_mean + mean_step, tile_anomaly - anomaly_step)
        new_mean, new_anomaly = lax.map(one_tile, (beside_all.reshape(tiles, 9, MEM + 5, OB), anomaly.reshape(tiles, MEM, COMP, CELLS), ens_mean.reshape(tiles, COMP, CELLS), base_x.reshape(tiles), base_y.reshape(tiles)))
        ens_mean = new_mean.reshape(TILES_X, TILES_Y, COMP, CELLS)
        anomaly = new_anomaly.reshape(TILES_X, TILES_Y, MEM, COMP, CELLS)
    return (ens_mean, anomaly)
```

```python
import functools

import jax
import jax.numpy as jnp
import numpy as np
from jax import lax
from jax.experimental import pallas as pl
from jax.experimental.pallas import tpu as pltpu
from jax.sharding import PartitionSpec as P

AX = 8
AY = 16
OB = 32
NB = 2
RAD = 2
CODE = 64
LIMIT = 32 * 1024 * 1024

MESH = pl.DeviceIdType.MESH
OFFS = [(dx, dy) for dx in (-1, 0, 1) for dy in (-1, 0, 1)]
OTHERS = [i for i in range(9) if i != 4]


def taper_of(dx, dy):
    return max(1.0 - (dx * dx + dy * dy) / float(RAD * RAD), 0.0) ** 2


@functools.lru_cache
def tables():
    cells = AX * AY
    own = [(c // AY, c % AY) for c in range(cells)]
    halo = [
        (x, y)
        for x in range(-RAD, AX + RAD)
        for y in range(-RAD, AY + RAD)
        if not (0 <= x < AX and 0 <= y < AY)
    ]
    lanes = own + halo
    where = {xy: n for n, xy in enumerate(lanes)}
    code = np.full((8, 2 * cells), -1.0, np.float32)
    for n, (x, y) in enumerate(lanes):
        code[:, n] = (x + AX) * CODE + (y + AY)
    move = np.zeros((2 * cells, 2, 8, cells), np.float32)
    for n, (x, y) in enumerate(lanes):
        for d, i in enumerate(OTHERS):
            dx, dy = OFFS[i]
            src = where.get((x + dx, y + dy))
            if src is not None:
                move[src, n // cells, d, n % cells] = 1.0
    pick = np.zeros((8, cells, cells), np.float32)
    for n, (x, y) in enumerate(halo):
        i = (x // AX + 1) * 3 + (y // AY + 1)
        pick[OTHERS.index(i), (x % AX) * AY + (y % AY), n] = 1.0
    return code, move.reshape(2 * cells, 16 * cells), pick.reshape(8 * cells, cells)


def split_rows(block):
    high = block.astype(jnp.bfloat16).astype(jnp.float32)
    return jnp.concatenate([high, block - high], axis=0).astype(jnp.bfloat16)


def exchange_kernel(
    src_ref, order_ref, cell_ref, live_ref, value_ref, error_ref, ocean_ref, weights_ref, atm_ref,
    code_in, move_in, pick_in,
    tiles_ref, metat_ref, held, fmean, code_ref, move_ref, pick_ref,
    ocn, wts, meta, src, order_in, cell_in, live_in, value_in, error_in,
    local_sem, send_sem, recv_sem,
):
    gx, gy = lax.axis_index("gx"), lax.axis_index("gy")
    nx, ny = lax.axis_size("gx"), lax.axis_size("gy")
    members = tiles_ref.shape[1]
    fields = atm_ref.shape[0]
    slots = order_in.shape[1]

    def has_x(dx):
        return (gx + dx >= 0) & (gx + dx < nx)

    def has_y(dy):
        return (gy + dy >= 0) & (gy + dy < ny)

    def there(i):
        return has_x(OFFS[i][0]) & has_y(OFFS[i][1])

    pairs = (
        (ocean_ref, ocn.at[4]), (order_ref, order_in), (cell_ref, cell_in), (live_ref, live_in),
        (value_ref, value_in), (error_ref, error_in), (src_ref, src), (weights_ref, wts),
        (atm_ref, held), (code_in, code_ref), (move_in, move_ref), (pick_in, pick_ref),
    )
    staged = [pltpu.make_async_copy(x, y, local_sem.at[n]) for n, (x, y) in enumerate(pairs)]
    for copy in staged:
        copy.start()

    barrier = pltpu.get_barrier_semaphore()
    for i in OTHERS:
        dx, dy = OFFS[i]

        @pl.when(there(i))
        def _():
            pl.semaphore_signal(barrier, inc=1, device_id=(gx + dx, gy + dy), device_id_type=MESH)

    for i in OTHERS:

        @pl.when(jnp.logical_not(there(i)))
        def _():
            tiles_ref[i] = jnp.zeros(tiles_ref.shape[1:], jnp.float32)
            meta[i] = jnp.zeros(meta.shape[1:], jnp.float32)

    for n in range(9, meta.shape[0]):
        meta[n] = jnp.zeros(meta.shape[1:], jnp.float32)

    for copy in staged[1:6]:
        copy.wait()
    cell = cell_in[...]
    spot = ((cell // AY) * CODE + cell % AY).astype(jnp.float32)
    rows = jnp.concatenate(
        [
            spot, value_in[...], error_in[...], live_in[...].astype(jnp.float32),
            jnp.zeros((4, slots), jnp.float32),
        ],
        axis=0,
    )
    slot = lax.broadcasted_iota(jnp.int32, (slots, slots), 0)
    perm = jnp.where(order_in[...] == slot, 1.0, 0.0)
    rows = jnp.dot(rows, perm, precision=lax.Precision.HIGHEST, preferred_element_type=jnp.float32)
    meta[4] = jnp.concatenate([rows, jnp.zeros((8, meta.shape[2] - slots), jnp.float32)], axis=1)

    staged[0].wait()
    across = 1 + has_x(-1).astype(jnp.int32) + has_x(1).astype(jnp.int32)
    along = 1 + has_y(-1).astype(jnp.int32) + has_y(1).astype(jnp.int32)
    pl.semaphore_wait(barrier, across * along - 1)

    outer = lax.rem(gy, 2) * 2 - 1

    first = (members // 2 + 15) // 16 * 16
    parts = ((0, 0, first), (3, first, members - first))

    def ocean(part, source, target, n, dx, dy):
        kind, low, size = part
        return pltpu.make_async_remote_copy(
            src_ref=ocn.at[source, pl.ds(low, size)],
            dst_ref=ocn.at[target, pl.ds(low, size)],
            send_sem=send_sem.at[kind, n],
            recv_sem=recv_sem.at[kind, target],
            device_id=(gx + dx, gy + dy),
            device_id_type=MESH,
        )

    def arrive(part, at, dx, dy):
        ocean(part, at, at, 4, dx, dy).wait_recv()

    firsts = [
        (cond, ocean(part, 4, target, n, dx, dy))
        for part in parts
        for cond, target, n, dx, dy in (
            (has_y(outer), 4 - outer, 1, 0, outer),
            (has_x(-1), 7, 2, -1, 0),
            (has_x(1), 1, 3, 1, 0),
            (has_y(-outer), 4 + outer, 0, 0, -outer),
        )
    ]
    relays = [
        (has_y(outer) & has_x(dx), ocean(part, 4 + outer, 4 - 3 * dx + outer, n, dx, 0))
        for part in parts
        for dx, n in ((-1, 5), (1, 6))
    ]
    hands = [
        (
            part, dx, has_x(dx) & has_y(-outer),
            ocean(part, 4 + 3 * dx, 4 + 3 * dx + outer, n, 0, -outer),
        )
        for part in parts
        for dx, n in ((-1, 7), (1, 8))
    ]

    def begin(cond, copy):
        @pl.when(cond)
        def _():
            copy.start()

    for cond, copy in firsts:
        begin(cond, copy)

    def remote(buf, kind, i):
        dx, dy = OFFS[i]
        return pltpu.make_async_remote_copy(
            src_ref=buf.at[4],
            dst_ref=buf.at[8 - i],
            send_sem=send_sem.at[kind, i],
            recv_sem=recv_sem.at[kind, 8 - i],
            device_id=(gx + dx, gy + dy),
            device_id_type=MESH,
        )

    def column(i):
        dx, dy = OFFS[i]
        return pltpu.make_async_remote_copy(
            src_ref=tiles_ref.at[4],
            dst_ref=tiles_ref.at[8 - i],
            send_sem=send_sem.at[2, i],
            recv_sem=recv_sem.at[2, 8 - i],
            device_id=(gx + dx, gy + dy),
            device_id_type=MESH,
        )

    def send(buf, kind):
        for i in OTHERS:

            @pl.when(there(i))
            def _():
                remote(buf, kind, i).start()

    def receive(buf, kind):
        for i in OTHERS:

            @pl.when(there(i))
            def _():
                remote(buf, kind, 8 - i).wait_recv()

    def settle(buf, kind):
        for i in OTHERS:

            @pl.when(there(i))
            def _():
                remote(buf, kind, i).wait_send()

    send(meta, 1)

    staged[8].wait()
    for v in range(fields):
        block = held[v]
        mean = jnp.sum(block, axis=0, keepdims=True) / members
        fmean[v : v + 1, :] = mean
        held[v] = block - mean

    for at, part in enumerate(parts):

        @pl.when(has_y(outer))
        def _():
            arrive(part, 4 + outer, 0, outer)

        for cond, copy in relays[2 * at : 2 * at + 2]:
            begin(cond, copy)
    for part, dx, cond, copy in hands:

        @pl.when(has_x(dx))
        def _():
            arrive(part, 4 + 3 * dx, dx, 0)

        begin(cond, copy)

    receive(meta, 1)
    flat = meta[...].reshape(meta.shape[0] * meta.shape[1], meta.shape[2])
    metat_ref[...] = flat.T
    staged[6].wait()
    staged[7].wait()

    for part in parts:

        @pl.when(has_y(-outer))
        def _():
            arrive(part, 4 - outer, 0, -outer)

        for dx in (-1, 1):
            for dy in (outer, -outer):

                @pl.when(has_x(dx) & has_y(dy))
                def _():
                    arrive(part, 4 + 3 * dx + dy, dx, 0)

    total = jnp.zeros(tiles_ref.shape[1:], jnp.float32)
    for k in range(wts.shape[0]):
        source = src[0, k]
        position = (source // ny - gx + 1) * 3 + (source % ny - gy + 1)
        position = jnp.clip(position, 0, 8)
        total += jnp.dot(ocn[position], wts[k], preferred_element_type=jnp.float32)
    tiles_ref[4] = total
    for i in OTHERS:

        @pl.when(there(i))
        def _():
            column(i).start()

    for cond, copy in firsts + relays + [hand[2:] for hand in hands]:

        @pl.when(cond)
        def _():
            copy.wait_send()

    settle(meta, 1)
    for copy in staged[9:]:
        copy.wait()
    for i in OTHERS:

        @pl.when(there(i))
        def _():
            column(i).wait_send()
            column(8 - i).wait_recv()


def analysis_kernel(
    tiles_ref, metat_ref, fields_in, fmean_ref, code_ref, move_ref, pick_ref,
    mean_ref, anom_ref,
    held, shifted, out_sem,
):
    fields, members, cells = fields_in.shape

    scale = 1.0 / (members - 1)
    beside = split_rows(jnp.concatenate([tiles_ref[i] for i in OTHERS], axis=1))
    halo = jnp.dot(beside, pick_ref[...], preferred_element_type=jnp.float32)
    grid = jnp.concatenate([tiles_ref[4], halo[:members] + halo[members:]], axis=1)
    gmean = jnp.sum(grid, axis=0, keepdims=True) / members
    grid = grid - gmean
    code = code_ref[0:1, :]

    for b in range(NB):
        last = b == NB - 1
        variance = jnp.sum(grid * grid, axis=0, keepdims=True) / (members - 1)
        gains = jnp.zeros((OB, 2 * cells), jnp.float32)
        sums = jnp.zeros((OB, 2 * cells), jnp.float32)
        weights = jnp.zeros((OB, 2 * cells), jnp.float32)
        for i in range(9):
            dx, dy = OFFS[i]
            column = metat_ref[b * OB : (b + 1) * OB, 8 * i : 8 * i + 4]
            spot = column[:, 0:1] + float((AX * dx + AX) * CODE + AY * dy + AY)
            error = column[:, 2:3]
            live = column[:, 3:4]
            denom = variance + (error + (1.0 - live))
            weighting = live / denom
            damping = 1.0 / (1.0 + jnp.sqrt(error / denom))
            hit = spot == code
            weighting = jnp.where(hit, weighting, 0.0)
            weights = weights + weighting
            gains = gains + weighting * damping
            sums = sums + weighting * column[:, 1:2]
        alpha = jnp.sum(gains, axis=0, keepdims=True)
        beta = jnp.sum(sums, axis=0, keepdims=True) - gmean * jnp.sum(weights, axis=0, keepdims=True)
        extra = jnp.concatenate([alpha, beta, jnp.zeros((6, 2 * cells), jnp.float32)], axis=0)
        left = split_rows(jnp.concatenate([grid, extra], axis=0))
        width = (8 if last else 16) * cells
        moved = jnp.dot(left, move_ref[:, :width], preferred_element_type=jnp.float32)
        rows = members + 8
        shifted[:, :width] = moved[:rows] + moved[rows:]

        def step(block, part, center, alpha, beta):
            total = jnp.zeros_like(block)
            mean = jnp.zeros((1, cells), jnp.float32)
            for d in range(9):
                if d == 8:
                    source, a, m = center, alpha * scale, beta * scale
                else:
                    dx, dy = OFFS[OTHERS[d]]
                    weight = scale * taper_of(dx, dy)
                    at = (part * 8 + d) * cells
                    source = shifted[:members, at : at + cells]
                    a = shifted[members : members + 1, at : at + cells] * weight
                    m = shifted[members + 1 : members + 2, at : at + cells] * weight
                cov = jnp.sum(block * source, axis=0, keepdims=True)
                mean = mean + cov * m
                total = total + source * (cov * a)
            return block - total, mean

        own = grid[:, :cells]
        held[fields] = own
        own_args = (alpha[:, :cells], beta[:, :cells])

        def one_field(v, carry, own_args=own_args, last=last, b=b, step=step):
            block, mean = step(fields_in[v] if b == 0 else held[v], 0, held[fields], *own_args)
            held[v] = block
            before = fmean_ref[pl.ds(v, 1), :] if b == 0 else mean_ref[v]
            mean_ref[v] = before + mean
            if last:
                pltpu.make_async_copy(held.at[v], anom_ref.at[v], out_sem.at[v]).start()
            return carry

        lax.fori_loop(0, fields, one_field, 0)
        block, mean = step(own, 0, own, *own_args)
        if last:
            held[fields] = block
            mean_ref[fields] = gmean[:, :cells] + mean
            pltpu.make_async_copy(
                held.at[fields], anom_ref.at[fields], out_sem.at[fields]
            ).start()
            for v in range(fields + 1):
                pltpu.make_async_copy(held.at[v], anom_ref.at[v], out_sem.at[v]).wait()
        else:
            outer = grid[:, cells:]
            far, far_mean = step(outer, 1, outer, alpha[:, cells:], beta[:, cells:])
            grid = jnp.concatenate([block, far], axis=1)
            gmean = gmean + jnp.concatenate([mean, far_mean], axis=1)


def local(
    atm_members, ocean_members, remap_weights, pair_src, obs_cell, obs_value, obs_error,
    obs_live, obs_order,
):
    members, fields, cells = atm_members.shape[2:]
    slots = obs_cell.shape[2]
    sources, depth = remap_weights.shape[2:4]
    vmem = pl.BlockSpec(memory_space=pltpu.VMEM)
    anywhere = pl.BlockSpec(memory_space=pl.ANY)
    code, move, pick = tables()
    results = (
        pltpu.VMEM((9, members, cells), jnp.float32),
        pltpu.VMEM((128, 128), jnp.float32),
        pltpu.VMEM((fields, members, cells), jnp.float32),
        pltpu.VMEM((fields, cells), jnp.float32),
        pltpu.VMEM(code.shape, jnp.float32),
        pltpu.VMEM(move.shape, jnp.bfloat16),
        pltpu.VMEM(pick.shape, jnp.bfloat16),
    )
    state = pl.pallas_call(
        exchange_kernel,
        out_shape=results,
        in_specs=[anywhere] * 12,
        out_specs=(vmem,) * 7,
        scratch_shapes=[
            pltpu.VMEM((9, members, depth), jnp.bfloat16),
            pltpu.VMEM((sources, depth, cells), jnp.bfloat16),
            pltpu.VMEM((16, 8, 128), jnp.float32),
            pltpu.SMEM((1, sources), jnp.int32),
            pltpu.VMEM((1, slots), jnp.int32),
            pltpu.VMEM((1, slots), jnp.int32),
            pltpu.VMEM((1, slots), jnp.int32),
            pltpu.VMEM((1, slots), jnp.float32),
            pltpu.VMEM((1, slots), jnp.float32),
            pltpu.SemaphoreType.DMA((12,)),
            pltpu.SemaphoreType.DMA((4, 9)),
            pltpu.SemaphoreType.DMA((4, 9)),
        ],
        compiler_params=pltpu.CompilerParams(
            collective_id=0, has_side_effects=True, vmem_limit_bytes=LIMIT
        ),
        name="exchange",
    )(
        *(
            pltpu.with_memory_space_constraint(x, pltpu.HBM)
            for x in (
                pair_src[0], obs_order[0], obs_cell[0], obs_live[0], obs_value[0], obs_error[0],
                ocean_members[0, 0], remap_weights[0, 0],
                jnp.transpose(atm_members[0, 0], (1, 0, 2)),
                jnp.asarray(code), jnp.asarray(move, jnp.bfloat16), jnp.asarray(pick, jnp.bfloat16),
            )
        )
    )
    post_mean, post_anom = pl.pallas_call(
        analysis_kernel,
        out_shape=(
            jax.ShapeDtypeStruct((fields + 1, 1, cells), jnp.float32),
            jax.ShapeDtypeStruct((fields + 1, members, cells), jnp.float32),
        ),
        in_specs=[vmem] * 7,
        out_specs=(vmem, anywhere),
        scratch_shapes=[
            pltpu.VMEM((fields + 1, members, cells), jnp.float32),
            pltpu.VMEM((members + 8, 16 * cells), jnp.float32),
            pltpu.SemaphoreType.DMA((fields + 1,)),
        ],
        compiler_params=pltpu.CompilerParams(vmem_limit_bytes=LIMIT),
        name="analysis",
    )(*state)
    return (post_mean.reshape(1, 1, fields + 1, cells), jnp.transpose(post_anom, (1, 0, 2))[None, None])


def solution(mesh):
    in_specs = (
        P("gx", "gy", None, None, None),
        P("gx", "gy", None, None),
        P("gx", "gy", None, None, None),
        P("gx", "gy", None),
        P("gx", "gy", None),
        P("gx", "gy", None),
        P("gx", "gy", None),
        P("gx", "gy", None),
        P("gx", "gy", None),
    )
    out_specs = (P("gx", "gy", None, None), P("gx", "gy", None, None, None))
    return jax.shard_map(local, mesh=mesh, in_specs=in_specs, out_specs=out_specs, check_vma=False)
```

```python
import functools

import jax
import jax.numpy as jnp
import numpy as np
from jax import lax
from jax.experimental import pallas as pl
from jax.experimental.pallas import tpu as pltpu
from jax.sharding import PartitionSpec as P

AX = 8
AY = 16
OB = 32
NB = 2
RAD = 2
CODE = 64
LIMIT = 32 * 1024 * 1024

MESH = pl.DeviceIdType.MESH
OFFS = [(dx, dy) for dx in (-1, 0, 1) for dy in (-1, 0, 1)]
OTHERS = [i for i in range(9) if i != 4]
NEAR = [1, 3, 5, 7]
FAR = [0, 2, 6, 8]
PIECE = 16
SHARE = 4


def taper_of(dx, dy):
    return max(1.0 - (dx * dx + dy * dy) / float(RAD * RAD), 0.0) ** 2


def edge(d, size):
    return {-1: range(RAD), 0: range(size), 1: range(size - RAD, size)}[d]


def strip(i):
    dx, dy = OFFS[i]
    return [(x, y) for x in edge(dx, AX) for y in edge(dy, AY)]


def strips():
    spans, at = {}, 0
    for i in OTHERS:
        rows = -(-len(strip(i)) // 8) * 8
        spans[i] = (at, rows)
        at += rows
    return spans


SPANS = strips()


@functools.lru_cache
def tables():
    cells = AX * AY
    where = {(c // AY, c % AY): c for c in range(cells)}
    out = np.zeros((cells, cells), np.float32)
    for i in OTHERS:
        dx, dy = OFFS[i]
        for n, (x, y) in enumerate(strip(i)):
            out[SPANS[i][0] + n, x * AY + y] = 1.0
        for n, (x, y) in enumerate(strip(8 - i)):
            where[(x + dx * AX, y + dy * AY)] = cells + SPANS[i][0] + n
    code = np.full((8, 2 * cells), -1.0, np.float32)
    move = np.zeros((2 * cells, 2, 8, cells), np.float32)
    for (x, y), n in where.items():
        code[:, n] = (x + AX) * CODE + (y + AY)
        for d, i in enumerate(OTHERS):
            dx, dy = OFFS[i]
            src = where.get((x + dx, y + dy))
            if src is not None:
                move[src, n // cells, d, n % cells] = 1.0
    return code, move.reshape(2 * cells, 16 * cells), out


def split_rows(block):
    high = block.astype(jnp.bfloat16).astype(jnp.float32)
    return jnp.concatenate([high, block - high], axis=0).astype(jnp.bfloat16)


def exchange_kernel(
    src_ref, order_ref, cell_ref, live_ref, value_ref, error_ref, ocean_ref, weights_ref, atm_ref,
    code_in, move_in, out_in,
    own_ref, halo_ref, metat_ref, held, fmean, code_ref, move_ref,
    ocn, wts, meta, src, order_in, cell_in, live_in, value_in, error_in, out, strip_ref,
    local_sem, send_sem, recv_sem, note_sem,
):
    gx, gy = lax.axis_index("gx"), lax.axis_index("gy")
    nx, ny = lax.axis_size("gx"), lax.axis_size("gy")
    members = own_ref.shape[0]
    fields = atm_ref.shape[0]
    slots = order_in.shape[1]

    def has_x(dx):
        return (gx + dx >= 0) & (gx + dx < nx)

    def has_y(dy):
        return (gy + dy >= 0) & (gy + dy < ny)

    def there(i):
        return has_x(OFFS[i][0]) & has_y(OFFS[i][1])

    pairs = (
        (ocean_ref, ocn.at[4]), (order_ref, order_in), (cell_ref, cell_in), (live_ref, live_in),
        (value_ref, value_in), (error_ref, error_in), (src_ref, src), (weights_ref, wts),
        (atm_ref, held), (code_in, code_ref), (move_in, move_ref), (out_in, out),
    )
    staged = [pltpu.make_async_copy(x, y, local_sem.at[n]) for n, (x, y) in enumerate(pairs)]
    for copy in staged:
        copy.start()

    barrier = pltpu.get_barrier_semaphore()
    for i in NEAR:
        dx, dy = OFFS[i]

        @pl.when(there(i))
        def _():
            pl.semaphore_signal(barrier, inc=1, device_id=(gx + dx, gy + dy), device_id_type=MESH)

    for i in OTHERS:

        @pl.when(jnp.logical_not(there(i)))
        def _():
            at, rows = SPANS[i]
            halo_ref[at : at + rows, :] = jnp.zeros((rows, halo_ref.shape[1]), jnp.float32)
            meta[i] = jnp.zeros(meta.shape[1:], jnp.float32)

    for n in range(9, meta.shape[0]):
        meta[n] = jnp.zeros(meta.shape[1:], jnp.float32)

    for copy in staged[1:6]:
        copy.wait()
    cell = cell_in[...]
    spot = ((cell // AY) * CODE + cell % AY).astype(jnp.float32)
    rows = jnp.concatenate(
        [
            spot, value_in[...], error_in[...], live_in[...].astype(jnp.float32),
            jnp.zeros((4, slots), jnp.float32),
        ],
        axis=0,
    )
    slot = lax.broadcasted_iota(jnp.int32, (slots, slots), 0)
    perm = jnp.where(order_in[...] == slot, 1.0, 0.0)
    rows = jnp.dot(rows, perm, precision=lax.Precision.HIGHEST, preferred_element_type=jnp.float32)
    meta[4] = jnp.concatenate([rows, jnp.zeros((8, meta.shape[2] - slots), jnp.float32)], axis=1)

    staged[0].wait()
    pl.semaphore_wait(barrier, sum(there(i).astype(jnp.int32) for i in NEAR))

    outer = lax.rem(gy, 2) * 2 - 1
    count = members // PIECE

    def relayed(y, p):
        at = lax.rem(y + 8, 8)
        return ((at == 2) | (at == 5)) if p >= SHARE else ((at != 1) & (at != 6))

    def ocean(p, source, target, kind, dx, dy, shared=False):
        return pltpu.make_async_remote_copy(
            src_ref=ocn.at[source, pl.ds(p * PIECE, PIECE)],
            dst_ref=ocn.at[target, pl.ds(p * PIECE, PIECE)],
            send_sem=send_sem.at[kind, p],
            recv_sem=recv_sem.at[target, 0 if shared else p],
            device_id=(gx + dx, gy + dy),
            device_id_type=MESH,
        )

    def arrive(p, at, dx, dy):
        ocean(p, at, at, 0, dx, dy).wait_recv()

    def arrive_all(at, dx, dy):
        pltpu.make_async_remote_copy(
            src_ref=ocn.at[at],
            dst_ref=ocn.at[at],
            send_sem=send_sem.at[0, 0],
            recv_sem=recv_sem.at[at, 0],
            device_id=(gx + dx, gy + dy),
            device_id_type=MESH,
        ).wait_recv()

    order = range(count)
    sends = [
        (has_y(outer), [ocean(p, 4, 4 - outer, 1, 0, outer) for p in order]),
        (has_x(-1), [ocean(p, 4, 7, 2, -1, 0) for p in reversed(order)]),
        (has_x(1), [ocean(p, 4, 1, 3, 1, 0) for p in reversed(order)]),
        (has_y(-outer), [ocean(p, 4, 4 + outer, 0, 0, -outer, True) for p in order]),
    ]
    for cond, copies in sends:

        @pl.when(cond)
        def _():
            for copy in copies:
                copy.start()

    def relay(p, dx):
        return ocean(p, 4 + outer, 4 - 3 * dx + outer, 4 if dx < 0 else 5, dx, 0, True)

    def forward(p, dx):
        return ocean(p, 4 + 3 * dx, 4 + 3 * dx - outer, 6 if dx < 0 else 7, 0, outer, True)

    def hand(p, dx):
        return ocean(p, 4 + 3 * dx, 4 + 3 * dx + outer, 8 if dx < 0 else 9, 0, -outer, True)

    for p in order:
        for dx in (-1, 1):
            sends.append((has_x(dx) & has_y(outer) & relayed(gy + outer, p), [relay(p, dx)]))
            sends.append(
                (has_x(dx) & has_y(outer) & jnp.logical_not(relayed(gy, p)), [forward(p, dx)])
            )
    for dx in (-1, 1):
        sends.append((has_x(dx) & has_y(-outer), [hand(p, dx) for p in order]))

    def remote(i):
        dx, dy = OFFS[i]
        return pltpu.make_async_remote_copy(
            src_ref=meta.at[4],
            dst_ref=meta.at[8 - i],
            send_sem=note_sem.at[0, i],
            recv_sem=note_sem.at[1, 8 - i],
            device_id=(gx + dx, gy + dy),
            device_id_type=MESH,
        )

    def border(i):
        dx, dy = OFFS[i]
        (source, rows), (target, _) = SPANS[i], SPANS[8 - i]
        return pltpu.make_async_remote_copy(
            src_ref=strip_ref.at[pl.ds(source, rows)],
            dst_ref=halo_ref.at[pl.ds(target, rows)],
            send_sem=note_sem.at[2, i],
            recv_sem=note_sem.at[3, 8 - i],
            device_id=(gx + dx, gy + dy),
            device_id_type=MESH,
        )

    def each(which, act):
        for i in which:

            @pl.when(there(i))
            def _():
                act(i)

    each(NEAR, lambda i: remote(i).start())

    staged[8].wait()
    for v in range(fields):
        block = held[v]
        mean = jnp.sum(block, axis=0, keepdims=True) / members
        fmean[v : v + 1, :] = mean
        held[v] = block - mean

    for p in order:
        back = count - 1 - p
        for dx in (-1, 1):

            @pl.when(has_x(dx))
            def _():
                arrive(back, 4 + 3 * dx, dx, 0)

                @pl.when(has_y(outer) & jnp.logical_not(relayed(gy, back)))
                def _():
                    forward(back, dx).start()

                @pl.when(has_y(-outer))
                def _():
                    hand(back, dx).start()

        if p == 0:
            each(FAR, lambda i: remote(i).start())

        @pl.when(has_y(outer))
        def _():
            arrive(p, 4 + outer, 0, outer)

            @pl.when(relayed(gy + outer, p))
            def _():
                for dx in (-1, 1):

                    @pl.when(has_x(dx))
                    def _():
                        relay(p, dx).start()

    each(OTHERS, lambda i: remote(8 - i).wait_recv())
    flat = meta[...].reshape(meta.shape[0] * meta.shape[1], meta.shape[2])
    metat_ref[...] = flat.T
    staged[6].wait()
    staged[7].wait()
    staged[11].wait()

    @pl.when(has_y(-outer))
    def _():
        arrive_all(4 - outer, 0, -outer)

    for dx in (-1, 1):
        for dy in (-outer, outer):

            @pl.when(has_x(dx) & has_y(dy))
            def _():
                arrive_all(4 + 3 * dx + dy, dx, 0)

    total = jnp.zeros(own_ref.shape, jnp.float32)
    for k in range(wts.shape[0]):
        source = src[0, k]
        position = (source // ny - gx + 1) * 3 + (source % ny - gy + 1)
        position = jnp.clip(position, 0, 8)
        total += jnp.dot(ocn[position], wts[k], preferred_element_type=jnp.float32)
    own_ref[...] = total
    rest = jnp.zeros((out.shape[0] - members, total.shape[1]), jnp.float32)
    picked = lax.dot_general(
        out[...], split_rows(jnp.concatenate([total, rest], axis=0)), (((1,), (1,)), ((), ())),
        preferred_element_type=jnp.float32,
    )
    strip_ref[...] = picked[:, : out.shape[0]] + picked[:, out.shape[0] :]
    each(FAR + NEAR, lambda i: border(i).start())
    for cond, copies in sends:

        @pl.when(cond)
        def _():
            for copy in copies:
                copy.wait_send()

    each(OTHERS, lambda i: remote(i).wait_send())
    for copy in staged[9:11]:
        copy.wait()
    each(OTHERS, lambda i: border(i).wait_send())
    each(OTHERS, lambda i: border(8 - i).wait_recv())


def analysis_kernel(
    own_ref, halo_ref, metat_ref, fields_in, fmean_ref, code_ref, move_ref,
    mean_ref, anom_ref,
    held, shifted, out_sem,
):
    fields, members, cells = fields_in.shape

    scale = 1.0 / (members - 1)
    grid = jnp.concatenate([own_ref[...], halo_ref[...].T[:members]], axis=1)
    gmean = jnp.sum(grid, axis=0, keepdims=True) / members
    grid = grid - gmean
    code = code_ref[0:1, :]

    for b in range(NB):
        last = b == NB - 1
        variance = jnp.sum(grid * grid, axis=0, keepdims=True) / (members - 1)
        gains = jnp.zeros((OB, 2 * cells), jnp.float32)
        sums = jnp.zeros((OB, 2 * cells), jnp.float32)
        weights = jnp.zeros((OB, 2 * cells), jnp.float32)
        for i in range(9):
            dx, dy = OFFS[i]
            column = metat_ref[b * OB : (b + 1) * OB, 8 * i : 8 * i + 4]
            spot = column[:, 0:1] + float((AX * dx + AX) * CODE + AY * dy + AY)
            error = column[:, 2:3]
            live = column[:, 3:4]
            denom = variance + (error + (1.0 - live))
            weighting = live / denom
            damping = 1.0 / (1.0 + jnp.sqrt(error / denom))
            hit = spot == code
            weighting = jnp.where(hit, weighting, 0.0)
            weights = weights + weighting
            gains = gains + weighting * damping
            sums = sums + weighting * column[:, 1:2]
        alpha = jnp.sum(gains, axis=0, keepdims=True)
        beta = jnp.sum(sums, axis=0, keepdims=True) - gmean * jnp.sum(weights, axis=0, keepdims=True)
        extra = jnp.concatenate([alpha, beta, jnp.zeros((6, 2 * cells), jnp.float32)], axis=0)
        left = split_rows(jnp.concatenate([grid, extra], axis=0))
        width = (8 if last else 16) * cells
        moved = jnp.dot(left, move_ref[:, :width], preferred_element_type=jnp.float32)
        rows = members + 8
        shifted[:, :width] = moved[:rows] + moved[rows:]

        def step(block, part, center, alpha, beta):
            total = jnp.zeros_like(block)
            mean = jnp.zeros((1, cells), jnp.float32)
            for d in range(9):
                if d == 8:
                    source, a, m = center, alpha * scale, beta * scale
                else:
                    dx, dy = OFFS[OTHERS[d]]
                    weight = scale * taper_of(dx, dy)
                    at = (part * 8 + d) * cells
                    source = shifted[:members, at : at + cells]
                    a = shifted[members : members + 1, at : at + cells] * weight
                    m = shifted[members + 1 : members + 2, at : at + cells] * weight
                cov = jnp.sum(block * source, axis=0, keepdims=True)
                mean = mean + cov * m
                total = total + source * (cov * a)
            return block - total, mean

        own = grid[:, :cells]
        held[fields] = own
        own_args = (alpha[:, :cells], beta[:, :cells])

        def one_field(v, carry, own_args=own_args, last=last, b=b, step=step):
            block, mean = step(fields_in[v] if b == 0 else held[v], 0, held[fields], *own_args)
            held[v] = block
            before = fmean_ref[pl.ds(v, 1), :] if b == 0 else mean_ref[v]
            mean_ref[v] = before + mean
            if last:
                pltpu.make_async_copy(held.at[v], anom_ref.at[v], out_sem.at[v]).start()
            return carry

        lax.fori_loop(0, fields, one_field, 0)
        block, mean = step(own, 0, own, *own_args)
        if last:
            held[fields] = block
            mean_ref[fields] = gmean[:, :cells] + mean
            pltpu.make_async_copy(
                held.at[fields], anom_ref.at[fields], out_sem.at[fields]
            ).start()
            for v in range(fields + 1):
                pltpu.make_async_copy(held.at[v], anom_ref.at[v], out_sem.at[v]).wait()
        else:
            outer = grid[:, cells:]
            far, far_mean = step(outer, 1, outer, alpha[:, cells:], beta[:, cells:])
            grid = jnp.concatenate([block, far], axis=1)
            gmean = gmean + jnp.concatenate([mean, far_mean], axis=1)


def local(
    atm_members, ocean_members, remap_weights, pair_src, obs_cell, obs_value, obs_error,
    obs_live, obs_order,
):
    members, fields, cells = atm_members.shape[2:]
    slots = obs_cell.shape[2]
    sources, depth = remap_weights.shape[2:4]
    vmem = pl.BlockSpec(memory_space=pltpu.VMEM)
    anywhere = pl.BlockSpec(memory_space=pl.ANY)
    code, move, out = tables()
    results = (
        pltpu.VMEM((members, cells), jnp.float32),
        pltpu.VMEM((cells, 128), jnp.float32),
        pltpu.VMEM((128, 128), jnp.float32),
        pltpu.VMEM((fields, members, cells), jnp.float32),
        pltpu.VMEM((fields, cells), jnp.float32),
        pltpu.VMEM(code.shape, jnp.float32),
        pltpu.VMEM(move.shape, jnp.bfloat16),
    )
    state = pl.pallas_call(
        exchange_kernel,
        out_shape=results,
        in_specs=[anywhere] * 12,
        out_specs=(vmem,) * 7,
        scratch_shapes=[
            pltpu.VMEM((9, members, depth), jnp.bfloat16),
            pltpu.VMEM((sources, depth, cells), jnp.bfloat16),
            pltpu.VMEM((16, 8, 128), jnp.float32),
            pltpu.SMEM((1, sources), jnp.int32),
            pltpu.VMEM((1, slots), jnp.int32),
            pltpu.VMEM((1, slots), jnp.int32),
            pltpu.VMEM((1, slots), jnp.int32),
            pltpu.VMEM((1, slots), jnp.float32),
            pltpu.VMEM((1, slots), jnp.float32),
            pltpu.VMEM(out.shape, jnp.bfloat16),
            pltpu.VMEM((cells, 128), jnp.float32),
            pltpu.SemaphoreType.DMA((12,)),
            pltpu.SemaphoreType.DMA((10, members // PIECE)),
            pltpu.SemaphoreType.DMA((9, members // PIECE)),
            pltpu.SemaphoreType.DMA((4, 9)),
        ],
        compiler_params=pltpu.CompilerParams(
            collective_id=0, has_side_effects=True, vmem_limit_bytes=LIMIT
        ),
        name="exchange",
    )(
        *(
            pltpu.with_memory_space_constraint(x, pltpu.HBM)
            for x in (
                pair_src[0], obs_order[0], obs_cell[0], obs_live[0], obs_value[0], obs_error[0],
                ocean_members[0, 0], remap_weights[0, 0],
                jnp.transpose(atm_members[0, 0], (1, 0, 2)),
                jnp.asarray(code), jnp.asarray(move, jnp.bfloat16), jnp.asarray(out, jnp.bfloat16),
            )
        )
    )
    post_mean, post_anom = pl.pallas_call(
        analysis_kernel,
        out_shape=(
            jax.ShapeDtypeStruct((fields + 1, 1, cells), jnp.float32),
            jax.ShapeDtypeStruct((fields + 1, members, cells), jnp.float32),
        ),
        in_specs=[vmem] * 7,
        out_specs=(vmem, anywhere),
        scratch_shapes=[
            pltpu.VMEM((fields + 1, members, cells), jnp.float32),
            pltpu.VMEM((members + 8, 16 * cells), jnp.float32),
            pltpu.SemaphoreType.DMA((fields + 1,)),
        ],
        compiler_params=pltpu.CompilerParams(vmem_limit_bytes=LIMIT),
        name="analysis",
    )(*state)
    return (post_mean.reshape(1, 1, fields + 1, cells), jnp.transpose(post_anom, (1, 0, 2))[None, None])


def solution(mesh):
    in_specs = (
        P("gx", "gy", None, None, None),
        P("gx", "gy", None, None),
        P("gx", "gy", None, None, None),
        P("gx", "gy", None),
        P("gx", "gy", None),
        P("gx", "gy", None),
        P("gx", "gy", None),
        P("gx", "gy", None),
        P("gx", "gy", None),
    )
    out_specs = (P("gx", "gy", None, None), P("gx", "gy", None, None, None))
    return jax.shard_map(local, mesh=mesh, in_specs=in_specs, out_specs=out_specs, check_vma=False)
```

```python
import functools

import jax
import jax.numpy as jnp
import numpy as np
from jax import lax
from jax.experimental import pallas as pl
from jax.experimental.pallas import tpu as pltpu
from jax.sharding import PartitionSpec as P

AX = 8
AY = 16
OB = 32
NB = 2
RAD = 2
CODE = 64
LIMIT = 32 * 1024 * 1024

MESH = pl.DeviceIdType.MESH
OFFS = [(dx, dy) for dx in (-1, 0, 1) for dy in (-1, 0, 1)]
OTHERS = [i for i in range(9) if i != 4]
NEAR = [1, 3, 5, 7]
FAR = [0, 2, 6, 8]
PIECE = 16
SHARE = 4
SLOTS = 5


def taper_of(dx, dy):
    return max(1.0 - (dx * dx + dy * dy) / float(RAD * RAD), 0.0) ** 2


def edge(d, size):
    return {-1: range(RAD), 0: range(size), 1: range(size - RAD, size)}[d]


def strip(i):
    dx, dy = OFFS[i]
    return [(x, y) for x in edge(dx, AX) for y in edge(dy, AY)]


def strips():
    spans, at = {}, 0
    for i in OTHERS:
        rows = -(-len(strip(i)) // 8) * 8
        spans[i] = (at, rows)
        at += rows
    return spans


SPANS = strips()


@functools.lru_cache
def tables():
    cells = AX * AY
    where = {(c // AY, c % AY): c for c in range(cells)}
    out = np.zeros((cells, cells), np.float32)
    for i in OTHERS:
        dx, dy = OFFS[i]
        for n, (x, y) in enumerate(strip(i)):
            out[SPANS[i][0] + n, x * AY + y] = 1.0
        for n, (x, y) in enumerate(strip(8 - i)):
            where[(x + dx * AX, y + dy * AY)] = cells + SPANS[i][0] + n
    code = np.full((8, 2 * cells), -1.0, np.float32)
    code[1:, :] = 0.0
    move = np.zeros((2 * cells, 2, 8, cells), np.float32)
    slot = np.zeros((2 * cells, SLOTS, cells), np.float32)
    for (x, y), n in where.items():
        code[0, n] = (x + AX) * CODE + (y + AY)
        taken = 0
        for d, i in enumerate(OTHERS):
            dx, dy = OFFS[i]
            src = where.get((x + dx, y + dy))
            if src is not None:
                move[src, n // cells, d, n % cells] = 1.0
                if n < cells <= src:
                    slot[src, taken, n] = 1.0
                    code[1 + taken, n] = taper_of(dx, dy)
                    taken += 1
    own = move[:, 0].reshape(2 * cells, 8 * cells)
    far = move[:, 1].reshape(2 * cells, 8 * cells)
    slot = slot.reshape(2 * cells, SLOTS * cells)
    return code, own, far, slot, out


def split_rows(block):
    high = block.astype(jnp.bfloat16).astype(jnp.float32)
    return jnp.concatenate([high, block - high], axis=0).astype(jnp.bfloat16)


def moments(block, members):
    mean = jnp.sum(block, axis=0, keepdims=True) / members
    return mean, block - mean


def strengths(block, mean, table, members):
    variance = jnp.sum(block * block, axis=0, keepdims=True) / (members - 1)
    live, error, value, base = table
    denom = variance + base
    weighting = live / denom
    damping = 1.0 / (1.0 + jnp.sqrt(error / denom))
    alpha = jnp.sum(weighting * damping, axis=0, keepdims=True)
    beta = jnp.sum(weighting * value, axis=0, keepdims=True)
    return alpha, beta - mean * jnp.sum(weighting, axis=0, keepdims=True)


def shift(block, alpha, beta, tables):
    rest = jnp.zeros((6, block.shape[1]), jnp.float32)
    rows = block.shape[0] + 8
    left = split_rows(jnp.concatenate([block, alpha, beta, rest], axis=0))
    moved = jnp.dot(left, tables, preferred_element_type=jnp.float32)
    return moved[:rows] + moved[rows:]


def gather(block, sources):
    total = jnp.zeros_like(block)
    mean = jnp.zeros((1, block.shape[1]), jnp.float32)
    for source, a, m in sources:
        cov = jnp.sum(block * source, axis=0, keepdims=True)
        mean = mean + cov * m
        total = total + source * (cov * a)
    return total, mean


def sources_of(shifted, members, weights):
    cells = weights[0][1]
    found = []
    for d, (weight, width) in enumerate(weights):
        part = slice(d * cells, d * cells + width)
        found.append(
            (
                shifted[:members, part],
                shifted[members : members + 1, part] * weight,
                shifted[members + 1 : members + 2, part] * weight,
            )
        )
    return found


def around(scale, cells):
    return [(scale * taper_of(*OFFS[i]), cells) for i in OTHERS]


def exchange_kernel(
    src_ref, order_ref, cell_ref, live_ref, value_ref, error_ref, ocean_ref, weights_ref, atm_ref,
    code_in, near_in, far_in, slot_in, out_in,
    own_ref, halo_ref, obs_ref, held, part_ref, fmean, beyond_ref, code_ref, near_ref, far_ref, slot_ref,
    ocn, wts, meta, src, order_in, cell_in, live_in, value_in, error_in, out, strip_ref, shifted,
    local_sem, send_sem, recv_sem, note_sem,
):
    gx, gy = lax.axis_index("gx"), lax.axis_index("gy")
    nx, ny = lax.axis_size("gx"), lax.axis_size("gy")
    members = own_ref.shape[0]
    fields = atm_ref.shape[0]
    slots = order_in.shape[1]

    def has_x(dx):
        return (gx + dx >= 0) & (gx + dx < nx)

    def has_y(dy):
        return (gy + dy >= 0) & (gy + dy < ny)

    def there(i):
        return has_x(OFFS[i][0]) & has_y(OFFS[i][1])

    pairs = (
        (ocean_ref, ocn.at[4]), (order_ref, order_in), (cell_ref, cell_in), (live_ref, live_in),
        (value_ref, value_in), (error_ref, error_in), (src_ref, src), (weights_ref, wts),
        (atm_ref, held), (code_in, code_ref), (out_in, out), (near_in, near_ref),
        (far_in, far_ref), (slot_in, slot_ref),
    )
    staged = [pltpu.make_async_copy(x, y, local_sem.at[n]) for n, (x, y) in enumerate(pairs)]
    for copy in staged:
        copy.start()

    barrier = pltpu.get_barrier_semaphore()
    for i in NEAR:
        dx, dy = OFFS[i]

        @pl.when(there(i))
        def _():
            pl.semaphore_signal(barrier, inc=1, device_id=(gx + dx, gy + dy), device_id_type=MESH)

    for i in OTHERS:

        @pl.when(jnp.logical_not(there(i)))
        def _():
            at, rows = SPANS[i]
            halo_ref[at : at + rows, :] = jnp.zeros((rows, halo_ref.shape[1]), jnp.float32)
            meta[i] = jnp.zeros(meta.shape[1:], jnp.float32)

    for n in range(9, meta.shape[0]):
        meta[n] = jnp.zeros(meta.shape[1:], jnp.float32)

    for copy in staged[1:6]:
        copy.wait()
    cell = cell_in[...]
    spot = ((cell // AY) * CODE + cell % AY).astype(jnp.float32)
    rows = jnp.concatenate(
        [
            spot, value_in[...], error_in[...], live_in[...].astype(jnp.float32),
            jnp.zeros((4, slots), jnp.float32),
        ],
        axis=0,
    )
    slot = lax.broadcasted_iota(jnp.int32, (slots, slots), 0)
    perm = jnp.where(order_in[...] == slot, 1.0, 0.0)
    rows = jnp.dot(rows, perm, precision=lax.Precision.HIGHEST, preferred_element_type=jnp.float32)
    meta[4] = jnp.concatenate([rows, jnp.zeros((8, meta.shape[2] - slots), jnp.float32)], axis=1)

    staged[0].wait()
    pl.semaphore_wait(barrier, sum(there(i).astype(jnp.int32) for i in NEAR))

    outer = lax.rem(gy, 2) * 2 - 1
    count = members // PIECE

    def relayed(y, p):
        at = lax.rem(y + 8, 8)
        return ((at == 2) | (at == 5)) if p >= SHARE else ((at != 1) & (at != 6))

    def ocean(p, source, target, kind, dx, dy, shared=False):
        return pltpu.make_async_remote_copy(
            src_ref=ocn.at[source, pl.ds(p * PIECE, PIECE)],
            dst_ref=ocn.at[target, pl.ds(p * PIECE, PIECE)],
            send_sem=send_sem.at[kind, p],
            recv_sem=recv_sem.at[target, 0 if shared else p],
            device_id=(gx + dx, gy + dy),
            device_id_type=MESH,
        )

    def arrive(p, at, dx, dy):
        ocean(p, at, at, 0, dx, dy).wait_recv()

    def arrive_all(at, dx, dy):
        pltpu.make_async_remote_copy(
            src_ref=ocn.at[at],
            dst_ref=ocn.at[at],
            send_sem=send_sem.at[0, 0],
            recv_sem=recv_sem.at[at, 0],
            device_id=(gx + dx, gy + dy),
            device_id_type=MESH,
        ).wait_recv()

    order = range(count)
    sends = [
        (has_y(outer), [ocean(p, 4, 4 - outer, 1, 0, outer) for p in order]),
        (has_x(-1), [ocean(p, 4, 7, 2, -1, 0) for p in reversed(order)]),
        (has_x(1), [ocean(p, 4, 1, 3, 1, 0) for p in reversed(order)]),
        (has_y(-outer), [ocean(p, 4, 4 + outer, 0, 0, -outer, True) for p in order]),
    ]
    for cond, copies in sends:

        @pl.when(cond)
        def _():
            for copy in copies:
                copy.start()

    def relay(p, dx):
        return ocean(p, 4 + outer, 4 - 3 * dx + outer, 4 if dx < 0 else 5, dx, 0, True)

    def forward(p, dx):
        return ocean(p, 4 + 3 * dx, 4 + 3 * dx - outer, 6 if dx < 0 else 7, 0, outer, True)

    def hand(p, dx):
        return ocean(p, 4 + 3 * dx, 4 + 3 * dx + outer, 8 if dx < 0 else 9, 0, -outer, True)

    for p in order:
        for dx in (-1, 1):
            sends.append((has_x(dx) & has_y(outer) & relayed(gy + outer, p), [relay(p, dx)]))
            sends.append(
                (has_x(dx) & has_y(outer) & jnp.logical_not(relayed(gy, p)), [forward(p, dx)])
            )
    for dx in (-1, 1):
        sends.append((has_x(dx) & has_y(-outer), [hand(p, dx) for p in order]))

    def remote(i):
        dx, dy = OFFS[i]
        return pltpu.make_async_remote_copy(
            src_ref=meta.at[4],
            dst_ref=meta.at[8 - i],
            send_sem=note_sem.at[0, i],
            recv_sem=note_sem.at[1, 8 - i],
            device_id=(gx + dx, gy + dy),
            device_id_type=MESH,
        )

    def border(i):
        dx, dy = OFFS[i]
        (source, rows), (target, _) = SPANS[i], SPANS[8 - i]
        return pltpu.make_async_remote_copy(
            src_ref=strip_ref.at[pl.ds(source, rows)],
            dst_ref=halo_ref.at[pl.ds(target, rows)],
            send_sem=note_sem.at[2, i],
            recv_sem=note_sem.at[3, 8 - i],
            device_id=(gx + dx, gy + dy),
            device_id_type=MESH,
        )

    def each(which, act):
        for i in which:

            @pl.when(there(i))
            def _():
                act(i)

    each(NEAR, lambda i: remote(i).start())

    staged[8].wait()
    for v in range(fields):
        block = held[v]
        mean = jnp.sum(block, axis=0, keepdims=True) / members
        fmean[v : v + 1, :] = mean
        held[v] = block - mean

    for p in order:
        back = count - 1 - p
        for dx in (-1, 1):

            @pl.when(has_x(dx))
            def _():
                arrive(back, 4 + 3 * dx, dx, 0)

                @pl.when(has_y(outer) & jnp.logical_not(relayed(gy, back)))
                def _():
                    forward(back, dx).start()

                @pl.when(has_y(-outer))
                def _():
                    hand(back, dx).start()

        if p == 0:
            each(FAR, lambda i: remote(i).start())

        @pl.when(has_y(outer))
        def _():
            arrive(p, 4 + outer, 0, outer)

            @pl.when(relayed(gy + outer, p))
            def _():
                for dx in (-1, 1):

                    @pl.when(has_x(dx))
                    def _():
                        relay(p, dx).start()

    each(OTHERS, lambda i: remote(8 - i).wait_recv())
    staged[6].wait()
    staged[7].wait()
    staged[10].wait()

    @pl.when(has_y(-outer))
    def _():
        arrive_all(4 - outer, 0, -outer)

    for dx in (-1, 1):
        for dy in (-outer, outer):

            @pl.when(has_x(dx) & has_y(dy))
            def _():
                arrive_all(4 + 3 * dx + dy, dx, 0)

    total = jnp.zeros(own_ref.shape, jnp.float32)
    for k in range(wts.shape[0]):
        source = src[0, k]
        position = (source // ny - gx + 1) * 3 + (source % ny - gy + 1)
        position = jnp.clip(position, 0, 8)
        total += jnp.dot(ocn[position], wts[k], preferred_element_type=jnp.float32)
    own_ref[...] = total
    rest = jnp.zeros((out.shape[0] - members, total.shape[1]), jnp.float32)
    picked = lax.dot_general(
        out[...], split_rows(jnp.concatenate([total, rest], axis=0)), (((1,), (1,)), ((), ())),
        preferred_element_type=jnp.float32,
    )
    strip_ref[...] = picked[:, : out.shape[0]] + picked[:, out.shape[0] :]
    each(FAR + NEAR, lambda i: border(i).start())

    flat = meta[...].reshape(meta.shape[0] * meta.shape[1], meta.shape[2]).T
    cells = total.shape[1]
    staged[9].wait()
    for b in range(NB):
        for half, tiles in ((0, [4]), (1, OTHERS)):
            code = code_ref[0:1, half * cells : (half + 1) * cells]
            live = jnp.zeros((OB, cells), jnp.float32)
            error = live + 1.0
            value = live
            base = live + 1.0
            for i in tiles:
                dx, dy = OFFS[i]
                column = flat[b * OB : (b + 1) * OB, 8 * i : 8 * i + 4]
                hit = column[:, 0:1] + float((AX * dx + AX) * CODE + AY * dy + AY) == code
                live = jnp.where(hit, column[:, 3:4], live)
                error = jnp.where(hit, column[:, 2:3], error)
                value = jnp.where(hit, column[:, 1:2], value)
                base = jnp.where(hit, column[:, 2:3] + (1.0 - column[:, 3:4]), base)
            for n, table in enumerate((live, error, value, base)):
                obs_ref[b, n, :, half * cells : (half + 1) * cells] = table

    scale = 1.0 / (members - 1)
    gmean, own = moments(own_ref[...], members)
    own_ref[...] = own
    alpha, beta = strengths(own, gmean, [obs_ref[0, n, :, :cells] for n in range(4)], members)
    staged[11].wait()
    shifted[...] = shift(own, alpha, beta, near_ref[:cells, :])
    center = (alpha * scale, beta * scale)

    def one_field(v, carry):
        block = held[v]
        near = sources_of(shifted, members, around(scale, cells))
        total, mean = gather(block, [*near, (own_ref[...], *center)])
        part_ref[v] = block - total
        fmean[pl.ds(v, 1), :] = fmean[pl.ds(v, 1), :] + mean
        return carry

    lax.fori_loop(0, fields, one_field, 0)
    near = sources_of(shifted, members, around(scale, cells))
    total, mean = gather(own, [*near, (own, *center)])
    part_ref[fields] = own - total
    fmean[fields : fields + 1, :] = gmean + mean
    staged[12].wait()
    beyond_ref[...] = shift(own, alpha, beta, far_ref[:cells, :])

    for cond, copies in sends:

        @pl.when(cond)
        def _():
            for copy in copies:
                copy.wait_send()

    each(OTHERS, lambda i: remote(i).wait_send())
    staged[13].wait()
    each(OTHERS, lambda i: border(i).wait_send())
    each(OTHERS, lambda i: border(8 - i).wait_recv())


def analysis_kernel(
    own_ref, halo_ref, obs_ref, held_in, part_ref, fmean_ref, beyond_ref, code_ref, near_ref, far_ref, slot_ref,
    mean_out, anom_ref,
    held, mean_ref, inner, shifted, out_sem,
):
    fields, members, cells = held_in.shape
    scale = 1.0 / (members - 1)
    own = own_ref[...]
    hmean, halo = moments(halo_ref[...].T[:members], members)
    alpha, beta = strengths(halo, hmean, [obs_ref[0, n, :, cells:] for n in range(4)], members)
    inner[...] = shift(halo, alpha, beta, slot_ref[cells:, :])
    taps = [(code_ref[1 + n : 2 + n, :cells] * scale, cells) for n in range(SLOTS)]
    total, mean = gather(own, sources_of(inner, members, taps))
    block = part_ref[fields] - total
    gmean = fmean_ref[fields : fields + 1, :] + mean
    beyond = beyond_ref[...] + shift(halo, alpha, beta, far_ref[cells:, :])
    edges = sources_of(beyond, members, around(scale, cells))
    total, mean = gather(halo, [*edges, (halo, alpha * scale, beta * scale)])
    grid = jnp.concatenate([block, halo - total], axis=1)
    gmean = jnp.concatenate([gmean, hmean + mean], axis=1)

    alpha, beta = strengths(grid, gmean, [obs_ref[1, n] for n in range(4)], members)
    shifted[...] = shift(grid, alpha, beta, near_ref[...])
    held[fields] = block
    center = (alpha[:, :cells] * scale, beta[:, :cells] * scale)

    def save(v):
        return pltpu.make_async_copy(held.at[v], anom_ref.at[v], out_sem.at[v])

    def one_field(v, carry):
        total, before = gather(held_in[v], sources_of(inner, members, taps))
        block = part_ref[v] - total
        near = sources_of(shifted, members, around(scale, cells))
        total, mean = gather(block, [*near, (held[fields], *center)])
        held[v] = block - total
        mean_ref[v] = fmean_ref[pl.ds(v, 1), :] + before + mean
        save(v).start()
        return carry

    lax.fori_loop(0, fields, one_field, 0)
    near = sources_of(shifted, members, around(scale, cells))
    total, mean = gather(block, [*near, (block, *center)])
    mean_ref[fields] = gmean[:, :cells] + mean
    means = pltpu.make_async_copy(mean_ref, mean_out, out_sem.at[fields + 1])
    means.start()
    held[fields] = block - total
    save(fields).start()
    means.wait()
    for v in range(fields + 1):
        save(v).wait()


def local(
    atm_members, ocean_members, remap_weights, pair_src, obs_cell, obs_value, obs_error,
    obs_live, obs_order,
):
    members, fields, cells = atm_members.shape[2:]
    slots = obs_cell.shape[2]
    sources, depth = remap_weights.shape[2:4]
    vmem = pl.BlockSpec(memory_space=pltpu.VMEM)
    anywhere = pl.BlockSpec(memory_space=pl.ANY)
    code, near, far, slot, out = tables()
    results = (
        pltpu.VMEM((members, cells), jnp.float32),
        pltpu.VMEM((cells, 128), jnp.float32),
        pltpu.VMEM((NB, 4, OB, 2 * cells), jnp.float32),
        pltpu.VMEM((fields, members, cells), jnp.float32),
        pltpu.VMEM((fields + 1, members, cells), jnp.float32),
        pltpu.VMEM((16, cells), jnp.float32),
        pltpu.VMEM((members + 8, 8 * cells), jnp.float32),
        pltpu.VMEM(code.shape, jnp.float32),
        pltpu.VMEM(near.shape, jnp.bfloat16),
        pltpu.VMEM(far.shape, jnp.bfloat16),
        pltpu.VMEM(slot.shape, jnp.bfloat16),
    )
    state = pl.pallas_call(
        exchange_kernel,
        out_shape=results,
        in_specs=[anywhere] * 14,
        out_specs=(vmem,) * len(results),
        scratch_shapes=[
            pltpu.VMEM((9, members, depth), jnp.bfloat16),
            pltpu.VMEM((sources, depth, cells), jnp.bfloat16),
            pltpu.VMEM((16, 8, 128), jnp.float32),
            pltpu.SMEM((1, sources), jnp.int32),
            pltpu.VMEM((1, slots), jnp.int32),
            pltpu.VMEM((1, slots), jnp.int32),
            pltpu.VMEM((1, slots), jnp.int32),
            pltpu.VMEM((1, slots), jnp.float32),
            pltpu.VMEM((1, slots), jnp.float32),
            pltpu.VMEM(out.shape, jnp.bfloat16),
            pltpu.VMEM((cells, 128), jnp.float32),
            pltpu.VMEM((members + 8, 8 * cells), jnp.float32),
            pltpu.SemaphoreType.DMA((14,)),
            pltpu.SemaphoreType.DMA((10, members // PIECE)),
            pltpu.SemaphoreType.DMA((9, members // PIECE)),
            pltpu.SemaphoreType.DMA((4, 9)),
        ],
        compiler_params=pltpu.CompilerParams(
            collective_id=0, has_side_effects=True, vmem_limit_bytes=LIMIT
        ),
        name="exchange",
    )(
        *(
            pltpu.with_memory_space_constraint(x, pltpu.HBM)
            for x in (
                pair_src[0], obs_order[0], obs_cell[0], obs_live[0], obs_value[0], obs_error[0],
                ocean_members[0, 0], remap_weights[0, 0],
                jnp.transpose(atm_members[0, 0], (1, 0, 2)),
                jnp.asarray(code), *(jnp.asarray(x, jnp.bfloat16) for x in (near, far, slot, out)),
            )
        )
    )
    post_mean, post_anom = pl.pallas_call(
        analysis_kernel,
        out_shape=(
            jax.ShapeDtypeStruct((fields + 1, 1, cells), jnp.float32),
            jax.ShapeDtypeStruct((fields + 1, members, cells), jnp.float32),
        ),
        in_specs=[vmem] * len(results),
        out_specs=(anywhere, anywhere),
        scratch_shapes=[
            pltpu.VMEM((fields + 1, members, cells), jnp.float32),
            pltpu.VMEM((fields + 1, 1, cells), jnp.float32),
            pltpu.VMEM((members + 8, SLOTS * cells), jnp.float32),
            pltpu.VMEM((members + 8, 8 * cells), jnp.float32),
            pltpu.SemaphoreType.DMA((fields + 2,)),
        ],
        compiler_params=pltpu.CompilerParams(vmem_limit_bytes=LIMIT),
        name="analysis",
    )(*state)
    return (post_mean.reshape(1, 1, fields + 1, cells), jnp.transpose(post_anom, (1, 0, 2))[None, None])


def solution(mesh):
    in_specs = (
        P("gx", "gy", None, None, None),
        P("gx", "gy", None, None),
        P("gx", "gy", None, None, None),
        P("gx", "gy", None),
        P("gx", "gy", None),
        P("gx", "gy", None),
        P("gx", "gy", None),
        P("gx", "gy", None),
        P("gx", "gy", None),
    )
    out_specs = (P("gx", "gy", None, None), P("gx", "gy", None, None, None))
    return jax.shard_map(local, mesh=mesh, in_specs=in_specs, out_specs=out_specs, check_vma=False)
```

```python
import functools

import jax
import jax.numpy as jnp
import numpy as np
from jax import lax
from jax.experimental import pallas as pl
from jax.experimental.pallas import tpu as pltpu
from jax.sharding import PartitionSpec as P

AX = 8
AY = 16
OB = 32
NB = 2
RAD = 2
CODE = 64
LIMIT = 32 * 1024 * 1024

MESH = pl.DeviceIdType.MESH
OFFS = [(dx, dy) for dx in (-1, 0, 1) for dy in (-1, 0, 1)]
OTHERS = [i for i in range(9) if i != 4]
NEAR = [1, 3, 5, 7]
FAR = [0, 2, 6, 8]
PIECE = 16
SHARES = (3, 1, 4, 4, 4, 4, 1, 3)
STEPS = [(True, 4), (True, 3), (False, 0), (False, 1), (True, 2), (False, 2), (True, 1), (False, 3), (True, 0), (False, 4)]
SLOTS = 5


def taper_of(dx, dy):
    return max(1.0 - (dx * dx + dy * dy) / float(RAD * RAD), 0.0) ** 2


def edge(d, size):
    return {-1: range(RAD), 0: range(size), 1: range(size - RAD, size)}[d]


def strip(i):
    dx, dy = OFFS[i]
    return [(x, y) for x in edge(dx, AX) for y in edge(dy, AY)]


def strips():
    spans, at = {}, 0
    for i in OTHERS:
        rows = -(-len(strip(i)) // 8) * 8
        spans[i] = (at, rows)
        at += rows
    return spans


SPANS = strips()


@functools.lru_cache
def tables():
    cells = AX * AY
    where = {(c // AY, c % AY): c for c in range(cells)}
    out = np.zeros((cells, cells), np.float32)
    for i in OTHERS:
        dx, dy = OFFS[i]
        for n, (x, y) in enumerate(strip(i)):
            out[SPANS[i][0] + n, x * AY + y] = 1.0
        for n, (x, y) in enumerate(strip(8 - i)):
            where[(x + dx * AX, y + dy * AY)] = cells + SPANS[i][0] + n
    code = np.full((8, 2 * cells), -1.0, np.float32)
    code[1:, :] = 0.0
    move = np.zeros((2 * cells, 2, 8, cells), np.float32)
    slot = np.zeros((2 * cells, SLOTS, cells), np.float32)
    for (x, y), n in where.items():
        code[0, n] = (x + AX) * CODE + (y + AY)
        taken = 0
        for d, i in enumerate(OTHERS):
            dx, dy = OFFS[i]
            src = where.get((x + dx, y + dy))
            if src is not None:
                move[src, n // cells, d, n % cells] = 1.0
                if n < cells <= src:
                    slot[src, taken, n] = 1.0
                    code[1 + taken, n] = taper_of(dx, dy)
                    taken += 1
    own = move[:, 0].reshape(2 * cells, 8 * cells)
    far = move[:, 1].reshape(2 * cells, 8 * cells)
    slot = slot.reshape(2 * cells, SLOTS * cells)
    out = np.concatenate([out, np.zeros_like(out)], axis=0)
    return code, np.concatenate([own, far, slot, out], axis=1)


def split_rows(block):
    high = block.astype(jnp.bfloat16).astype(jnp.float32)
    return jnp.concatenate([high, block - high], axis=0).astype(jnp.bfloat16)


def moments(block, members):
    mean = jnp.sum(block, axis=0, keepdims=True) / members
    return mean, block - mean


def strengths(block, mean, table, members):
    variance = jnp.sum(block * block, axis=0, keepdims=True) / (members - 1)
    live, error, value, base = table
    denom = variance + base
    weighting = live / denom
    damping = 1.0 / (1.0 + jnp.sqrt(error / denom))
    alpha = jnp.sum(weighting * damping, axis=0, keepdims=True)
    beta = jnp.sum(weighting * value, axis=0, keepdims=True)
    return alpha, beta - mean * jnp.sum(weighting, axis=0, keepdims=True)


def shift(block, alpha, beta, tables):
    rest = jnp.zeros((6, block.shape[1]), jnp.float32)
    rows = block.shape[0] + 8
    left = split_rows(jnp.concatenate([block, alpha, beta, rest], axis=0))
    moved = jnp.dot(left, tables, preferred_element_type=jnp.float32)
    return moved[:rows] + moved[rows:]


def gather(block, sources):
    total = jnp.zeros_like(block)
    mean = jnp.zeros((1, block.shape[1]), jnp.float32)
    for source, a, m in sources:
        cov = jnp.sum(block * source, axis=0, keepdims=True)
        mean = mean + cov * m
        total = total + source * (cov * a)
    return total, mean


def sources_of(shifted, members, weights):
    cells = weights[0][1]
    found = []
    for d, (weight, width) in enumerate(weights):
        part = slice(d * cells, d * cells + width)
        found.append(
            (
                shifted[:members, part],
                shifted[members : members + 1, part] * weight,
                shifted[members + 1 : members + 2, part] * weight,
            )
        )
    return found


def around(scale, cells):
    return [(scale * taper_of(*OFFS[i]), cells) for i in OTHERS]


def exchange_kernel(
    src_ref, order_ref, cell_ref, live_ref, value_ref, error_ref, ocean_ref, weights_ref, atm_ref,
    code_in, table_in,
    own_ref, halo_ref, obs_ref, held, part_ref, fmean, beyond_ref, code_ref, table_ref,
    ocn, wts, meta, src, order_in, cell_in, live_in, value_in, error_in, strip_ref, shifted,
    local_sem, send_sem, recv_sem, note_sem,
):
    gx, gy = lax.axis_index("gx"), lax.axis_index("gy")
    nx, ny = lax.axis_size("gx"), lax.axis_size("gy")
    members = own_ref.shape[0]
    fields = atm_ref.shape[0]
    slots = order_in.shape[1]

    def has_x(dx):
        return (gx + dx >= 0) & (gx + dx < nx)

    def has_y(dy):
        return (gy + dy >= 0) & (gy + dy < ny)

    def there(i):
        return has_x(OFFS[i][0]) & has_y(OFFS[i][1])

    pairs = (
        (ocean_ref, ocn.at[4]), (order_ref, order_in), (cell_ref, cell_in), (live_ref, live_in),
        (value_ref, value_in), (error_ref, error_in), (src_ref, src), (weights_ref, wts),
        (atm_ref, held), (code_in, code_ref), (table_in, table_ref),
    )
    staged = [pltpu.make_async_copy(x, y, local_sem.at[n]) for n, (x, y) in enumerate(pairs)]
    for copy in staged:
        copy.start()

    barrier = pltpu.get_barrier_semaphore()
    for i in NEAR:
        dx, dy = OFFS[i]

        @pl.when(there(i))
        def _():
            pl.semaphore_signal(barrier, inc=1, device_id=(gx + dx, gy + dy), device_id_type=MESH)

    for i in OTHERS:

        @pl.when(jnp.logical_not(there(i)))
        def _():
            at, rows = SPANS[i]
            halo_ref[at : at + rows, :] = jnp.zeros((rows, halo_ref.shape[1]), jnp.float32)
            meta[i] = jnp.zeros(meta.shape[1:], jnp.float32)

    for n in range(9, meta.shape[0]):
        meta[n] = jnp.zeros(meta.shape[1:], jnp.float32)

    for copy in staged[1:6]:
        copy.wait()
    cell = cell_in[...]
    spot = ((cell // AY) * CODE + cell % AY).astype(jnp.float32)
    rows = jnp.concatenate(
        [
            spot, value_in[...], error_in[...], live_in[...].astype(jnp.float32),
            jnp.zeros((4, slots), jnp.float32),
        ],
        axis=0,
    )
    slot = lax.broadcasted_iota(jnp.int32, (slots, slots), 0)
    perm = jnp.where(order_in[...] == slot, 1.0, 0.0)
    rows = jnp.dot(rows, perm, precision=lax.Precision.HIGHEST, preferred_element_type=jnp.float32)
    meta[4] = jnp.concatenate([rows, jnp.zeros((8, meta.shape[2] - slots), jnp.float32)], axis=1)

    staged[0].wait()
    pl.semaphore_wait(barrier, sum(there(i).astype(jnp.int32) for i in NEAR))

    outer = lax.rem(gy, 2) * 2 - 1
    count = members // PIECE

    def among(y, wanted):
        at = lax.rem(y + 8, 8)
        return sum((at == n).astype(jnp.int32) for n, share in enumerate(SHARES) if wanted(share)) > 0

    def relayed(y, p):
        return among(y, lambda share: p < share)

    def ocean(low, rows, source, target, kind, index, dx, dy):
        return pltpu.make_async_remote_copy(
            src_ref=ocn.at[source, pl.ds(low, rows)],
            dst_ref=ocn.at[target, pl.ds(low, rows)],
            send_sem=send_sem.at[kind],
            recv_sem=recv_sem.at[index],
            device_id=(gx + dx, gy + dy),
            device_id_type=MESH,
        )

    def piece(p, *where):
        return ocean(p * PIECE, PIECE, *where)

    def arrive(at, index, dx, dy, low=0, rows=members):
        ocean(low, rows, at, at, 0, index, dx, dy).wait_recv()

    def sent(rows, kind, dx, dy):
        ocean(0, rows, 4, 4, kind, 0, dx, dy).wait_send()

    order = range(count)

    def start(cond, copies):
        @pl.when(cond)
        def _():
            for copy in copies:
                copy.start()

    def from_side(dx):
        return count * (dx > 0)

    beside, inside = 2 * count, 3 * count

    def corner(dx, inner):
        return inside + 1 + 2 * (dx > 0) + inner

    start(has_y(outer), [piece(p, 4, 4 - outer, 0, beside + p, 0, outer) for p in order])
    for dx in (-1, 1):
        start(
            has_x(dx),
            [piece(p, 4, 4 - 3 * dx, 2 + (dx > 0), from_side(-dx) + p, dx, 0) for p in reversed(order)],
        )
    start(has_y(-outer), [piece(p, 4, 4 + outer, 1, inside, 0, -outer) for p in order])

    def relay(p, dx):
        return piece(p, 4 + outer, 4 - 3 * dx + outer, 4 + (dx > 0), corner(-dx, 0), dx, 0)

    def forward(p, dx):
        return piece(p, 4 + 3 * dx, 4 + 3 * dx - outer, 6 + (dx > 0), corner(dx, 0), 0, outer)

    def hand(p, dx):
        return piece(p, 4 + 3 * dx, 4 + 3 * dx + outer, 8 + (dx > 0), corner(dx, 1), 0, -outer)

    def all_sent():
        @pl.when(has_y(outer))
        def _():
            sent(members, 0, 0, outer)

        @pl.when(has_y(-outer))
        def _():
            sent(members, 1, 0, -outer)

        for dx in (-1, 1):

            @pl.when(has_x(dx))
            def _():
                sent(members, 2 + (dx > 0), dx, 0)

            @pl.when(has_x(dx) & has_y(-outer))
            def _():
                sent(members, 8 + (dx > 0), 0, -outer)

            for n in sorted(set(SHARES)):

                @pl.when(has_x(dx) & has_y(outer) & among(gy + outer, lambda share: share == n))
                def _():
                    if n:
                        sent(n * PIECE, 4 + (dx > 0), dx, 0)

                @pl.when(has_x(dx) & has_y(outer) & among(gy, lambda share: share == n))
                def _():
                    if n < count:
                        sent((count - n) * PIECE, 6 + (dx > 0), 0, outer)

    def remote(i):
        dx, dy = OFFS[i]
        return pltpu.make_async_remote_copy(
            src_ref=meta.at[4],
            dst_ref=meta.at[8 - i],
            send_sem=note_sem.at[0],
            recv_sem=note_sem.at[1],
            device_id=(gx + dx, gy + dy),
            device_id_type=MESH,
        )

    def border(i):
        dx, dy = OFFS[i]
        (source, rows), (target, _) = SPANS[i], SPANS[8 - i]
        return pltpu.make_async_remote_copy(
            src_ref=strip_ref.at[pl.ds(source, rows)],
            dst_ref=halo_ref.at[pl.ds(target, rows)],
            send_sem=note_sem.at[2],
            recv_sem=note_sem.at[3],
            device_id=(gx + dx, gy + dy),
            device_id_type=MESH,
        )

    beside_x = has_x(-1).astype(jnp.int32) + has_x(1).astype(jnp.int32)
    beside_y = has_y(-1).astype(jnp.int32) + has_y(1).astype(jnp.int32)

    def all_of(act):
        for nx_ in range(3):
            for ny_ in range(3):
                if nx_ + ny_:

                    @pl.when((beside_x == nx_) & (beside_y == ny_))
                    def _():
                        act(nx_, ny_)

    def whole_notes(nx_, ny_):
        n = (nx_ + 1) * (ny_ + 1) - 1
        return pltpu.make_async_remote_copy(
            src_ref=meta.at[pl.ds(0, n)], dst_ref=meta.at[pl.ds(0, n)],
            send_sem=note_sem.at[0], recv_sem=note_sem.at[1],
            device_id=(gx, gy + outer), device_id_type=MESH,
        )

    def whole_border(nx_, ny_):
        rows = nx_ * SPANS[1][1] + ny_ * SPANS[3][1] + nx_ * ny_ * SPANS[0][1]
        return pltpu.make_async_remote_copy(
            src_ref=strip_ref.at[pl.ds(0, rows)], dst_ref=halo_ref.at[pl.ds(0, rows)],
            send_sem=note_sem.at[2], recv_sem=note_sem.at[3],
            device_id=(gx, gy + outer), device_id_type=MESH,
        )

    def each(which, act):
        for i in which:

            @pl.when(there(i))
            def _():
                act(i)

    each(NEAR, lambda i: remote(i).start())

    staged[8].wait()
    for v in range(fields):
        block = held[v]
        mean = jnp.sum(block, axis=0, keepdims=True) / members
        fmean[v : v + 1, :] = mean
        held[v] = block - mean

    def from_x(p):
        for dx in (-1, 1):

            @pl.when(has_x(dx))
            def _():
                arrive(4 + 3 * dx, from_side(dx) + p, dx, 0, p * PIECE, PIECE)

                @pl.when(has_y(outer) & jnp.logical_not(relayed(gy, p)))
                def _():
                    forward(p, dx).start()

                @pl.when(has_y(-outer))
                def _():
                    hand(p, dx).start()

    def from_y(p):
        @pl.when(has_y(outer))
        def _():
            arrive(4 + outer, beside + p, 0, outer, p * PIECE, PIECE)

            @pl.when(relayed(gy + outer, p))
            def _():
                for dx in (-1, 1):

                    @pl.when(has_x(dx))
                    def _():
                        relay(p, dx).start()

    for n, (over_x, p) in enumerate(STEPS):
        (from_x if over_x else from_y)(p)
        if n == 0:
            each(FAR, lambda i: remote(i).start())

    staged[6].wait()
    staged[7].wait()
    staged[10].wait()

    @pl.when(has_y(-outer))
    def _():
        arrive(4 - outer, inside, 0, -outer)

    for inner, dy in ((1, -outer), (0, outer)):
        for dx in (-1, 1):

            @pl.when(has_x(dx) & has_y(dy))
            def _():
                arrive(4 + 3 * dx + dy, corner(dx, inner), dx, 0)

    total = jnp.zeros(own_ref.shape, jnp.float32)
    for k in range(wts.shape[0]):
        source = src[0, k]
        position = (source // ny - gx + 1) * 3 + (source % ny - gy + 1)
        position = jnp.clip(position, 0, 8)
        total += jnp.dot(ocn[position], wts[k], preferred_element_type=jnp.float32)
    own_ref[...] = total
    width = strip_ref.shape[0]
    near, far = slice(0, 8 * width), slice(8 * width, 16 * width)
    rest = jnp.zeros((width - members, total.shape[1]), jnp.float32)
    picked = lax.dot_general(
        table_ref[:width, (16 + SLOTS) * width :], split_rows(jnp.concatenate([total, rest], axis=0)), (((1,), (1,)), ((), ())),
        preferred_element_type=jnp.float32,
    )
    strip_ref[...] = picked[:, :width] + picked[:, width:]
    each(FAR + NEAR, lambda i: border(i).start())

    all_of(lambda *n: whole_notes(*n).wait_recv())
    flat = meta[...].reshape(meta.shape[0] * meta.shape[1], meta.shape[2]).T
    cells = total.shape[1]
    staged[9].wait()
    for b in range(NB):
        for half, tiles in ((0, [4]), (1, OTHERS)):
            code = code_ref[0:1, half * cells : (half + 1) * cells]
            live = jnp.zeros((OB, cells), jnp.float32)
            error = live + 1.0
            value = live
            base = live + 1.0
            for i in tiles:
                dx, dy = OFFS[i]
                column = flat[b * OB : (b + 1) * OB, 8 * i : 8 * i + 4]
                hit = column[:, 0:1] + float((AX * dx + AX) * CODE + AY * dy + AY) == code
                live = jnp.where(hit, column[:, 3:4], live)
                error = jnp.where(hit, column[:, 2:3], error)
                value = jnp.where(hit, column[:, 1:2], value)
                base = jnp.where(hit, column[:, 2:3] + (1.0 - column[:, 3:4]), base)
            for n, table in enumerate((live, error, value, base)):
                obs_ref[b, n, :, half * cells : (half + 1) * cells] = table

    scale = 1.0 / (members - 1)
    gmean, own = moments(own_ref[...], members)
    own_ref[...] = own
    alpha, beta = strengths(own, gmean, [obs_ref[0, n, :, :cells] for n in range(4)], members)
    shifted[...] = shift(own, alpha, beta, table_ref[:cells, near])
    center = (alpha * scale, beta * scale)

    def one_field(v, carry):
        block = held[v]
        found = sources_of(shifted, members, around(scale, cells))
        total, mean = gather(block, [*found, (own_ref[...], *center)])
        part_ref[v] = block - total
        fmean[pl.ds(v, 1), :] = fmean[pl.ds(v, 1), :] + mean
        return carry

    lax.fori_loop(0, fields, one_field, 0)
    found = sources_of(shifted, members, around(scale, cells))
    total, mean = gather(own, [*found, (own, *center)])
    part_ref[fields] = own - total
    fmean[fields : fields + 1, :] = gmean + mean
    beyond_ref[...] = shift(own, alpha, beta, table_ref[:cells, far])

    all_sent()
    all_of(lambda *n: whole_notes(*n).wait_send())
    all_of(lambda *n: whole_border(*n).wait_send())
    all_of(lambda *n: whole_border(*n).wait_recv())


def analysis_kernel(
    own_ref, halo_ref, obs_ref, held_in, part_ref, fmean_ref, beyond_ref, code_ref, table_ref,
    mean_out, anom_ref,
    held, mean_ref, inner, shifted, out_sem,
):
    fields, members, cells = held_in.shape
    scale = 1.0 / (members - 1)
    own = own_ref[...]
    hmean, halo = moments(halo_ref[...].T[:members], members)
    alpha, beta = strengths(halo, hmean, [obs_ref[0, n, :, cells:] for n in range(4)], members)
    inner[...] = shift(halo, alpha, beta, table_ref[cells:, 16 * cells : (16 + SLOTS) * cells])
    taps = [(code_ref[1 + n : 2 + n, :cells] * scale, cells) for n in range(SLOTS)]
    total, mean = gather(own, sources_of(inner, members, taps))
    block = part_ref[fields] - total
    gmean = fmean_ref[fields : fields + 1, :] + mean
    beyond = beyond_ref[...] + shift(halo, alpha, beta, table_ref[cells:, 8 * cells : 16 * cells])
    edges = sources_of(beyond, members, around(scale, cells))
    total, mean = gather(halo, [*edges, (halo, alpha * scale, beta * scale)])
    grid = jnp.concatenate([block, halo - total], axis=1)
    gmean = jnp.concatenate([gmean, hmean + mean], axis=1)

    alpha, beta = strengths(grid, gmean, [obs_ref[1, n] for n in range(4)], members)
    shifted[...] = shift(grid, alpha, beta, table_ref[:, : 8 * cells])
    held[fields] = block
    center = (alpha[:, :cells] * scale, beta[:, :cells] * scale)

    def save(v):
        return pltpu.make_async_copy(held.at[v], anom_ref.at[v], out_sem.at[0])

    def one_field(v, carry):
        total, before = gather(held_in[v], sources_of(inner, members, taps))
        block = part_ref[v] - total
        near = sources_of(shifted, members, around(scale, cells))
        total, mean = gather(block, [*near, (held[fields], *center)])
        held[v] = block - total
        mean_ref[v] = fmean_ref[pl.ds(v, 1), :] + before + mean
        save(v).start()
        return carry

    lax.fori_loop(0, fields, one_field, 0)
    near = sources_of(shifted, members, around(scale, cells))
    total, mean = gather(block, [*near, (block, *center)])
    mean_ref[fields] = gmean[:, :cells] + mean
    means = pltpu.make_async_copy(mean_ref, mean_out, out_sem.at[1])
    means.start()
    held[fields] = block - total
    save(fields).start()
    means.wait()
    pltpu.make_async_copy(held, anom_ref, out_sem.at[0]).wait()


def local(
    atm_members, ocean_members, remap_weights, pair_src, obs_cell, obs_value, obs_error,
    obs_live, obs_order,
):
    members, fields, cells = atm_members.shape[2:]
    slots = obs_cell.shape[2]
    sources, depth = remap_weights.shape[2:4]
    vmem = pl.BlockSpec(memory_space=pltpu.VMEM)
    anywhere = pl.BlockSpec(memory_space=pl.ANY)
    code, table = tables()
    results = (
        pltpu.VMEM((members, cells), jnp.float32),
        pltpu.VMEM((cells, 128), jnp.float32),
        pltpu.VMEM((NB, 4, OB, 2 * cells), jnp.float32),
        pltpu.VMEM((fields, members, cells), jnp.float32),
        pltpu.VMEM((fields + 1, members, cells), jnp.float32),
        pltpu.VMEM((16, cells), jnp.float32),
        pltpu.VMEM((members + 8, 8 * cells), jnp.float32),
        pltpu.VMEM(code.shape, jnp.float32),
        pltpu.VMEM(table.shape, jnp.bfloat16),
    )
    state = pl.pallas_call(
        exchange_kernel,
        out_shape=results,
        in_specs=[anywhere] * 11,
        out_specs=(vmem,) * len(results),
        scratch_shapes=[
            pltpu.VMEM((9, members, depth), jnp.bfloat16),
            pltpu.VMEM((sources, depth, cells), jnp.bfloat16),
            pltpu.VMEM((16, 8, 128), jnp.float32),
            pltpu.SMEM((1, sources), jnp.int32),
            pltpu.VMEM((1, slots), jnp.int32),
            pltpu.VMEM((1, slots), jnp.int32),
            pltpu.VMEM((1, slots), jnp.int32),
            pltpu.VMEM((1, slots), jnp.float32),
            pltpu.VMEM((1, slots), jnp.float32),
            pltpu.VMEM((cells, 128), jnp.float32),
            pltpu.VMEM((members + 8, 8 * cells), jnp.float32),
            pltpu.SemaphoreType.DMA((11,)),
            pltpu.SemaphoreType.DMA((10,)),
            pltpu.SemaphoreType.DMA((3 * (members // PIECE) + 5,)),
            pltpu.SemaphoreType.DMA((4,)),
        ],
        compiler_params=pltpu.CompilerParams(
            collective_id=0, has_side_effects=True, vmem_limit_bytes=LIMIT
        ),
        name="exchange",
    )(
        *(
            pltpu.with_memory_space_constraint(x, pltpu.HBM)
            for x in (
                pair_src[0], obs_order[0], obs_cell[0], obs_live[0], obs_value[0], obs_error[0],
                ocean_members[0, 0], remap_weights[0, 0],
                jnp.transpose(atm_members[0, 0], (1, 0, 2)),
                jnp.asarray(code), jnp.asarray(table, jnp.bfloat16),
            )
        )
    )
    post_mean, post_anom = pl.pallas_call(
        analysis_kernel,
        out_shape=(
            jax.ShapeDtypeStruct((fields + 1, 1, cells), jnp.float32),
            jax.ShapeDtypeStruct((fields + 1, members, cells), jnp.float32),
        ),
        in_specs=[vmem] * len(results),
        out_specs=(anywhere, anywhere),
        scratch_shapes=[
            pltpu.VMEM((fields + 1, members, cells), jnp.float32),
            pltpu.VMEM((fields + 1, 1, cells), jnp.float32),
            pltpu.VMEM((members + 8, SLOTS * cells), jnp.float32),
            pltpu.VMEM((members + 8, 8 * cells), jnp.float32),
            pltpu.SemaphoreType.DMA((2,)),
        ],
        compiler_params=pltpu.CompilerParams(vmem_limit_bytes=LIMIT),
        name="analysis",
    )(*state)
    return (post_mean.reshape(1, 1, fields + 1, cells), jnp.transpose(post_anom, (1, 0, 2))[None, None])


def solution(mesh):
    in_specs = (
        P("gx", "gy", None, None, None),
        P("gx", "gy", None, None),
        P("gx", "gy", None, None, None),
        P("gx", "gy", None),
        P("gx", "gy", None),
        P("gx", "gy", None),
        P("gx", "gy", None),
        P("gx", "gy", None),
        P("gx", "gy", None),
    )
    out_specs = (P("gx", "gy", None, None), P("gx", "gy", None, None, None))
    return jax.shard_map(local, mesh=mesh, in_specs=in_specs, out_specs=out_specs, check_vma=False)
```

```python
import functools

import jax
import jax.numpy as jnp
import numpy as np
from jax import lax
from jax.experimental import pallas as pl
from jax.experimental.pallas import tpu as pltpu
from jax.sharding import PartitionSpec as P

AX = 8
AY = 16
OB = 32
NB = 2
RAD = 2
CODE = 64
LIMIT = 32 * 1024 * 1024

MESH = pl.DeviceIdType.MESH
OFFS = [(dx, dy) for dx in (-1, 0, 1) for dy in (-1, 0, 1)]
OTHERS = [i for i in range(9) if i != 4]
NEAR = [1, 3, 5, 7]
FAR = [0, 2, 6, 8]
PIECE = 16
SHARES = (3, 1, 3, 4, 4, 3, 1, 3)
EVEN = [(False, 0), (False, 1), (True, 4), (False, 2), (True, 3), (True, 2), (False, 3), (True, 1), (True, 0), (False, 4)]
ODD = [(True, 4), (True, 3), (False, 0), (True, 2), (False, 1), (True, 1), (False, 2), (True, 0), (False, 3), (False, 4)]
SLOTS = 5


def taper_of(dx, dy):
    return max(1.0 - (dx * dx + dy * dy) / float(RAD * RAD), 0.0) ** 2


def edge(d, size):
    return {-1: range(RAD), 0: range(size), 1: range(size - RAD, size)}[d]


def strip(i):
    dx, dy = OFFS[i]
    return [(x, y) for x in edge(dx, AX) for y in edge(dy, AY)]


def strips():
    spans, at = {}, 0
    for i in OTHERS:
        rows = -(-len(strip(i)) // 8) * 8
        spans[i] = (at, rows)
        at += rows
    return spans


SPANS = strips()


@functools.lru_cache
def tables():
    cells = AX * AY
    where = {(c // AY, c % AY): c for c in range(cells)}
    out = np.zeros((cells, cells), np.float32)
    for i in OTHERS:
        dx, dy = OFFS[i]
        for n, (x, y) in enumerate(strip(i)):
            out[SPANS[i][0] + n, x * AY + y] = 1.0
        for n, (x, y) in enumerate(strip(8 - i)):
            where[(x + dx * AX, y + dy * AY)] = cells + SPANS[i][0] + n
    code = np.zeros((2 * cells, 2 * cells), np.float32)
    code[:2, :] = -1.0
    move = np.zeros((2 * cells, 2, 8, cells), np.float32)
    slot = np.zeros((2 * cells, SLOTS, cells), np.float32)
    for (x, y), n in where.items():
        code[0, n], code[1, n] = x + AX, y + AY
        taken = 0
        for d, i in enumerate(OTHERS):
            dx, dy = OFFS[i]
            src = where.get((x + dx, y + dy))
            if src is not None:
                move[src, n // cells, d, n % cells] = 1.0
                if n < cells <= src:
                    slot[src, taken, n] = 1.0
                    code[2 + taken, n] = taper_of(dx, dy)
                    taken += 1
    own = move[:, 0].reshape(2 * cells, 8 * cells)
    far = move[:, 1].reshape(2 * cells, 8 * cells)
    slot = slot.reshape(2 * cells, SLOTS * cells)
    out = np.concatenate([out, np.zeros_like(out)], axis=0)
    return np.concatenate([own, far, slot, out, code], axis=1)


def split_rows(block):
    high = block.astype(jnp.bfloat16).astype(jnp.float32)
    return jnp.concatenate([high, block - high], axis=0).astype(jnp.bfloat16)


def moments(block, members):
    mean = jnp.sum(block, axis=0, keepdims=True) / members
    return mean, block - mean


def strengths(block, mean, table, members):
    variance = jnp.sum(block * block, axis=0, keepdims=True) / (members - 1)
    live, error, value, base = table
    denom = variance + base
    weighting = live / denom
    damping = 1.0 / (1.0 + jnp.sqrt(error / denom))
    alpha = jnp.sum(weighting * damping, axis=0, keepdims=True)
    beta = jnp.sum(weighting * value, axis=0, keepdims=True)
    return alpha, beta - mean * jnp.sum(weighting, axis=0, keepdims=True)


def shift(block, alpha, beta, tables):
    rest = jnp.zeros((6, block.shape[1]), jnp.float32)
    rows = block.shape[0] + 8
    left = split_rows(jnp.concatenate([block, alpha, beta, rest], axis=0))
    moved = jnp.dot(left, tables, preferred_element_type=jnp.float32)
    return moved[:rows] + moved[rows:]


def gather(block, sources):
    total = jnp.zeros_like(block)
    mean = jnp.zeros((1, block.shape[1]), jnp.float32)
    for source, a, m in sources:
        cov = jnp.sum(block * source, axis=0, keepdims=True)
        mean = mean + cov * m
        total = total + source * (cov * a)
    return total, mean


def sources_of(shifted, members, weights):
    cells = weights[0][1]
    found = []
    for d, (weight, width) in enumerate(weights):
        part = slice(d * cells, d * cells + width)
        found.append(
            (
                shifted[:members, part],
                shifted[members : members + 1, part] * weight,
                shifted[members + 1 : members + 2, part] * weight,
            )
        )
    return found


def around(scale, cells):
    return [(scale * taper_of(*OFFS[i]), cells) for i in OTHERS]


def exchange_kernel(
    src_ref, order_ref, cell_ref, live_ref, value_ref, error_ref, ocean_ref, weights_ref, atm_ref,
    table_in,
    own_ref, halo_ref, obs_ref, held, part_ref, fmean, beyond_ref, table_ref,
    ocn, late, wts, meta, src, ints, floats, strip_ref, shifted,
    local_sem, send_sem, recv_sem, note_sem,
):
    gx, gy = lax.axis_index("gx"), lax.axis_index("gy")
    nx, ny = lax.axis_size("gx"), lax.axis_size("gy")
    members = own_ref.shape[0]
    fields = atm_ref.shape[0]
    slots = ints.shape[2]

    def has_x(dx):
        return (gx + dx >= 0) & (gx + dx < nx)

    def has_y(dy):
        return (gy + dy >= 0) & (gy + dy < ny)

    def there(i):
        return has_x(OFFS[i][0]) & has_y(OFFS[i][1])

    depth = wts.shape[0] - 1
    pairs = (
        (ocean_ref, ocn.at[4], 0), (order_ref, ints.at[0], 1), (cell_ref, ints.at[1], 1),
        (live_ref, ints.at[2], 1), (value_ref, floats.at[0], 2), (error_ref, floats.at[1], 2),
        (src_ref, src, 3), (weights_ref, wts.at[0:depth], 4), (atm_ref, held, 5),
        (table_in, table_ref, 6),
    )
    staged = [pltpu.make_async_copy(x, y, local_sem.at[n]) for x, y, n in pairs]
    outer = lax.rem(gy, 2) * 2 - 1
    for copy in staged:
        copy.start()

    barrier = pltpu.get_barrier_semaphore()
    for i in NEAR:
        dx, dy = OFFS[i]

        @pl.when(there(i))
        def _():
            pl.semaphore_signal(barrier, inc=1, device_id=(gx + dx, gy + dy), device_id_type=MESH)

    for i in OTHERS:

        @pl.when(jnp.logical_not(there(i)))
        def _():
            at, rows = SPANS[i]
            halo_ref[at : at + rows, :] = jnp.zeros((rows, halo_ref.shape[1]), jnp.float32)
            meta[i] = jnp.zeros(meta.shape[1:], jnp.float32)

    for dx in (-1, 1):
        ocn[4 + 3 * dx + outer] = jnp.zeros(ocn.shape[1:], ocn.dtype)

        @pl.when(jnp.logical_not(has_x(dx) & has_y(outer)))
        def _():
            late[int(dx > 0)] = jnp.zeros(late.shape[1:], late.dtype)

    wts[depth] = jnp.zeros(wts.shape[1:], wts.dtype)
    for n in range(9, meta.shape[0]):
        meta[n] = jnp.zeros(meta.shape[1:], jnp.float32)

    staged[0].wait()
    pl.semaphore_wait(barrier, sum(there(i).astype(jnp.int32) for i in NEAR))

    count = members // PIECE

    def among(y, wanted):
        at = lax.rem(y + 8, 8)
        return sum((at == n).astype(jnp.int32) for n, share in enumerate(SHARES) if wanted(share)) > 0

    def relayed(y, p):
        return among(y, lambda share: p < share)

    def ocean(low, rows, source, target, kind, index, dx, dy):
        return pltpu.make_async_remote_copy(
            src_ref=ocn.at[source, pl.ds(low, rows)],
            dst_ref=target.at[pl.ds(low, rows)],
            send_sem=send_sem.at[0],
            recv_sem=recv_sem.at[index],
            device_id=(gx + dx, gy + dy),
            device_id_type=MESH,
        )

    def piece(p, source, target, kind, index, dx, dy):
        return ocean(p * PIECE, PIECE, source, target, kind, index, dx, dy)

    def arrive(at, index, dx, dy, p):
        ocean(p * PIECE, PIECE, at, ocn.at[at], 0, index, dx, dy).wait_recv()

    def sent(rows, kind, dx, dy):
        ocean(0, rows, 4, ocn.at[4], kind, 0, dx, dy).wait_send()

    def whole(blocks, index, dx, dy):
        pltpu.make_async_remote_copy(
            src_ref=ocn.at[pl.ds(0, blocks)],
            dst_ref=ocn.at[pl.ds(0, blocks)],
            send_sem=send_sem.at[0],
            recv_sem=recv_sem.at[index],
            device_id=(gx + dx, gy + dy),
            device_id_type=MESH,
        ).wait_recv()

    order = range(count)

    def start(cond, copies):
        @pl.when(cond)
        def _():
            for copy in copies:
                copy.start()

    def from_side(dx):
        return count * (dx > 0)

    beside, inside = 2 * count, 3 * count

    mine = lax.rem(gy, 8)
    yields = (mine == 2) | (mine == 5)
    to_outer = [piece(p, 4, ocn.at[4 - outer], 0, beside + p, 0, outer) for p in order]
    start(has_y(outer) & jnp.logical_not(yields), to_outer)
    for dx in (-1, 1):
        start(
            has_x(dx),
            [
                piece(p, 4, ocn.at[4 - 3 * dx], 2 + (dx > 0), from_side(-dx) + p, dx, 0)
                for p in reversed(order)
            ],
        )
    start(has_y(-outer), [ocean(0, members, 4, ocn.at[4 + outer], 1, inside, 0, -outer)])

    def relay(p, dx):
        return piece(p, 4 + outer, late.at[int(dx < 0)], 4 + (dx > 0), inside + 1, dx, 0)

    def forward(p, dx):
        return piece(p, 4 + 3 * dx, late.at[int(dx > 0)], 6 + (dx > 0), inside + 1, 0, outer)

    def hand(p, dx):
        return piece(p, 4 + 3 * dx, ocn.at[4 + 3 * dx + outer], 8 + (dx > 0), inside, 0, -outer)

    def all_sent():
        @pl.when(has_y(outer))
        def _():
            sent(members, 0, 0, outer)

        @pl.when(has_y(-outer))
        def _():
            sent(members, 1, 0, -outer)

        for dx in (-1, 1):

            @pl.when(has_x(dx))
            def _():
                sent(members, 2 + (dx > 0), dx, 0)

            @pl.when(has_x(dx) & has_y(-outer))
            def _():
                sent(members, 8 + (dx > 0), 0, -outer)

            for n in sorted(set(SHARES)):

                @pl.when(has_x(dx) & has_y(outer) & among(gy + outer, lambda share: share == n))
                def _():
                    if n:
                        sent(n * PIECE, 4 + (dx > 0), dx, 0)

                @pl.when(has_x(dx) & has_y(outer) & among(gy, lambda share: share == n))
                def _():
                    if n < count:
                        sent((count - n) * PIECE, 6 + (dx > 0), 0, outer)

    beside_x = has_x(-1).astype(jnp.int32) + has_x(1).astype(jnp.int32)
    beside_y = has_y(-1).astype(jnp.int32) + has_y(1).astype(jnp.int32)

    def remote(i):
        dx, dy = OFFS[i]
        return pltpu.make_async_remote_copy(
            src_ref=meta.at[4],
            dst_ref=meta.at[8 - i],
            send_sem=send_sem.at[0],
            recv_sem=note_sem.at[0],
            device_id=(gx + dx, gy + dy),
            device_id_type=MESH,
        )

    def border(i):
        dx, dy = OFFS[i]
        (source, rows), (target, _) = SPANS[i], SPANS[8 - i]
        return pltpu.make_async_remote_copy(
            src_ref=strip_ref.at[pl.ds(source, rows)],
            dst_ref=halo_ref.at[pl.ds(target, rows)],
            send_sem=send_sem.at[0],
            recv_sem=note_sem.at[1],
            device_id=(gx + dx, gy + dy),
            device_id_type=MESH,
        )

    def all_of(act):
        for nx_ in range(3):
            for ny_ in range(3):
                if nx_ + ny_:

                    @pl.when((beside_x == nx_) & (beside_y == ny_))
                    def _():
                        act(nx_, ny_)

    def whole_notes(nx_, ny_):
        n = (nx_ + 1) * (ny_ + 1) - 1
        return pltpu.make_async_remote_copy(
            src_ref=meta.at[pl.ds(0, n)], dst_ref=meta.at[pl.ds(0, n)],
            send_sem=send_sem.at[0], recv_sem=note_sem.at[0],
            device_id=(gx, gy + outer), device_id_type=MESH,
        )

    def whole_border(nx_, ny_):
        rows = nx_ * SPANS[1][1] + ny_ * SPANS[3][1] + nx_ * ny_ * SPANS[0][1]
        return pltpu.make_async_remote_copy(
            src_ref=strip_ref.at[pl.ds(0, rows)], dst_ref=halo_ref.at[pl.ds(0, rows)],
            send_sem=send_sem.at[0], recv_sem=note_sem.at[1],
            device_id=(gx, gy + outer), device_id_type=MESH,
        )

    def each(which, act):
        for i in which:

            @pl.when(there(i))
            def _():
                act(i)

    pltpu.make_async_copy(ints, ints, local_sem.at[1]).wait()
    pltpu.make_async_copy(floats, floats, local_sem.at[2]).wait()
    cell = ints[1]
    spot = ((cell // AY) * CODE + cell % AY).astype(jnp.float32)
    rows = jnp.concatenate(
        [
            spot, floats[0], floats[1], ints[2].astype(jnp.float32),
            jnp.zeros((4, slots), jnp.float32),
        ],
        axis=0,
    )
    slot = lax.broadcasted_iota(jnp.int32, (slots, slots), 0)
    perm = jnp.where(ints[0] == slot, 1.0, 0.0)
    rows = jnp.dot(rows, perm, precision=lax.Precision.HIGHEST, preferred_element_type=jnp.float32)
    meta[4] = jnp.concatenate([rows, jnp.zeros((8, meta.shape[2] - slots), jnp.float32)], axis=1)

    each(NEAR, lambda i: remote(i).start())

    staged[8].wait()
    for v in range(fields):
        block = held[v]
        mean = jnp.sum(block, axis=0, keepdims=True) / members
        fmean[v : v + 1, :] = mean
        held[v] = block - mean

    start(has_y(outer) & yields, to_outer)

    def from_x(p):
        for dx in (-1, 1):

            @pl.when(has_x(dx))
            def _():
                arrive(4 + 3 * dx, from_side(dx) + p, dx, 0, p)

                @pl.when(has_y(outer) & jnp.logical_not(relayed(gy, p)))
                def _():
                    forward(p, dx).start()

                @pl.when(has_y(-outer))
                def _():
                    hand(p, dx).start()

    def from_y(p):
        @pl.when(has_y(outer))
        def _():
            arrive(4 + outer, beside + p, 0, outer, p)

            @pl.when(relayed(gy + outer, p))
            def _():
                for dx in (-1, 1):

                    @pl.when(has_x(dx))
                    def _():
                        relay(p, dx).start()

    for parity, steps in enumerate((EVEN, ODD)):

        @pl.when(lax.rem(gy, 2) == parity)
        def _():
            first = [over_x for over_x, _ in steps].index(True)
            for n, (over_x, p) in enumerate(steps):
                (from_x if over_x else from_y)(p)
                if n == first:
                    each(FAR, lambda i: remote(i).start())

    staged[6].wait()
    staged[7].wait()
    staged[9].wait()
    for n in range(3):

        @pl.when((beside_x == n) & has_y(-outer))
        def _():
            whole(n + 1, inside, 0, -outer)

    total = jnp.zeros(own_ref.shape, jnp.float32)
    places = []
    for k in range(depth):
        source = src[0, k]
        position = (source // ny - gx + 1) * 3 + (source % ny - gy + 1)
        places.append(jnp.clip(position, 0, 8))
        total += jnp.dot(ocn[places[k]], wts[k], preferred_element_type=jnp.float32)
    own_ref[...] = total

    @pl.when(has_y(outer))
    def _():
        for n in range(1, 3):

            @pl.when(beside_x == n)
            def _():
                whole(n, inside + 1, 0, outer)

        total = own_ref[...]
        for dx in (-1, 1):
            match = depth
            for k in range(depth):
                match = jnp.where(places[k] == 4 + 3 * dx + outer, k, match)
            total += jnp.dot(late[int(dx > 0)], wts[match], preferred_element_type=jnp.float32)
        own_ref[...] = total

    total = own_ref[...]
    width = strip_ref.shape[0]
    near, far = slice(0, 8 * width), slice(8 * width, 16 * width)
    rest = jnp.zeros((width - members, total.shape[1]), jnp.float32)
    picked = lax.dot_general(
        table_ref[:width, (16 + SLOTS) * width : (17 + SLOTS) * width], split_rows(jnp.concatenate([total, rest], axis=0)), (((1,), (1,)), ((), ())),
        preferred_element_type=jnp.float32,
    )
    strip_ref[...] = picked[:, :width] + picked[:, width:]
    each(FAR + NEAR, lambda i: border(i).start())

    all_of(lambda *n: whole_notes(*n).wait_recv())
    flat = meta[...].reshape(meta.shape[0] * meta.shape[1], meta.shape[2]).T
    cells = total.shape[1]
    places = table_ref[:16, (17 + SLOTS) * cells :].astype(jnp.float32)
    places = places[0:1] * CODE + places[1:2]
    for b in range(NB):
        for half, tiles in ((0, [4]), (1, OTHERS)):
            code = places[:, half * cells : (half + 1) * cells]
            live = jnp.zeros((OB, cells), jnp.float32)
            error = live + 1.0
            value = live
            base = live + 1.0
            for i in tiles:
                dx, dy = OFFS[i]
                column = flat[b * OB : (b + 1) * OB, 8 * i : 8 * i + 4]
                hit = column[:, 0:1] + float((AX * dx + AX) * CODE + AY * dy + AY) == code
                live = jnp.where(hit, column[:, 3:4], live)
                error = jnp.where(hit, column[:, 2:3], error)
                value = jnp.where(hit, column[:, 1:2], value)
                base = jnp.where(hit, column[:, 2:3] + (1.0 - column[:, 3:4]), base)
            for n, table in enumerate((live, error, value, base)):
                obs_ref[b, n, :, half * cells : (half + 1) * cells] = table

    scale = 1.0 / (members - 1)
    gmean, own = moments(own_ref[...], members)
    own_ref[...] = own
    alpha, beta = strengths(own, gmean, [obs_ref[0, n, :, :cells] for n in range(4)], members)
    shifted[...] = shift(own, alpha, beta, table_ref[:cells, near])
    center = (alpha * scale, beta * scale)

    def one_field(v, carry):
        block = held[v]
        found = sources_of(shifted, members, around(scale, cells))
        total, mean = gather(block, [*found, (own_ref[...], *center)])
        part_ref[v] = block - total
        fmean[pl.ds(v, 1), :] = fmean[pl.ds(v, 1), :] + mean
        return carry

    lax.fori_loop(0, fields, one_field, 0)
    found = sources_of(shifted, members, around(scale, cells))
    total, mean = gather(own, [*found, (own, *center)])
    part_ref[fields] = own - total
    fmean[fields : fields + 1, :] = gmean + mean
    beyond_ref[...] = shift(own, alpha, beta, table_ref[:cells, far])

    all_sent()
    all_of(lambda *n: whole_notes(*n).wait_send())
    all_of(lambda *n: whole_border(*n).wait_send())
    all_of(lambda *n: whole_border(*n).wait_recv())


def analysis_kernel(
    own_ref, halo_ref, obs_ref, held_in, part_ref, fmean_ref, beyond_ref, table_ref,
    mean_out, anom_ref,
    held, mean_ref, inner, shifted, out_sem,
):
    fields, members, cells = held_in.shape
    scale = 1.0 / (members - 1)
    own = own_ref[...]
    hmean, halo = moments(halo_ref[...].T[:members], members)
    alpha, beta = strengths(halo, hmean, [obs_ref[0, n, :, cells:] for n in range(4)], members)
    inner[...] = shift(halo, alpha, beta, table_ref[cells:, 16 * cells : (16 + SLOTS) * cells])
    taps = table_ref[:16, (17 + SLOTS) * cells : (18 + SLOTS) * cells].astype(jnp.float32) * scale
    taps = [(taps[2 + n : 3 + n], cells) for n in range(SLOTS)]
    total, mean = gather(own, sources_of(inner, members, taps))
    block = part_ref[fields] - total
    gmean = fmean_ref[fields : fields + 1, :] + mean
    beyond = beyond_ref[...] + shift(halo, alpha, beta, table_ref[cells:, 8 * cells : 16 * cells])
    edges = sources_of(beyond, members, around(scale, cells))
    total, mean = gather(halo, [*edges, (halo, alpha * scale, beta * scale)])
    grid = jnp.concatenate([block, halo - total], axis=1)
    gmean = jnp.concatenate([gmean, hmean + mean], axis=1)

    alpha, beta = strengths(grid, gmean, [obs_ref[1, n] for n in range(4)], members)
    shifted[...] = shift(grid, alpha, beta, table_ref[:, : 8 * cells])
    held[fields] = block
    center = (alpha[:, :cells] * scale, beta[:, :cells] * scale)

    def save(v):
        return pltpu.make_async_copy(held.at[v], anom_ref.at[v], out_sem.at[0])

    def one_field(v, carry):
        total, before = gather(held_in[v], sources_of(inner, members, taps))
        block = part_ref[v] - total
        near = sources_of(shifted, members, around(scale, cells))
        total, mean = gather(block, [*near, (held[fields], *center)])
        held[v] = block - total
        mean_ref[v] = fmean_ref[pl.ds(v, 1), :] + before + mean
        save(v).start()
        return carry

    lax.fori_loop(0, fields, one_field, 0)
    near = sources_of(shifted, members, around(scale, cells))
    total, mean = gather(block, [*near, (block, *center)])
    mean_ref[fields] = gmean[:, :cells] + mean
    means = pltpu.make_async_copy(mean_ref, mean_out, out_sem.at[1])
    means.start()
    held[fields] = block - total
    save(fields).start()
    means.wait()
    pltpu.make_async_copy(held, anom_ref, out_sem.at[0]).wait()


def local(
    atm_members, ocean_members, remap_weights, pair_src, obs_cell, obs_value, obs_error,
    obs_live, obs_order,
):
    members, fields, cells = atm_members.shape[2:]
    slots = obs_cell.shape[2]
    sources, depth = remap_weights.shape[2:4]
    vmem = pl.BlockSpec(memory_space=pltpu.VMEM)
    anywhere = pl.BlockSpec(memory_space=pl.ANY)
    table = tables()
    results = (
        pltpu.VMEM((members, cells), jnp.float32),
        pltpu.VMEM((cells, 128), jnp.float32),
        pltpu.VMEM((NB, 4, OB, 2 * cells), jnp.float32),
        pltpu.VMEM((fields, members, cells), jnp.float32),
        pltpu.VMEM((fields + 1, members, cells), jnp.float32),
        pltpu.VMEM((16, cells), jnp.float32),
        pltpu.VMEM((members + 8, 8 * cells), jnp.float32),
        pltpu.VMEM(table.shape, jnp.bfloat16),
    )
    state = pl.pallas_call(
        exchange_kernel,
        out_shape=results,
        in_specs=[anywhere] * 10,
        out_specs=(vmem,) * len(results),
        scratch_shapes=[
            pltpu.VMEM((9, members, depth), jnp.bfloat16),
            pltpu.VMEM((2, members, depth), jnp.bfloat16),
            pltpu.VMEM((sources + 1, depth, cells), jnp.bfloat16),
            pltpu.VMEM((16, 8, 128), jnp.float32),
            pltpu.SMEM((1, sources), jnp.int32),
            pltpu.VMEM((3, 1, slots), jnp.int32),
            pltpu.VMEM((2, 1, slots), jnp.float32),
            pltpu.VMEM((cells, 128), jnp.float32),
            pltpu.VMEM((members + 8, 8 * cells), jnp.float32),
            pltpu.SemaphoreType.DMA((7,)),
            pltpu.SemaphoreType.DMA((1,)),
            pltpu.SemaphoreType.DMA((3 * (members // PIECE) + 2,)),
            pltpu.SemaphoreType.DMA((2,)),
        ],
        compiler_params=pltpu.CompilerParams(
            collective_id=0, has_side_effects=True, vmem_limit_bytes=LIMIT
        ),
        name="exchange",
    )(
        *(
            pltpu.with_memory_space_constraint(x, pltpu.HBM)
            for x in (
                pair_src[0], obs_order[0], obs_cell[0], obs_live[0], obs_value[0], obs_error[0],
                ocean_members[0, 0], remap_weights[0, 0],
                jnp.transpose(atm_members[0, 0], (1, 0, 2)),
                jnp.asarray(table, jnp.bfloat16),
            )
        )
    )
    post_mean, post_anom = pl.pallas_call(
        analysis_kernel,
        out_shape=(
            jax.ShapeDtypeStruct((fields + 1, 1, cells), jnp.float32),
            jax.ShapeDtypeStruct((fields + 1, members, cells), jnp.float32),
        ),
        in_specs=[vmem] * len(results),
        out_specs=(anywhere, anywhere),
        scratch_shapes=[
            pltpu.VMEM((fields + 1, members, cells), jnp.float32),
            pltpu.VMEM((fields + 1, 1, cells), jnp.float32),
            pltpu.VMEM((members + 8, SLOTS * cells), jnp.float32),
            pltpu.VMEM((members + 8, 8 * cells), jnp.float32),
            pltpu.SemaphoreType.DMA((2,)),
        ],
        compiler_params=pltpu.CompilerParams(vmem_limit_bytes=LIMIT),
        name="analysis",
    )(*state)
    return (post_mean.reshape(1, 1, fields + 1, cells), jnp.transpose(post_anom, (1, 0, 2))[None, None])


def solution(mesh):
    in_specs = (
        P("gx", "gy", None, None, None),
        P("gx", "gy", None, None),
        P("gx", "gy", None, None, None),
        P("gx", "gy", None),
        P("gx", "gy", None),
        P("gx", "gy", None),
        P("gx", "gy", None),
        P("gx", "gy", None),
        P("gx", "gy", None),
    )
    out_specs = (P("gx", "gy", None, None), P("gx", "gy", None, None, None))
    return jax.shard_map(local, mesh=mesh, in_specs=in_specs, out_specs=out_specs, check_vma=False)
```

```python
import functools

import jax
import jax.numpy as jnp
import numpy as np
from jax import lax
from jax.experimental import pallas as pl
from jax.experimental.pallas import tpu as pltpu
from jax.sharding import PartitionSpec as P

AX = 8
AY = 16
OB = 32
NB = 2
RAD = 2
CODE = 64
LIMIT = 32 * 1024 * 1024

MESH = pl.DeviceIdType.MESH
OFFS = [(dx, dy) for dx in (-1, 0, 1) for dy in (-1, 0, 1)]
OTHERS = [i for i in range(9) if i != 4]
NEAR = [1, 3, 5, 7]
FAR = [0, 2, 6, 8]
PIECE = 16
SHARES = (3, 1, 3, 4, 4, 3, 1, 3)
EVEN = [(False, 0), (False, 1), (True, 4), (False, 2), (True, 3), (True, 2), (False, 3), (True, 1), (True, 0), (False, 4)]
ODD = [(True, 4), (True, 3), (False, 0), (True, 2), (False, 1), (True, 1), (False, 2), (True, 0), (False, 3), (False, 4)]
SLOTS = 5


def taper_of(dx, dy):
    return max(1.0 - (dx * dx + dy * dy) / float(RAD * RAD), 0.0) ** 2


def edge(d, size):
    return {-1: range(RAD), 0: range(size), 1: range(size - RAD, size)}[d]


def strip(i):
    dx, dy = OFFS[i]
    return [(x, y) for x in edge(dx, AX) for y in edge(dy, AY)]


def strips():
    spans, at = {}, 0
    for i in OTHERS:
        rows = -(-len(strip(i)) // 8) * 8
        spans[i] = (at, rows)
        at += rows
    return spans


SPANS = strips()


@functools.lru_cache
def tables():
    cells = AX * AY
    where = {(c // AY, c % AY): c for c in range(cells)}
    out = np.zeros((cells, cells), np.float32)
    for i in OTHERS:
        dx, dy = OFFS[i]
        for n, (x, y) in enumerate(strip(i)):
            out[SPANS[i][0] + n, x * AY + y] = 1.0
        for n, (x, y) in enumerate(strip(8 - i)):
            where[(x + dx * AX, y + dy * AY)] = cells + SPANS[i][0] + n
    code = np.zeros((2 * cells, 2 * cells), np.float32)
    code[:2, :] = -1.0
    move = np.zeros((2 * cells, 2, 8, cells), np.float32)
    slot = np.zeros((2 * cells, SLOTS, cells), np.float32)
    for (x, y), n in where.items():
        code[0, n], code[1, n] = x + AX, y + AY
        taken = 0
        for d, i in enumerate(OTHERS):
            dx, dy = OFFS[i]
            src = where.get((x + dx, y + dy))
            if src is not None:
                move[src, n // cells, d, n % cells] = 1.0
                if n < cells <= src:
                    slot[src, taken, n] = 1.0
                    code[2 + taken, n] = taper_of(dx, dy)
                    taken += 1
    own = move[:, 0].reshape(2 * cells, 8 * cells)
    far = move[:, 1].reshape(2 * cells, 8 * cells)
    slot = slot.reshape(2 * cells, SLOTS * cells)
    out = np.concatenate([out, np.zeros_like(out)], axis=0)
    return np.concatenate([own, far, slot, out, code], axis=1)


def split_rows(block):
    high = block.astype(jnp.bfloat16).astype(jnp.float32)
    return jnp.concatenate([high, block - high], axis=0).astype(jnp.bfloat16)


def moments(block, members):
    mean = jnp.sum(block, axis=0, keepdims=True) / members
    return mean, block - mean


def strengths(block, mean, table, members):
    variance = jnp.sum(block * block, axis=0, keepdims=True) / (members - 1)
    live, error, value, base = table
    denom = variance + base
    weighting = live / denom
    damping = 1.0 / (1.0 + jnp.sqrt(error / denom))
    alpha = jnp.sum(weighting * damping, axis=0, keepdims=True)
    beta = jnp.sum(weighting * value, axis=0, keepdims=True)
    return alpha, beta - mean * jnp.sum(weighting, axis=0, keepdims=True)


def shift(block, alpha, beta, tables):
    rest = jnp.zeros((6, block.shape[1]), jnp.float32)
    rows = block.shape[0] + 8
    left = split_rows(jnp.concatenate([block, alpha, beta, rest], axis=0))
    moved = jnp.dot(left, tables, preferred_element_type=jnp.float32)
    return moved[:rows] + moved[rows:]


def gather(block, sources, left):
    mean = jnp.zeros((1, block.shape[1]), jnp.float32)
    for source, a, m in sources:
        cov = jnp.sum(block * source, axis=0, keepdims=True)
        mean = mean + cov * m
        left = left - source * (cov * a)
    return left, mean


def sources_of(shifted, members, weights):
    cells = weights[0][1]
    found = []
    for d, (weight, width) in enumerate(weights):
        part = slice(d * cells, d * cells + width)
        found.append(
            (
                shifted[:members, part],
                shifted[members : members + 1, part] * weight,
                shifted[members + 1 : members + 2, part] * weight,
            )
        )
    return found


def around(scale, cells):
    return [(scale * taper_of(*OFFS[i]), cells) for i in OTHERS]


def exchange_kernel(
    src_ref, order_ref, cell_ref, live_ref, value_ref, error_ref, ocean_ref, weights_ref, atm_ref,
    table_in,
    own_ref, halo_ref, obs_ref, held, part_ref, fmean, beyond_ref, table_ref,
    ocn, late, wts, meta, src, ints, floats, strip_ref, shifted,
    local_sem, send_sem, recv_sem, note_sem,
):
    gx, gy = lax.axis_index("gx"), lax.axis_index("gy")
    nx, ny = lax.axis_size("gx"), lax.axis_size("gy")
    members = own_ref.shape[0]
    fields = atm_ref.shape[0]
    slots = ints.shape[2]

    def has_x(dx):
        return (gx + dx >= 0) & (gx + dx < nx)

    def has_y(dy):
        return (gy + dy >= 0) & (gy + dy < ny)

    def there(i):
        return has_x(OFFS[i][0]) & has_y(OFFS[i][1])

    barrier = pltpu.get_barrier_semaphore()
    for i in NEAR:
        dx, dy = OFFS[i]

        @pl.when(there(i))
        def _():
            pl.semaphore_signal(barrier, inc=1, device_id=(gx + dx, gy + dy), device_id_type=MESH)

    depth = wts.shape[0] - 1
    pairs = (
        (ocean_ref, ocn.at[4], 0), (order_ref, ints.at[0], 1), (cell_ref, ints.at[1], 1),
        (live_ref, ints.at[2], 1), (value_ref, floats.at[0], 2), (error_ref, floats.at[1], 2),
        (src_ref, src, 3), (weights_ref, wts.at[0:depth], 4), (atm_ref, held, 5),
        (table_in, table_ref, 6),
    )
    staged = [pltpu.make_async_copy(x, y, local_sem.at[n]) for x, y, n in pairs]
    outer = lax.rem(gy, 2) * 2 - 1
    for copy in staged:
        copy.start()

    for i in OTHERS:

        @pl.when(jnp.logical_not(there(i)))
        def _():
            at, rows = SPANS[i]
            halo_ref[at : at + rows, :] = jnp.zeros((rows, halo_ref.shape[1]), jnp.float32)
            meta[i] = jnp.zeros(meta.shape[1:], jnp.float32)

    for dx in (-1, 1):
        ocn[4 + 3 * dx + outer] = jnp.zeros(ocn.shape[1:], ocn.dtype)

        @pl.when(jnp.logical_not(has_x(dx) & has_y(outer)))
        def _():
            late[int(dx > 0)] = jnp.zeros(late.shape[1:], late.dtype)

    wts[depth] = jnp.zeros(wts.shape[1:], wts.dtype)
    for n in range(9, meta.shape[0]):
        meta[n] = jnp.zeros(meta.shape[1:], jnp.float32)

    staged[0].wait()
    pl.semaphore_wait(barrier, sum(there(i).astype(jnp.int32) for i in NEAR))

    count = members // PIECE

    def among(y, wanted):
        at = lax.rem(y + 8, 8)
        return sum((at == n).astype(jnp.int32) for n, share in enumerate(SHARES) if wanted(share)) > 0

    def relayed(y, p):
        return among(y, lambda share: p < share)

    def ocean(low, rows, source, target, kind, index, dx, dy):
        return pltpu.make_async_remote_copy(
            src_ref=ocn.at[source, pl.ds(low, rows)],
            dst_ref=target.at[pl.ds(low, rows)],
            send_sem=send_sem.at[0],
            recv_sem=recv_sem.at[index],
            device_id=(gx + dx, gy + dy),
            device_id_type=MESH,
        )

    def piece(p, source, target, kind, index, dx, dy):
        return ocean(p * PIECE, PIECE, source, target, kind, index, dx, dy)

    def arrive(at, index, dx, dy, p):
        ocean(p * PIECE, PIECE, at, ocn.at[at], 0, index, dx, dy).wait_recv()

    def sent(rows, kind, dx, dy):
        ocean(0, rows, 4, ocn.at[4], kind, 0, dx, dy).wait_send()

    def whole(blocks, index, dx, dy):
        pltpu.make_async_remote_copy(
            src_ref=ocn.at[pl.ds(0, blocks)],
            dst_ref=ocn.at[pl.ds(0, blocks)],
            send_sem=send_sem.at[0],
            recv_sem=recv_sem.at[index],
            device_id=(gx + dx, gy + dy),
            device_id_type=MESH,
        ).wait_recv()

    order = range(count)

    def start(cond, copies):
        @pl.when(cond)
        def _():
            for copy in copies:
                copy.start()

    def from_side(dx):
        return count * (dx > 0)

    beside, inside = 2 * count, 3 * count

    mine = lax.rem(gy, 8)
    yields = (mine == 2) | (mine == 5)
    to_outer = [piece(p, 4, ocn.at[4 - outer], 0, beside + p, 0, outer) for p in order]
    start(has_y(outer) & jnp.logical_not(yields), to_outer)
    for dx in (-1, 1):
        start(
            has_x(dx),
            [
                piece(p, 4, ocn.at[4 - 3 * dx], 2 + (dx > 0), from_side(-dx) + p, dx, 0)
                for p in reversed(order)
            ],
        )
    start(has_y(-outer), [ocean(0, members, 4, ocn.at[4 + outer], 1, inside, 0, -outer)])

    def relay(p, dx):
        return piece(p, 4 + outer, late.at[int(dx < 0)], 4 + (dx > 0), inside + 1, dx, 0)

    def forward(p, dx):
        return piece(p, 4 + 3 * dx, late.at[int(dx > 0)], 6 + (dx > 0), inside + 1, 0, outer)

    def hand(p, dx):
        return piece(p, 4 + 3 * dx, ocn.at[4 + 3 * dx + outer], 8 + (dx > 0), inside, 0, -outer)

    def all_sent():
        @pl.when(has_y(outer))
        def _():
            sent(members, 0, 0, outer)

        @pl.when(has_y(-outer))
        def _():
            sent(members, 1, 0, -outer)

        for dx in (-1, 1):

            @pl.when(has_x(dx))
            def _():
                sent(members, 2 + (dx > 0), dx, 0)

            @pl.when(has_x(dx) & has_y(-outer))
            def _():
                sent(members, 8 + (dx > 0), 0, -outer)

            for n in sorted(set(SHARES)):

                @pl.when(has_x(dx) & has_y(outer) & among(gy + outer, lambda share: share == n))
                def _():
                    if n:
                        sent(n * PIECE, 4 + (dx > 0), dx, 0)

                @pl.when(has_x(dx) & has_y(outer) & among(gy, lambda share: share == n))
                def _():
                    if n < count:
                        sent((count - n) * PIECE, 6 + (dx > 0), 0, outer)

    beside_x = has_x(-1).astype(jnp.int32) + has_x(1).astype(jnp.int32)
    beside_y = has_y(-1).astype(jnp.int32) + has_y(1).astype(jnp.int32)

    def remote(i):
        dx, dy = OFFS[i]
        return pltpu.make_async_remote_copy(
            src_ref=meta.at[4],
            dst_ref=meta.at[8 - i],
            send_sem=send_sem.at[0],
            recv_sem=note_sem.at[0],
            device_id=(gx + dx, gy + dy),
            device_id_type=MESH,
        )

    def border(i):
        dx, dy = OFFS[i]
        (source, rows), (target, _) = SPANS[i], SPANS[8 - i]
        return pltpu.make_async_remote_copy(
            src_ref=strip_ref.at[pl.ds(source, rows)],
            dst_ref=halo_ref.at[pl.ds(target, rows)],
            send_sem=send_sem.at[0],
            recv_sem=note_sem.at[1],
            device_id=(gx + dx, gy + dy),
            device_id_type=MESH,
        )

    def all_of(act):
        for nx_ in range(3):
            for ny_ in range(3):
                if nx_ + ny_:

                    @pl.when((beside_x == nx_) & (beside_y == ny_))
                    def _():
                        act(nx_, ny_)

    def whole_notes(nx_, ny_):
        n = (nx_ + 1) * (ny_ + 1) - 1
        return pltpu.make_async_remote_copy(
            src_ref=meta.at[pl.ds(0, n)], dst_ref=meta.at[pl.ds(0, n)],
            send_sem=send_sem.at[0], recv_sem=note_sem.at[0],
            device_id=(gx, gy + outer), device_id_type=MESH,
        )

    def whole_border(nx_, ny_):
        rows = nx_ * SPANS[1][1] + ny_ * SPANS[3][1] + nx_ * ny_ * SPANS[0][1]
        return pltpu.make_async_remote_copy(
            src_ref=strip_ref.at[pl.ds(0, rows)], dst_ref=halo_ref.at[pl.ds(0, rows)],
            send_sem=send_sem.at[0], recv_sem=note_sem.at[1],
            device_id=(gx, gy + outer), device_id_type=MESH,
        )

    def each(which, act):
        for i in which:

            @pl.when(there(i))
            def _():
                act(i)

    pltpu.make_async_copy(ints, ints, local_sem.at[1]).wait()
    pltpu.make_async_copy(floats, floats, local_sem.at[2]).wait()
    cell = ints[1]
    spot = ((cell // AY) * CODE + cell % AY).astype(jnp.float32)
    rows = jnp.concatenate(
        [
            spot, floats[0], floats[1], ints[2].astype(jnp.float32),
            jnp.zeros((4, slots), jnp.float32),
        ],
        axis=0,
    )
    slot = lax.broadcasted_iota(jnp.int32, (slots, slots), 0)
    perm = jnp.where(ints[0] == slot, 1.0, 0.0)
    rows = jnp.dot(rows, perm, precision=lax.Precision.HIGHEST, preferred_element_type=jnp.float32)
    meta[4] = jnp.concatenate([rows, jnp.zeros((8, meta.shape[2] - slots), jnp.float32)], axis=1)

    each(NEAR, lambda i: remote(i).start())

    staged[8].wait()
    for v in range(fields):
        block = held[v]
        mean = jnp.sum(block, axis=0, keepdims=True) / members
        fmean[v : v + 1, :] = mean
        held[v] = block - mean

    start(has_y(outer) & yields, to_outer)

    def from_x(p):
        for dx in (-1, 1):

            @pl.when(has_x(dx))
            def _():
                arrive(4 + 3 * dx, from_side(dx) + p, dx, 0, p)

                @pl.when(has_y(outer) & jnp.logical_not(relayed(gy, p)))
                def _():
                    forward(p, dx).start()

                @pl.when(has_y(-outer))
                def _():
                    hand(p, dx).start()

    def from_y(p):
        @pl.when(has_y(outer))
        def _():
            arrive(4 + outer, beside + p, 0, outer, p)

            @pl.when(relayed(gy + outer, p))
            def _():
                for dx in (-1, 1):

                    @pl.when(has_x(dx))
                    def _():
                        relay(p, dx).start()

    for parity, steps in enumerate((EVEN, ODD)):

        @pl.when(lax.rem(gy, 2) == parity)
        def _():
            first = [over_x for over_x, _ in steps].index(True)
            for n, (over_x, p) in enumerate(steps):
                (from_x if over_x else from_y)(p)
                if n == first:
                    each(FAR, lambda i: remote(i).start())

    staged[6].wait()
    staged[7].wait()
    staged[9].wait()
    for n in range(3):

        @pl.when((beside_x == n) & has_y(-outer))
        def _():
            whole(n + 1, inside, 0, -outer)

    total = jnp.zeros(own_ref.shape, jnp.float32)
    places = []
    for k in range(depth):
        source = src[0, k]
        position = (source // ny - gx + 1) * 3 + (source % ny - gy + 1)
        places.append(jnp.clip(position, 0, 8))
        total += jnp.dot(ocn[places[k]], wts[k], preferred_element_type=jnp.float32)
    for n in range(1, 3):

        @pl.when((beside_x == n) & has_y(outer))
        def _():
            whole(n, inside + 1, 0, outer)

    for dx in (-1, 1):
        match = depth
        for k in range(depth):
            match = jnp.where(places[k] == 4 + 3 * dx + outer, k, match)
        total += jnp.dot(late[int(dx > 0)], wts[match], preferred_element_type=jnp.float32)
    own_ref[...] = total
    width = strip_ref.shape[0]
    near, far = slice(0, 8 * width), slice(8 * width, 16 * width)
    rest = jnp.zeros((width - members, total.shape[1]), jnp.float32)
    picked = lax.dot_general(
        table_ref[:width, (16 + SLOTS) * width : (17 + SLOTS) * width], split_rows(jnp.concatenate([total, rest], axis=0)), (((1,), (1,)), ((), ())),
        preferred_element_type=jnp.float32,
    )
    strip_ref[...] = picked[:, :width] + picked[:, width:]
    each(FAR + NEAR, lambda i: border(i).start())

    all_of(lambda *n: whole_notes(*n).wait_recv())
    flat = meta[...].reshape(meta.shape[0] * meta.shape[1], meta.shape[2]).T
    cells = total.shape[1]
    places = table_ref[:16, (17 + SLOTS) * cells :].astype(jnp.float32)
    places = places[0:1] * CODE + places[1:2]
    for b in range(NB):
        for half, tiles in ((0, [4]), (1, OTHERS)):
            code = places[:, half * cells : (half + 1) * cells]
            live = jnp.zeros((OB, cells), jnp.float32)
            error = live + 1.0
            value = live
            base = live + 1.0
            for i in tiles:
                dx, dy = OFFS[i]
                column = flat[b * OB : (b + 1) * OB, 8 * i : 8 * i + 4]
                hit = column[:, 0:1] + float((AX * dx + AX) * CODE + AY * dy + AY) == code
                live = jnp.where(hit, column[:, 3:4], live)
                error = jnp.where(hit, column[:, 2:3], error)
                value = jnp.where(hit, column[:, 1:2], value)
                base = jnp.where(hit, column[:, 2:3] + (1.0 - column[:, 3:4]), base)
            for n, table in enumerate((live, error, value, base)):
                obs_ref[b, n, :, half * cells : (half + 1) * cells] = table

    scale = 1.0 / (members - 1)
    gmean, own = moments(own_ref[...], members)
    own_ref[...] = own
    alpha, beta = strengths(own, gmean, [obs_ref[0, n, :, :cells] for n in range(4)], members)
    shifted[...] = shift(own, alpha, beta, table_ref[:cells, near])
    center = (alpha * scale, beta * scale)

    def one_field(v, carry):
        block = held[v]
        found = sources_of(shifted, members, around(scale, cells))
        part_ref[v], mean = gather(block, [*found, (own_ref[...], *center)], block)
        fmean[pl.ds(v, 1), :] = fmean[pl.ds(v, 1), :] + mean
        return carry

    lax.fori_loop(0, fields, one_field, 0)
    found = sources_of(shifted, members, around(scale, cells))
    part_ref[fields], mean = gather(own, [*found, (own, *center)], own)
    fmean[fields : fields + 1, :] = gmean + mean
    beyond_ref[...] = shift(own, alpha, beta, table_ref[:cells, far])

    all_sent()
    all_of(lambda *n: whole_notes(*n).wait_send())
    all_of(lambda *n: whole_border(*n).wait_send())
    all_of(lambda *n: whole_border(*n).wait_recv())


def analysis_kernel(
    own_ref, halo_ref, obs_ref, held_in, part_ref, fmean_ref, beyond_ref, table_ref,
    mean_out, anom_ref,
    held, mean_ref, inner, shifted, out_sem,
):
    fields, members, cells = held_in.shape
    scale = 1.0 / (members - 1)
    own = own_ref[...]
    hmean, halo = moments(halo_ref[...].T[:members], members)
    alpha, beta = strengths(halo, hmean, [obs_ref[0, n, :, cells:] for n in range(4)], members)
    inner[...] = shift(halo, alpha, beta, table_ref[cells:, 16 * cells : (16 + SLOTS) * cells])
    taps = table_ref[:16, (17 + SLOTS) * cells : (18 + SLOTS) * cells].astype(jnp.float32) * scale
    taps = [(taps[2 + n : 3 + n], cells) for n in range(SLOTS)]
    block, mean = gather(own, sources_of(inner, members, taps), part_ref[fields])
    gmean = fmean_ref[fields : fields + 1, :] + mean
    beyond = beyond_ref[...] + shift(halo, alpha, beta, table_ref[cells:, 8 * cells : 16 * cells])
    edges = sources_of(beyond, members, around(scale, cells))
    halo, mean = gather(halo, [*edges, (halo, alpha * scale, beta * scale)], halo)
    grid = jnp.concatenate([block, halo], axis=1)
    gmean = jnp.concatenate([gmean, hmean + mean], axis=1)

    alpha, beta = strengths(grid, gmean, [obs_ref[1, n] for n in range(4)], members)
    shifted[...] = shift(grid, alpha, beta, table_ref[:, : 8 * cells])
    held[fields] = block
    center = (alpha[:, :cells] * scale, beta[:, :cells] * scale)

    def save(v):
        return pltpu.make_async_copy(held.at[v], anom_ref.at[v], out_sem.at[0])

    def one_field(v, carry):
        block, before = gather(held_in[v], sources_of(inner, members, taps), part_ref[v])
        near = sources_of(shifted, members, around(scale, cells))
        held[v], mean = gather(block, [*near, (held[fields], *center)], block)
        mean_ref[v] = fmean_ref[pl.ds(v, 1), :] + before + mean
        save(v).start()
        return carry

    lax.fori_loop(0, fields, one_field, 0)
    near = sources_of(shifted, members, around(scale, cells))
    rest, mean = gather(block, [*near, (block, *center)], block)
    mean_ref[fields] = gmean[:, :cells] + mean
    means = pltpu.make_async_copy(mean_ref, mean_out, out_sem.at[1])
    means.start()
    held[fields] = rest
    save(fields).start()
    means.wait()
    pltpu.make_async_copy(held, anom_ref, out_sem.at[0]).wait()


def local(
    atm_members, ocean_members, remap_weights, pair_src, obs_cell, obs_value, obs_error,
    obs_live, obs_order,
):
    members, fields, cells = atm_members.shape[2:]
    slots = obs_cell.shape[2]
    sources, depth = remap_weights.shape[2:4]
    vmem = pl.BlockSpec(memory_space=pltpu.VMEM)
    anywhere = pl.BlockSpec(memory_space=pl.ANY)
    table = tables()
    results = (
        pltpu.VMEM((members, cells), jnp.float32),
        pltpu.VMEM((cells, 128), jnp.float32),
        pltpu.VMEM((NB, 4, OB, 2 * cells), jnp.float32),
        pltpu.VMEM((fields, members, cells), jnp.float32),
        pltpu.VMEM((fields + 1, members, cells), jnp.float32),
        pltpu.VMEM((16, cells), jnp.float32),
        pltpu.VMEM((members + 8, 8 * cells), jnp.float32),
        pltpu.VMEM(table.shape, jnp.bfloat16),
    )
    state = pl.pallas_call(
        exchange_kernel,
        out_shape=results,
        in_specs=[anywhere] * 10,
        out_specs=(vmem,) * len(results),
        scratch_shapes=[
            pltpu.VMEM((9, members, depth), jnp.bfloat16),
            pltpu.VMEM((2, members, depth), jnp.bfloat16),
            pltpu.VMEM((sources + 1, depth, cells), jnp.bfloat16),
            pltpu.VMEM((16, 8, 128), jnp.float32),
            pltpu.SMEM((1, sources), jnp.int32),
            pltpu.VMEM((3, 1, slots), jnp.int32),
            pltpu.VMEM((2, 1, slots), jnp.float32),
            pltpu.VMEM((cells, 128), jnp.float32),
            pltpu.VMEM((members + 8, 8 * cells), jnp.float32),
            pltpu.SemaphoreType.DMA((7,)),
            pltpu.SemaphoreType.DMA((1,)),
            pltpu.SemaphoreType.DMA((3 * (members // PIECE) + 2,)),
            pltpu.SemaphoreType.DMA((2,)),
        ],
        compiler_params=pltpu.CompilerParams(
            collective_id=0, has_side_effects=True, vmem_limit_bytes=LIMIT
        ),
        name="exchange",
    )(
        *(
            pltpu.with_memory_space_constraint(x, pltpu.HBM)
            for x in (
                pair_src[0], obs_order[0], obs_cell[0], obs_live[0], obs_value[0], obs_error[0],
                ocean_members[0, 0], remap_weights[0, 0],
                jnp.transpose(atm_members[0, 0], (1, 0, 2)),
                jnp.asarray(table, jnp.bfloat16),
            )
        )
    )
    post_mean, post_anom = pl.pallas_call(
        analysis_kernel,
        out_shape=(
            jax.ShapeDtypeStruct((fields + 1, 1, cells), jnp.float32),
            jax.ShapeDtypeStruct((fields + 1, members, cells), jnp.float32),
        ),
        in_specs=[vmem] * len(results),
        out_specs=(anywhere, anywhere),
        scratch_shapes=[
            pltpu.VMEM((fields + 1, members, cells), jnp.float32),
            pltpu.VMEM((fields + 1, 1, cells), jnp.float32),
            pltpu.VMEM((members + 8, SLOTS * cells), jnp.float32),
            pltpu.VMEM((members + 8, 8 * cells), jnp.float32),
            pltpu.SemaphoreType.DMA((2,)),
        ],
        compiler_params=pltpu.CompilerParams(vmem_limit_bytes=LIMIT),
        name="analysis",
    )(*state)
    return (post_mean.reshape(1, 1, fields + 1, cells), jnp.transpose(post_anom, (1, 0, 2))[None, None])


def solution(mesh):
    in_specs = (
        P("gx", "gy", None, None, None),
        P("gx", "gy", None, None),
        P("gx", "gy", None, None, None),
        P("gx", "gy", None),
        P("gx", "gy", None),
        P("gx", "gy", None),
        P("gx", "gy", None),
        P("gx", "gy", None),
        P("gx", "gy", None),
    )
    out_specs = (P("gx", "gy", None, None), P("gx", "gy", None, None, None))
    return jax.shard_map(local, mesh=mesh, in_specs=in_specs, out_specs=out_specs, check_vma=False)
```

```python
import functools

import jax
import jax.numpy as jnp
import numpy as np
from jax import lax
from jax.experimental import pallas as pl
from jax.experimental.pallas import tpu as pltpu
from jax.sharding import PartitionSpec as P

AX = 8
AY = 16
OB = 32
NB = 2
RAD = 2
CODE = 64
LIMIT = 32 * 1024 * 1024

MESH = pl.DeviceIdType.MESH
OFFS = [(dx, dy) for dx in (-1, 0, 1) for dy in (-1, 0, 1)]
OTHERS = [i for i in range(9) if i != 4]
NEAR = [1, 3, 5, 7]
FAR = [0, 2, 6, 8]
PIECE = 16
SHARES = (3, 1, 3, 4, 4, 3, 1, 3)
EVEN = [(False, 0), (False, 1), (True, 4), (False, 2), (True, 3), (True, 2), (False, 3), (True, 1), (True, 0), (False, 4)]
ODD = [(True, 4), (True, 3), (False, 0), (True, 2), (False, 1), (True, 1), (False, 2), (True, 0), (False, 3), (False, 4)]
SLOTS = 5


def taper_of(dx, dy):
    return max(1.0 - (dx * dx + dy * dy) / float(RAD * RAD), 0.0) ** 2


def edge(d, size):
    return {-1: range(RAD), 0: range(size), 1: range(size - RAD, size)}[d]


def strip(i):
    dx, dy = OFFS[i]
    return [(x, y) for x in edge(dx, AX) for y in edge(dy, AY)]


def strips():
    spans, at = {}, 0
    for i in OTHERS:
        rows = -(-len(strip(i)) // 8) * 8
        spans[i] = (at, rows)
        at += rows
    return spans


SPANS = strips()


@functools.lru_cache
def tables():
    cells = AX * AY
    where = {(c // AY, c % AY): c for c in range(cells)}
    out = np.zeros((cells, cells), np.float32)
    for i in OTHERS:
        dx, dy = OFFS[i]
        for n, (x, y) in enumerate(strip(i)):
            out[SPANS[i][0] + n, x * AY + y] = 1.0
        for n, (x, y) in enumerate(strip(8 - i)):
            where[(x + dx * AX, y + dy * AY)] = cells + SPANS[i][0] + n
    code = np.zeros((2 * cells, 2 * cells), np.float32)
    code[:2, :] = -1.0
    move = np.zeros((2 * cells, 2, 8, cells), np.float32)
    slot = np.zeros((2 * cells, SLOTS, cells), np.float32)
    for (x, y), n in where.items():
        code[0, n], code[1, n] = x + AX, y + AY
        taken = 0
        for d, i in enumerate(OTHERS):
            dx, dy = OFFS[i]
            src = where.get((x + dx, y + dy))
            if src is not None:
                move[src, n // cells, d, n % cells] = 1.0
                if n < cells <= src:
                    slot[src, taken, n] = 1.0
                    code[2 + taken, n] = taper_of(dx, dy)
                    taken += 1
    own = move[:, 0].reshape(2 * cells, 8 * cells)
    far = move[:, 1].reshape(2 * cells, 8 * cells)
    slot = slot.reshape(2 * cells, SLOTS * cells)
    out = np.concatenate([out, np.zeros_like(out)], axis=0)
    return np.concatenate([own, far, slot, out, code], axis=1)


def split_rows(block):
    high = block.astype(jnp.bfloat16).astype(jnp.float32)
    return jnp.concatenate([high, block - high], axis=0).astype(jnp.bfloat16)


def moments(block, members):
    mean = jnp.sum(block, axis=0, keepdims=True) / members
    return mean, block - mean


def strengths(block, mean, table, members):
    variance = jnp.sum(block * block, axis=0, keepdims=True) / (members - 1)
    live, error, value, base = table
    denom = variance + base
    weighting = live / denom
    damping = 1.0 / (1.0 + jnp.sqrt(error / denom))
    alpha = jnp.sum(weighting * damping, axis=0, keepdims=True)
    beta = jnp.sum(weighting * value, axis=0, keepdims=True)
    return alpha, beta - mean * jnp.sum(weighting, axis=0, keepdims=True)


def shift(block, alpha, beta, tables):
    rest = jnp.zeros((6, block.shape[1]), jnp.float32)
    rows = block.shape[0] + 8
    left = split_rows(jnp.concatenate([block, alpha, beta, rest], axis=0))
    moved = jnp.dot(left, tables, preferred_element_type=jnp.float32)
    return moved[:rows] + moved[rows:]


def gather(block, sources, left):
    mean = jnp.zeros((1, block.shape[1]), jnp.float32)
    for source, a, m in sources:
        cov = jnp.sum(block * source, axis=0, keepdims=True)
        mean = mean + cov * m
        left = left - source * (cov * a)
    return left, mean


def sources_of(shifted, members, weights):
    cells = weights[0][1]
    found = []
    for d, (weight, width) in enumerate(weights):
        part = slice(d * cells, d * cells + width)
        found.append(
            (
                shifted[:members, part],
                shifted[members : members + 1, part] * weight,
                shifted[members + 1 : members + 2, part] * weight,
            )
        )
    return found


def around(scale, cells):
    return [(scale * taper_of(*OFFS[i]), cells) for i in OTHERS]


def exchange_kernel(
    src_ref, order_ref, cell_ref, live_ref, value_ref, error_ref, ocean_ref, weights_ref, atm_ref,
    table_in,
    own_ref, halo_ref, obs_ref, held, part_ref, fmean, beyond_ref, table_ref,
    ocn, late, wts, meta, src, ints, floats, strip_ref, shifted,
    local_sem, send_sem, recv_sem, note_sem,
):
    gx, gy = lax.axis_index("gx"), lax.axis_index("gy")
    nx, ny = lax.axis_size("gx"), lax.axis_size("gy")
    members = own_ref.shape[0]
    fields = atm_ref.shape[0]
    slots = ints.shape[2]

    def has_x(dx):
        return (gx + dx >= 0) & (gx + dx < nx)

    def has_y(dy):
        return (gy + dy >= 0) & (gy + dy < ny)

    def there(i):
        return has_x(OFFS[i][0]) & has_y(OFFS[i][1])

    barrier = pltpu.get_barrier_semaphore()
    for i in NEAR:
        dx, dy = OFFS[i]

        @pl.when(there(i))
        def _():
            pl.semaphore_signal(barrier, inc=1, device_id=(gx + dx, gy + dy), device_id_type=MESH)

    depth = wts.shape[0] - 1
    pairs = (
        (ocean_ref, ocn.at[4], 0), (order_ref, ints.at[0], 1), (cell_ref, ints.at[1], 1),
        (live_ref, ints.at[2], 1), (value_ref, floats.at[0], 2), (error_ref, floats.at[1], 2),
        (src_ref, src, 3), (weights_ref, wts.at[0:depth], 4), (atm_ref, held, 5),
        (table_in, table_ref, 6),
    )
    staged = [pltpu.make_async_copy(x, y, local_sem.at[n]) for x, y, n in pairs]
    outer = lax.rem(gy, 2) * 2 - 1
    for copy in staged:
        copy.start()

    for i in OTHERS:

        @pl.when(jnp.logical_not(there(i)))
        def _():
            at, rows = SPANS[i]
            halo_ref[at : at + rows, :] = jnp.zeros((rows, halo_ref.shape[1]), jnp.float32)
            meta[i] = jnp.zeros(meta.shape[1:], jnp.float32)

    for dx in (-1, 1):
        ocn[4 + 3 * dx + outer] = jnp.zeros(ocn.shape[1:], ocn.dtype)

        @pl.when(jnp.logical_not(has_x(dx) & has_y(outer)))
        def _():
            late[int(dx > 0)] = jnp.zeros(late.shape[1:], late.dtype)

    wts[depth] = jnp.zeros(wts.shape[1:], wts.dtype)
    for n in range(9, meta.shape[0]):
        meta[n] = jnp.zeros(meta.shape[1:], jnp.float32)

    staged[0].wait()
    pl.semaphore_wait(barrier, sum(there(i).astype(jnp.int32) for i in NEAR))

    count = members // PIECE

    def among(y, wanted):
        at = lax.rem(y + 8, 8)
        return sum((at == n).astype(jnp.int32) for n, share in enumerate(SHARES) if wanted(share)) > 0

    def relayed(y, p):
        return among(y, lambda share: p < share)

    def ocean(low, rows, source, target, kind, index, dx, dy):
        return pltpu.make_async_remote_copy(
            src_ref=ocn.at[source, pl.ds(low, rows)],
            dst_ref=target.at[pl.ds(low, rows)],
            send_sem=send_sem.at[0],
            recv_sem=recv_sem.at[index],
            device_id=(gx + dx, gy + dy),
            device_id_type=MESH,
        )

    def piece(p, source, target, kind, index, dx, dy):
        return ocean(p * PIECE, PIECE, source, target, kind, index, dx, dy)

    def arrive(at, index, dx, dy, p):
        ocean(p * PIECE, PIECE, at, ocn.at[at], 0, index, dx, dy).wait_recv()

    def sent(rows, kind, dx, dy):
        ocean(0, rows, 4, ocn.at[4], kind, 0, dx, dy).wait_send()

    def whole(blocks, index, dx, dy):
        pltpu.make_async_remote_copy(
            src_ref=ocn.at[pl.ds(0, blocks)],
            dst_ref=ocn.at[pl.ds(0, blocks)],
            send_sem=send_sem.at[0],
            recv_sem=recv_sem.at[index],
            device_id=(gx + dx, gy + dy),
            device_id_type=MESH,
        ).wait_recv()

    order = range(count)

    def start(cond, copies):
        @pl.when(cond)
        def _():
            for copy in copies:
                copy.start()

    def from_side(dx):
        return count * (dx > 0)

    beside, inside = 2 * count, 3 * count

    mine = lax.rem(gy, 8)
    yields = (mine == 2) | (mine == 5)
    to_outer = [piece(p, 4, ocn.at[4 - outer], 0, beside + p, 0, outer) for p in order]
    start(has_y(outer) & jnp.logical_not(yields), to_outer)
    for dx in (-1, 1):
        start(
            has_x(dx),
            [
                piece(p, 4, ocn.at[4 - 3 * dx], 2 + (dx > 0), from_side(-dx) + p, dx, 0)
                for p in reversed(order)
            ],
        )
    start(has_y(-outer), [ocean(0, members, 4, ocn.at[4 + outer], 1, inside, 0, -outer)])

    def relay(p, dx):
        return piece(p, 4 + outer, late.at[int(dx < 0)], 4 + (dx > 0), inside + 1 + (dx < 0), dx, 0)

    def forward(p, dx):
        return piece(p, 4 + 3 * dx, late.at[int(dx > 0)], 6 + (dx > 0), inside + 1 + (dx > 0), 0, outer)

    def hand(p, dx):
        return piece(p, 4 + 3 * dx, ocn.at[4 + 3 * dx + outer], 8 + (dx > 0), inside, 0, -outer)

    def all_sent():
        @pl.when(has_y(outer))
        def _():
            sent(members, 0, 0, outer)

        @pl.when(has_y(-outer))
        def _():
            sent(members, 1, 0, -outer)

        for dx in (-1, 1):

            @pl.when(has_x(dx))
            def _():
                sent(members, 2 + (dx > 0), dx, 0)

            @pl.when(has_x(dx) & has_y(-outer))
            def _():
                sent(members, 8 + (dx > 0), 0, -outer)

            for n in sorted(set(SHARES)):

                @pl.when(has_x(dx) & has_y(outer) & among(gy + outer, lambda share: share == n))
                def _():
                    if n:
                        sent(n * PIECE, 4 + (dx > 0), dx, 0)

                @pl.when(has_x(dx) & has_y(outer) & among(gy, lambda share: share == n))
                def _():
                    if n < count:
                        sent((count - n) * PIECE, 6 + (dx > 0), 0, outer)

    beside_x = has_x(-1).astype(jnp.int32) + has_x(1).astype(jnp.int32)
    beside_y = has_y(-1).astype(jnp.int32) + has_y(1).astype(jnp.int32)

    def remote(i):
        dx, dy = OFFS[i]
        return pltpu.make_async_remote_copy(
            src_ref=meta.at[4],
            dst_ref=meta.at[8 - i],
            send_sem=send_sem.at[0],
            recv_sem=note_sem.at[0],
            device_id=(gx + dx, gy + dy),
            device_id_type=MESH,
        )

    def border(i):
        dx, dy = OFFS[i]
        (source, rows), (target, _) = SPANS[i], SPANS[8 - i]
        return pltpu.make_async_remote_copy(
            src_ref=strip_ref.at[pl.ds(source, rows)],
            dst_ref=halo_ref.at[pl.ds(target, rows)],
            send_sem=send_sem.at[0],
            recv_sem=note_sem.at[1],
            device_id=(gx + dx, gy + dy),
            device_id_type=MESH,
        )

    def all_of(act):
        for nx_ in range(3):
            for ny_ in range(3):
                if nx_ + ny_:

                    @pl.when((beside_x == nx_) & (beside_y == ny_))
                    def _():
                        act(nx_, ny_)

    def whole_notes(nx_, ny_):
        n = (nx_ + 1) * (ny_ + 1) - 1
        return pltpu.make_async_remote_copy(
            src_ref=meta.at[pl.ds(0, n)], dst_ref=meta.at[pl.ds(0, n)],
            send_sem=send_sem.at[0], recv_sem=note_sem.at[0],
            device_id=(gx, gy + outer), device_id_type=MESH,
        )

    def whole_border(nx_, ny_):
        rows = nx_ * SPANS[1][1] + ny_ * SPANS[3][1] + nx_ * ny_ * SPANS[0][1]
        return pltpu.make_async_remote_copy(
            src_ref=strip_ref.at[pl.ds(0, rows)], dst_ref=halo_ref.at[pl.ds(0, rows)],
            send_sem=send_sem.at[0], recv_sem=note_sem.at[1],
            device_id=(gx, gy + outer), device_id_type=MESH,
        )

    def each(which, act):
        for i in which:

            @pl.when(there(i))
            def _():
                act(i)

    pltpu.make_async_copy(ints, ints, local_sem.at[1]).wait()
    pltpu.make_async_copy(floats, floats, local_sem.at[2]).wait()
    cell = ints[1]
    spot = ((cell // AY) * CODE + cell % AY).astype(jnp.float32)
    rows = jnp.concatenate(
        [
            spot, floats[0], floats[1], ints[2].astype(jnp.float32),
            jnp.zeros((4, slots), jnp.float32),
        ],
        axis=0,
    )
    slot = lax.broadcasted_iota(jnp.int32, (slots, slots), 0)
    perm = jnp.where(ints[0] == slot, 1.0, 0.0)
    rows = jnp.dot(rows, perm, precision=lax.Precision.HIGHEST, preferred_element_type=jnp.float32)
    meta[4] = jnp.concatenate([rows, jnp.zeros((8, meta.shape[2] - slots), jnp.float32)], axis=1)

    each(NEAR, lambda i: remote(i).start())

    staged[8].wait()
    for v in range(fields):
        block = held[v]
        mean = jnp.sum(block, axis=0, keepdims=True) / members
        fmean[v : v + 1, :] = mean
        held[v] = block - mean

    start(has_y(outer) & yields, to_outer)

    def from_x(p):
        for dx in (-1, 1):

            @pl.when(has_x(dx))
            def _():
                arrive(4 + 3 * dx, from_side(dx) + p, dx, 0, p)

                @pl.when(has_y(outer) & jnp.logical_not(relayed(gy, p)))
                def _():
                    forward(p, dx).start()

                @pl.when(has_y(-outer))
                def _():
                    hand(p, dx).start()

    def from_y(p):
        @pl.when(has_y(outer))
        def _():
            arrive(4 + outer, beside + p, 0, outer, p)

            @pl.when(relayed(gy + outer, p))
            def _():
                for dx in (-1, 1):

                    @pl.when(has_x(dx))
                    def _():
                        relay(p, dx).start()

    for parity, steps in enumerate((EVEN, ODD)):

        @pl.when(lax.rem(gy, 2) == parity)
        def _():
            first = [over_x for over_x, _ in steps].index(True)
            for n, (over_x, p) in enumerate(steps):
                (from_x if over_x else from_y)(p)
                if n == first:
                    each(FAR, lambda i: remote(i).start())

    staged[6].wait()
    staged[7].wait()
    staged[9].wait()
    for n in range(3):

        @pl.when((beside_x == n) & has_y(-outer))
        def _():
            whole(n + 1, inside, 0, -outer)

    total = jnp.zeros(own_ref.shape, jnp.float32)
    places = []
    for k in range(depth):
        source = src[0, k]
        position = (source // ny - gx + 1) * 3 + (source % ny - gy + 1)
        places.append(jnp.clip(position, 0, 8))
        total += jnp.dot(ocn[places[k]], wts[k], preferred_element_type=jnp.float32)
    for dx in (-1, 1):
        match = depth
        for k in range(depth):
            match = jnp.where(places[k] == 4 + 3 * dx + outer, k, match)

        @pl.when(has_x(dx) & has_y(outer))
        def _():
            whole(1, inside + 1 + (dx > 0), 0, outer)

        total += jnp.dot(late[int(dx > 0)], wts[match], preferred_element_type=jnp.float32)
    own_ref[...] = total
    width = strip_ref.shape[0]
    near, far = slice(0, 8 * width), slice(8 * width, 16 * width)
    rest = jnp.zeros((width - members, total.shape[1]), jnp.float32)
    picked = lax.dot_general(
        table_ref[:width, (16 + SLOTS) * width : (17 + SLOTS) * width], split_rows(jnp.concatenate([total, rest], axis=0)), (((1,), (1,)), ((), ())),
        preferred_element_type=jnp.float32,
    )
    strip_ref[...] = picked[:, :width] + picked[:, width:]
    each(FAR + NEAR, lambda i: border(i).start())

    all_of(lambda *n: whole_notes(*n).wait_recv())
    flat = meta[...].reshape(meta.shape[0] * meta.shape[1], meta.shape[2]).T
    cells = total.shape[1]
    places = table_ref[:16, (17 + SLOTS) * cells :].astype(jnp.float32)
    places = places[0:1] * CODE + places[1:2]
    for b in range(NB):
        for half, tiles in ((0, [4]), (1, OTHERS)):
            code = places[:, half * cells : (half + 1) * cells]
            live = jnp.zeros((OB, cells), jnp.float32)
            error = live + 1.0
            value = live
            base = live + 1.0
            for i in tiles:
                dx, dy = OFFS[i]
                column = flat[b * OB : (b + 1) * OB, 8 * i : 8 * i + 4]
                hit = column[:, 0:1] + float((AX * dx + AX) * CODE + AY * dy + AY) == code
                live = jnp.where(hit, column[:, 3:4], live)
                error = jnp.where(hit, column[:, 2:3], error)
                value = jnp.where(hit, column[:, 1:2], value)
                base = jnp.where(hit, column[:, 2:3] + (1.0 - column[:, 3:4]), base)
            for n, table in enumerate((live, error, value, base)):
                obs_ref[b, n, :, half * cells : (half + 1) * cells] = table

    scale = 1.0 / (members - 1)
    gmean, own = moments(own_ref[...], members)
    own_ref[...] = own
    alpha, beta = strengths(own, gmean, [obs_ref[0, n, :, :cells] for n in range(4)], members)
    shifted[...] = shift(own, alpha, beta, table_ref[:cells, near])
    center = (alpha * scale, beta * scale)

    def one_field(v, carry):
        block = held[v]
        found = sources_of(shifted, members, around(scale, cells))
        part_ref[v], mean = gather(block, [*found, (own_ref[...], *center)], block)
        fmean[pl.ds(v, 1), :] = fmean[pl.ds(v, 1), :] + mean
        return carry

    lax.fori_loop(0, fields, one_field, 0)
    found = sources_of(shifted, members, around(scale, cells))
    part_ref[fields], mean = gather(own, [*found, (own, *center)], own)
    fmean[fields : fields + 1, :] = gmean + mean
    beyond_ref[...] = shift(own, alpha, beta, table_ref[:cells, far])

    all_sent()
    all_of(lambda *n: whole_notes(*n).wait_send())
    all_of(lambda *n: whole_border(*n).wait_send())
    all_of(lambda *n: whole_border(*n).wait_recv())


def analysis_kernel(
    own_ref, halo_ref, obs_ref, held_in, part_ref, fmean_ref, beyond_ref, table_ref,
    mean_out, anom_ref,
    held, mean_ref, inner, shifted, out_sem,
):
    fields, members, cells = held_in.shape
    scale = 1.0 / (members - 1)
    own = own_ref[...]
    hmean, halo = moments(halo_ref[...].T[:members], members)
    alpha, beta = strengths(halo, hmean, [obs_ref[0, n, :, cells:] for n in range(4)], members)
    inner[...] = shift(halo, alpha, beta, table_ref[cells:, 16 * cells : (16 + SLOTS) * cells])
    taps = table_ref[:16, (17 + SLOTS) * cells : (18 + SLOTS) * cells].astype(jnp.float32) * scale
    taps = [(taps[2 + n : 3 + n], cells) for n in range(SLOTS)]
    block, mean = gather(own, sources_of(inner, members, taps), part_ref[fields])
    gmean = fmean_ref[fields : fields + 1, :] + mean
    beyond = beyond_ref[...] + shift(halo, alpha, beta, table_ref[cells:, 8 * cells : 16 * cells])
    edges = sources_of(beyond, members, around(scale, cells))
    halo, mean = gather(halo, [*edges, (halo, alpha * scale, beta * scale)], halo)
    grid = jnp.concatenate([block, halo], axis=1)
    gmean = jnp.concatenate([gmean, hmean + mean], axis=1)

    alpha, beta = strengths(grid, gmean, [obs_ref[1, n] for n in range(4)], members)
    shifted[...] = shift(grid, alpha, beta, table_ref[:, : 8 * cells])
    held[fields] = block
    center = (alpha[:, :cells] * scale, beta[:, :cells] * scale)

    def save(v):
        return pltpu.make_async_copy(held.at[v], anom_ref.at[v], out_sem.at[0])

    def one_field(v, carry):
        block, before = gather(held_in[v], sources_of(inner, members, taps), part_ref[v])
        near = sources_of(shifted, members, around(scale, cells))
        held[v], mean = gather(block, [*near, (held[fields], *center)], block)
        mean_ref[v] = fmean_ref[pl.ds(v, 1), :] + before + mean
        save(v).start()
        return carry

    lax.fori_loop(0, fields, one_field, 0)
    near = sources_of(shifted, members, around(scale, cells))
    rest, mean = gather(block, [*near, (block, *center)], block)
    mean_ref[fields] = gmean[:, :cells] + mean
    means = pltpu.make_async_copy(mean_ref, mean_out, out_sem.at[1])
    means.start()
    held[fields] = rest
    save(fields).start()
    means.wait()
    pltpu.make_async_copy(held, anom_ref, out_sem.at[0]).wait()


def local(
    atm_members, ocean_members, remap_weights, pair_src, obs_cell, obs_value, obs_error,
    obs_live, obs_order,
):
    members, fields, cells = atm_members.shape[2:]
    slots = obs_cell.shape[2]
    sources, depth = remap_weights.shape[2:4]
    vmem = pl.BlockSpec(memory_space=pltpu.VMEM)
    anywhere = pl.BlockSpec(memory_space=pl.ANY)
    table = tables()
    results = (
        pltpu.VMEM((members, cells), jnp.float32),
        pltpu.VMEM((cells, 128), jnp.float32),
        pltpu.VMEM((NB, 4, OB, 2 * cells), jnp.float32),
        pltpu.VMEM((fields, members, cells), jnp.float32),
        pltpu.VMEM((fields + 1, members, cells), jnp.float32),
        pltpu.VMEM((16, cells), jnp.float32),
        pltpu.VMEM((members + 8, 8 * cells), jnp.float32),
        pltpu.VMEM(table.shape, jnp.bfloat16),
    )
    state = pl.pallas_call(
        exchange_kernel,
        out_shape=results,
        in_specs=[anywhere] * 10,
        out_specs=(vmem,) * len(results),
        scratch_shapes=[
            pltpu.VMEM((9, members, depth), jnp.bfloat16),
            pltpu.VMEM((2, members, depth), jnp.bfloat16),
            pltpu.VMEM((sources + 1, depth, cells), jnp.bfloat16),
            pltpu.VMEM((16, 8, 128), jnp.float32),
            pltpu.SMEM((1, sources), jnp.int32),
            pltpu.VMEM((3, 1, slots), jnp.int32),
            pltpu.VMEM((2, 1, slots), jnp.float32),
            pltpu.VMEM((cells, 128), jnp.float32),
            pltpu.VMEM((members + 8, 8 * cells), jnp.float32),
            pltpu.SemaphoreType.DMA((7,)),
            pltpu.SemaphoreType.DMA((1,)),
            pltpu.SemaphoreType.DMA((3 * (members // PIECE) + 3,)),
            pltpu.SemaphoreType.DMA((2,)),
        ],
        compiler_params=pltpu.CompilerParams(
            collective_id=0, has_side_effects=True, vmem_limit_bytes=LIMIT
        ),
        name="exchange",
    )(
        *(
            pltpu.with_memory_space_constraint(x, pltpu.HBM)
            for x in (
                pair_src[0], obs_order[0], obs_cell[0], obs_live[0], obs_value[0], obs_error[0],
                ocean_members[0, 0], remap_weights[0, 0],
                jnp.transpose(atm_members[0, 0], (1, 0, 2)),
                jnp.asarray(table, jnp.bfloat16),
            )
        )
    )
    post_mean, post_anom = pl.pallas_call(
        analysis_kernel,
        out_shape=(
            jax.ShapeDtypeStruct((fields + 1, 1, cells), jnp.float32),
            jax.ShapeDtypeStruct((fields + 1, members, cells), jnp.float32),
        ),
        in_specs=[vmem] * len(results),
        out_specs=(anywhere, anywhere),
        scratch_shapes=[
            pltpu.VMEM((fields + 1, members, cells), jnp.float32),
            pltpu.VMEM((fields + 1, 1, cells), jnp.float32),
            pltpu.VMEM((members + 8, SLOTS * cells), jnp.float32),
            pltpu.VMEM((members + 8, 8 * cells), jnp.float32),
            pltpu.SemaphoreType.DMA((2,)),
        ],
        compiler_params=pltpu.CompilerParams(vmem_limit_bytes=LIMIT),
        name="analysis",
    )(*state)
    return (post_mean.reshape(1, 1, fields + 1, cells), jnp.transpose(post_anom, (1, 0, 2))[None, None])


def solution(mesh):
    in_specs = (
        P("gx", "gy", None, None, None),
        P("gx", "gy", None, None),
        P("gx", "gy", None, None, None),
        P("gx", "gy", None),
        P("gx", "gy", None),
        P("gx", "gy", None),
        P("gx", "gy", None),
        P("gx", "gy", None),
        P("gx", "gy", None),
    )
    out_specs = (P("gx", "gy", None, None), P("gx", "gy", None, None, None))
    return jax.shard_map(local, mesh=mesh, in_specs=in_specs, out_specs=out_specs, check_vma=False)
```

```python
import functools

import jax
import jax.numpy as jnp
import numpy as np
from jax import lax
from jax.experimental import pallas as pl
from jax.experimental.pallas import tpu as pltpu
from jax.sharding import PartitionSpec as P

AX = 8
AY = 16
OB = 32
NB = 2
RAD = 2
CODE = 64
LIMIT = 32 * 1024 * 1024

MESH = pl.DeviceIdType.MESH
OFFS = [(dx, dy) for dx in (-1, 0, 1) for dy in (-1, 0, 1)]
OTHERS = [i for i in range(9) if i != 4]
NEAR = [1, 3, 5, 7]
FAR = [0, 2, 6, 8]
PIECE = 16
SHARES = (3, 1, 3, 4, 4, 3, 1, 3)
EVEN = [(False, 0), (False, 1), (True, 4), (False, 2), (True, 3), (True, 2), (False, 3), (True, 1), (True, 0), (False, 4)]
ODD = [(True, 4), (True, 3), (False, 0), (True, 2), (False, 1), (True, 1), (False, 2), (True, 0), (False, 3), (False, 4)]
SLOTS = 5


def taper_of(dx, dy):
    return max(1.0 - (dx * dx + dy * dy) / float(RAD * RAD), 0.0) ** 2


def edge(d, size):
    return {-1: range(RAD), 0: range(size), 1: range(size - RAD, size)}[d]


def strip(i):
    dx, dy = OFFS[i]
    return [(x, y) for x in edge(dx, AX) for y in edge(dy, AY)]


def strips():
    spans, at = {}, 0
    for i in OTHERS:
        rows = -(-len(strip(i)) // 8) * 8
        spans[i] = (at, rows)
        at += rows
    return spans


SPANS = strips()


@functools.lru_cache
def tables():
    cells = AX * AY
    where = {(c // AY, c % AY): c for c in range(cells)}
    out = np.zeros((cells, cells), np.float32)
    for i in OTHERS:
        dx, dy = OFFS[i]
        for n, (x, y) in enumerate(strip(i)):
            out[SPANS[i][0] + n, x * AY + y] = 1.0
        for n, (x, y) in enumerate(strip(8 - i)):
            where[(x + dx * AX, y + dy * AY)] = cells + SPANS[i][0] + n
    code = np.zeros((2 * cells, 2 * cells), np.float32)
    code[:2, :] = -1.0
    move = np.zeros((2 * cells, 2, 8, cells), np.float32)
    slot = np.zeros((2 * cells, SLOTS, cells), np.float32)
    for (x, y), n in where.items():
        code[0, n], code[1, n] = x + AX, y + AY
        taken = 0
        for d, i in enumerate(OTHERS):
            dx, dy = OFFS[i]
            src = where.get((x + dx, y + dy))
            if src is not None:
                move[src, n // cells, d, n % cells] = 1.0
                if n < cells <= src:
                    slot[src, taken, n] = 1.0
                    code[2 + taken, n] = taper_of(dx, dy)
                    taken += 1
    own = move[:, 0].reshape(2 * cells, 8 * cells)
    far = move[:, 1].reshape(2 * cells, 8 * cells)
    slot = slot.reshape(2 * cells, SLOTS * cells)
    out = np.concatenate([out, np.zeros_like(out)], axis=0)
    return np.concatenate([own, far, slot, out, code], axis=1)


def split_rows(block):
    high = block.astype(jnp.bfloat16).astype(jnp.float32)
    return jnp.concatenate([high, block - high], axis=0).astype(jnp.bfloat16)


def moments(block, members):
    mean = jnp.sum(block, axis=0, keepdims=True) / members
    return mean, block - mean


def strengths(block, mean, table, members):
    variance = jnp.sum(block * block, axis=0, keepdims=True) / (members - 1)
    live, error, value, base = table
    denom = variance + base
    weighting = live / denom
    damping = 1.0 / (1.0 + jnp.sqrt(error / denom))
    alpha = jnp.sum(weighting * damping, axis=0, keepdims=True)
    beta = jnp.sum(weighting * value, axis=0, keepdims=True)
    return alpha, beta - mean * jnp.sum(weighting, axis=0, keepdims=True)


def shift(block, alpha, beta, tables):
    rest = jnp.zeros((6, block.shape[1]), jnp.float32)
    rows = block.shape[0] + 8
    left = split_rows(jnp.concatenate([block, alpha, beta, rest], axis=0))
    moved = jnp.dot(left, tables, preferred_element_type=jnp.float32)
    return moved[:rows] + moved[rows:]


def gather(block, sources, left):
    mean = jnp.zeros((1, block.shape[1]), jnp.float32)
    for source, a, m in sources:
        cov = jnp.sum(block * source, axis=0, keepdims=True)
        mean = mean + cov * m
        left = left - source * (cov * a)
    return left, mean


def sources_of(shifted, members, weights):
    cells = weights[0][1]
    found = []
    for d, (weight, width) in enumerate(weights):
        part = slice(d * cells, d * cells + width)
        found.append(
            (
                shifted[:members, part],
                shifted[members : members + 1, part] * weight,
                shifted[members + 1 : members + 2, part] * weight,
            )
        )
    return found


def around(scale, cells):
    return [(scale * taper_of(*OFFS[i]), cells) for i in OTHERS]


def exchange_kernel(
    src_ref, order_ref, cell_ref, live_ref, value_ref, error_ref, ocean_ref, weights_ref, atm_ref,
    table_in,
    own_ref, halo_ref, obs_ref, held, part_ref, fmean, beyond_ref, table_ref,
    ocn, late, wts, meta, src, ints, floats, strip_ref, shifted,
    local_sem, send_sem, recv_sem, note_sem,
):
    gx, gy = lax.axis_index("gx"), lax.axis_index("gy")
    nx, ny = lax.axis_size("gx"), lax.axis_size("gy")
    members = own_ref.shape[0]
    fields = atm_ref.shape[0]
    slots = ints.shape[2]

    def has_x(dx):
        return (gx + dx >= 0) & (gx + dx < nx)

    def has_y(dy):
        return (gy + dy >= 0) & (gy + dy < ny)

    def there(i):
        return has_x(OFFS[i][0]) & has_y(OFFS[i][1])

    barrier = pltpu.get_barrier_semaphore()
    for i in NEAR:
        dx, dy = OFFS[i]

        @pl.when(there(i))
        def _():
            pl.semaphore_signal(barrier, inc=1, device_id=(gx + dx, gy + dy), device_id_type=MESH)

    depth = wts.shape[0] - 1
    pairs = (
        (ocean_ref, ocn.at[4], 0), (order_ref, ints.at[0], 1), (cell_ref, ints.at[1], 1),
        (live_ref, ints.at[2], 1), (value_ref, floats.at[0], 2), (error_ref, floats.at[1], 2),
        (src_ref, src, 3), (weights_ref, wts.at[0:depth], 4), (atm_ref, held, 5),
        (table_in, table_ref, 6),
    )
    staged = [pltpu.make_async_copy(x, y, local_sem.at[n]) for x, y, n in pairs]
    outer = lax.rem(gy, 2) * 2 - 1
    for copy in staged:
        copy.start()

    for i in OTHERS:

        @pl.when(jnp.logical_not(there(i)))
        def _():
            at, rows = SPANS[i]
            halo_ref[at : at + rows, :] = jnp.zeros((rows, halo_ref.shape[1]), jnp.float32)
            meta[i] = jnp.zeros(meta.shape[1:], jnp.float32)

    for dx in (-1, 1):
        ocn[4 + 3 * dx + outer] = jnp.zeros(ocn.shape[1:], ocn.dtype)

        @pl.when(jnp.logical_not(has_x(dx) & has_y(outer)))
        def _():
            late[int(dx > 0)] = jnp.zeros(late.shape[1:], late.dtype)

    wts[depth] = jnp.zeros(wts.shape[1:], wts.dtype)
    for n in range(9, meta.shape[0]):
        meta[n] = jnp.zeros(meta.shape[1:], jnp.float32)

    staged[0].wait()
    pl.semaphore_wait(barrier, sum(there(i).astype(jnp.int32) for i in NEAR))

    count = members // PIECE

    def among(y, wanted):
        at = lax.rem(y + 8, 8)
        return sum((at == n).astype(jnp.int32) for n, share in enumerate(SHARES) if wanted(share)) > 0

    def relayed(y, p):
        return among(y, lambda share: p < share)

    def ocean(low, rows, source, target, kind, index, dx, dy):
        return pltpu.make_async_remote_copy(
            src_ref=ocn.at[source, pl.ds(low, rows)],
            dst_ref=target.at[pl.ds(low, rows)],
            send_sem=send_sem.at[0],
            recv_sem=recv_sem.at[index],
            device_id=(gx + dx, gy + dy),
            device_id_type=MESH,
        )

    def piece(p, source, target, kind, index, dx, dy):
        return ocean(p * PIECE, PIECE, source, target, kind, index, dx, dy)

    def arrive(at, index, dx, dy, p):
        ocean(p * PIECE, PIECE, at, ocn.at[at], 0, index, dx, dy).wait_recv()

    def sent(rows, kind, dx, dy):
        ocean(0, rows, 4, ocn.at[4], kind, 0, dx, dy).wait_send()

    def whole(blocks, index, dx, dy):
        pltpu.make_async_remote_copy(
            src_ref=ocn.at[pl.ds(0, blocks)],
            dst_ref=ocn.at[pl.ds(0, blocks)],
            send_sem=send_sem.at[0],
            recv_sem=recv_sem.at[index],
            device_id=(gx + dx, gy + dy),
            device_id_type=MESH,
        ).wait_recv()

    order = range(count)

    def start(cond, copies):
        @pl.when(cond)
        def _():
            for copy in copies:
                copy.start()

    def from_side(dx):
        return count * (dx > 0)

    beside, inside = 2 * count, 3 * count

    mine = lax.rem(gy, 8)
    yields = mine == 2
    to_outer = [piece(p, 4, ocn.at[4 - outer], 0, beside + p, 0, outer) for p in order]
    start(has_y(outer) & jnp.logical_not(yields), to_outer)
    for dx in (-1, 1):
        start(
            has_x(dx),
            [
                piece(p, 4, ocn.at[4 - 3 * dx], 2 + (dx > 0), from_side(-dx) + p, dx, 0)
                for p in reversed(order)
            ],
        )
    start(has_y(-outer), [ocean(0, members, 4, ocn.at[4 + outer], 1, inside, 0, -outer)])

    def relay(p, dx):
        return piece(p, 4 + outer, late.at[int(dx < 0)], 4 + (dx > 0), inside + 1 + (dx < 0), dx, 0)

    def forward(p, dx):
        return piece(p, 4 + 3 * dx, late.at[int(dx > 0)], 6 + (dx > 0), inside + 1 + (dx > 0), 0, outer)

    def hand(p, dx):
        return piece(p, 4 + 3 * dx, ocn.at[4 + 3 * dx + outer], 8 + (dx > 0), inside, 0, -outer)

    def all_sent():
        @pl.when(has_y(outer))
        def _():
            sent(members, 0, 0, outer)

        @pl.when(has_y(-outer))
        def _():
            sent(members, 1, 0, -outer)

        for dx in (-1, 1):

            @pl.when(has_x(dx))
            def _():
                sent(members, 2 + (dx > 0), dx, 0)

            @pl.when(has_x(dx) & has_y(-outer))
            def _():
                sent(members, 8 + (dx > 0), 0, -outer)

            for n in sorted(set(SHARES)):

                @pl.when(has_x(dx) & has_y(outer) & among(gy + outer, lambda share: share == n))
                def _():
                    if n:
                        sent(n * PIECE, 4 + (dx > 0), dx, 0)

                @pl.when(has_x(dx) & has_y(outer) & among(gy, lambda share: share == n))
                def _():
                    if n < count:
                        sent((count - n) * PIECE, 6 + (dx > 0), 0, outer)

    beside_x = has_x(-1).astype(jnp.int32) + has_x(1).astype(jnp.int32)
    beside_y = has_y(-1).astype(jnp.int32) + has_y(1).astype(jnp.int32)

    def remote(i):
        dx, dy = OFFS[i]
        return pltpu.make_async_remote_copy(
            src_ref=meta.at[4],
            dst_ref=meta.at[8 - i],
            send_sem=send_sem.at[0],
            recv_sem=note_sem.at[0],
            device_id=(gx + dx, gy + dy),
            device_id_type=MESH,
        )

    def border(i):
        dx, dy = OFFS[i]
        (source, rows), (target, _) = SPANS[i], SPANS[8 - i]
        return pltpu.make_async_remote_copy(
            src_ref=strip_ref.at[pl.ds(source, rows)],
            dst_ref=halo_ref.at[pl.ds(target, rows)],
            send_sem=send_sem.at[0],
            recv_sem=note_sem.at[1],
            device_id=(gx + dx, gy + dy),
            device_id_type=MESH,
        )

    def all_of(act):
        for nx_ in range(3):
            for ny_ in range(3):
                if nx_ + ny_:

                    @pl.when((beside_x == nx_) & (beside_y == ny_))
                    def _():
                        act(nx_, ny_)

    def whole_notes(nx_, ny_):
        n = (nx_ + 1) * (ny_ + 1) - 1
        return pltpu.make_async_remote_copy(
            src_ref=meta.at[pl.ds(0, n)], dst_ref=meta.at[pl.ds(0, n)],
            send_sem=send_sem.at[0], recv_sem=note_sem.at[0],
            device_id=(gx, gy + outer), device_id_type=MESH,
        )

    def whole_border(nx_, ny_):
        rows = nx_ * SPANS[1][1] + ny_ * SPANS[3][1] + nx_ * ny_ * SPANS[0][1]
        return pltpu.make_async_remote_copy(
            src_ref=strip_ref.at[pl.ds(0, rows)], dst_ref=halo_ref.at[pl.ds(0, rows)],
            send_sem=send_sem.at[0], recv_sem=note_sem.at[1],
            device_id=(gx, gy + outer), device_id_type=MESH,
        )

    def each(which, act):
        for i in which:

            @pl.when(there(i))
            def _():
                act(i)

    pltpu.make_async_copy(ints, ints, local_sem.at[1]).wait()
    pltpu.make_async_copy(floats, floats, local_sem.at[2]).wait()
    cell = ints[1]
    spot = ((cell // AY) * CODE + cell % AY).astype(jnp.float32)
    rows = jnp.concatenate(
        [
            spot, floats[0], floats[1], ints[2].astype(jnp.float32),
            jnp.zeros((4, slots), jnp.float32),
        ],
        axis=0,
    )
    slot = lax.broadcasted_iota(jnp.int32, (slots, slots), 0)
    perm = jnp.where(ints[0] == slot, 1.0, 0.0)
    rows = jnp.dot(rows, perm, precision=lax.Precision.HIGHEST, preferred_element_type=jnp.float32)
    meta[4] = jnp.concatenate([rows, jnp.zeros((8, meta.shape[2] - slots), jnp.float32)], axis=1)

    each(NEAR, lambda i: remote(i).start())

    staged[8].wait()
    for v in range(fields):
        block = held[v]
        mean = jnp.sum(block, axis=0, keepdims=True) / members
        fmean[v : v + 1, :] = mean
        held[v] = block - mean

    start(has_y(outer) & yields, to_outer)

    def from_x(p):
        for dx in (-1, 1):

            @pl.when(has_x(dx))
            def _():
                arrive(4 + 3 * dx, from_side(dx) + p, dx, 0, p)

                @pl.when(has_y(outer) & jnp.logical_not(relayed(gy, p)))
                def _():
                    forward(p, dx).start()

                @pl.when(has_y(-outer))
                def _():
                    hand(p, dx).start()

    def from_y(p):
        @pl.when(has_y(outer))
        def _():
            arrive(4 + outer, beside + p, 0, outer, p)

            @pl.when(relayed(gy + outer, p))
            def _():
                for dx in (-1, 1):

                    @pl.when(has_x(dx))
                    def _():
                        relay(p, dx).start()

    for parity, steps in enumerate((EVEN, ODD)):

        @pl.when(lax.rem(gy, 2) == parity)
        def _():
            first = [over_x for over_x, _ in steps].index(True)
            for n, (over_x, p) in enumerate(steps):
                (from_x if over_x else from_y)(p)
                if n == first:
                    each(FAR, lambda i: remote(i).start())

    staged[6].wait()
    staged[7].wait()
    staged[9].wait()
    for n in range(3):

        @pl.when((beside_x == n) & has_y(-outer))
        def _():
            whole(n + 1, inside, 0, -outer)

    total = jnp.zeros(own_ref.shape, jnp.float32)
    places = []
    for k in range(depth):
        source = src[0, k]
        position = (source // ny - gx + 1) * 3 + (source % ny - gy + 1)
        places.append(jnp.clip(position, 0, 8))
        total += jnp.dot(ocn[places[k]], wts[k], preferred_element_type=jnp.float32)
    for dx in (-1, 1):
        match = depth
        for k in range(depth):
            match = jnp.where(places[k] == 4 + 3 * dx + outer, k, match)

        @pl.when(has_x(dx) & has_y(outer))
        def _():
            whole(1, inside + 1 + (dx > 0), 0, outer)

        total += jnp.dot(late[int(dx > 0)], wts[match], preferred_element_type=jnp.float32)
    own_ref[...] = total
    width = strip_ref.shape[0]
    near, far = slice(0, 8 * width), slice(8 * width, 16 * width)
    rest = jnp.zeros((width - members, total.shape[1]), jnp.float32)
    picked = lax.dot_general(
        table_ref[:width, (16 + SLOTS) * width : (17 + SLOTS) * width], split_rows(jnp.concatenate([total, rest], axis=0)), (((1,), (1,)), ((), ())),
        preferred_element_type=jnp.float32,
    )
    strip_ref[...] = picked[:, :width] + picked[:, width:]
    each(FAR + NEAR, lambda i: border(i).start())

    all_of(lambda *n: whole_notes(*n).wait_recv())
    flat = meta[...].reshape(meta.shape[0] * meta.shape[1], meta.shape[2]).T
    cells = total.shape[1]
    places = table_ref[:16, (17 + SLOTS) * cells :].astype(jnp.float32)
    places = places[0:1] * CODE + places[1:2]
    for b in range(NB):
        for half, tiles in ((0, [4]), (1, OTHERS)):
            code = places[:, half * cells : (half + 1) * cells]
            live = jnp.zeros((OB, cells), jnp.float32)
            error = live + 1.0
            value = live
            base = live + 1.0
            for i in tiles:
                dx, dy = OFFS[i]
                column = flat[b * OB : (b + 1) * OB, 8 * i : 8 * i + 4]
                hit = column[:, 0:1] + float((AX * dx + AX) * CODE + AY * dy + AY) == code
                live = jnp.where(hit, column[:, 3:4], live)
                error = jnp.where(hit, column[:, 2:3], error)
                value = jnp.where(hit, column[:, 1:2], value)
                base = jnp.where(hit, column[:, 2:3] + (1.0 - column[:, 3:4]), base)
            for n, table in enumerate((live, error, value, base)):
                obs_ref[b, n, :, half * cells : (half + 1) * cells] = table

    scale = 1.0 / (members - 1)
    gmean, own = moments(own_ref[...], members)
    own_ref[...] = own
    alpha, beta = strengths(own, gmean, [obs_ref[0, n, :, :cells] for n in range(4)], members)
    shifted[...] = shift(own, alpha, beta, table_ref[:cells, near])
    center = (alpha * scale, beta * scale)

    def one_field(v, carry):
        block = held[v]
        found = sources_of(shifted, members, around(scale, cells))
        part_ref[v], mean = gather(block, [*found, (own_ref[...], *center)], block)
        fmean[pl.ds(v, 1), :] = fmean[pl.ds(v, 1), :] + mean
        return carry

    lax.fori_loop(0, fields, one_field, 0)
    found = sources_of(shifted, members, around(scale, cells))
    part_ref[fields], mean = gather(own, [*found, (own, *center)], own)
    fmean[fields : fields + 1, :] = gmean + mean
    beyond_ref[...] = shift(own, alpha, beta, table_ref[:cells, far])

    all_sent()
    all_of(lambda *n: whole_notes(*n).wait_send())
    all_of(lambda *n: whole_border(*n).wait_send())
    all_of(lambda *n: whole_border(*n).wait_recv())


def analysis_kernel(
    own_ref, halo_ref, obs_ref, held_in, part_ref, fmean_ref, beyond_ref, table_ref,
    mean_out, anom_ref,
    held, mean_ref, inner, shifted, out_sem,
):
    fields, members, cells = held_in.shape
    scale = 1.0 / (members - 1)
    own = own_ref[...]
    hmean, halo = moments(halo_ref[...].T[:members], members)
    alpha, beta = strengths(halo, hmean, [obs_ref[0, n, :, cells:] for n in range(4)], members)
    inner[...] = shift(halo, alpha, beta, table_ref[cells:, 16 * cells : (16 + SLOTS) * cells])
    taps = table_ref[:16, (17 + SLOTS) * cells : (18 + SLOTS) * cells].astype(jnp.float32) * scale
    taps = [(taps[2 + n : 3 + n], cells) for n in range(SLOTS)]
    block, mean = gather(own, sources_of(inner, members, taps), part_ref[fields])
    gmean = fmean_ref[fields : fields + 1, :] + mean
    beyond = beyond_ref[...] + shift(halo, alpha, beta, table_ref[cells:, 8 * cells : 16 * cells])
    edges = sources_of(beyond, members, around(scale, cells))
    halo, mean = gather(halo, [*edges, (halo, alpha * scale, beta * scale)], halo)
    grid = jnp.concatenate([block, halo], axis=1)
    gmean = jnp.concatenate([gmean, hmean + mean], axis=1)

    alpha, beta = strengths(grid, gmean, [obs_ref[1, n] for n in range(4)], members)
    shifted[...] = shift(grid, alpha, beta, table_ref[:, : 8 * cells])
    held[fields] = block
    center = (alpha[:, :cells] * scale, beta[:, :cells] * scale)

    def save(v):
        return pltpu.make_async_copy(held.at[v], anom_ref.at[v], out_sem.at[0])

    def one_field(v, carry):
        block, before = gather(held_in[v], sources_of(inner, members, taps), part_ref[v])
        near = sources_of(shifted, members, around(scale, cells))
        held[v], mean = gather(block, [*near, (held[fields], *center)], block)
        mean_ref[v] = fmean_ref[pl.ds(v, 1), :] + before + mean
        save(v).start()
        return carry

    lax.fori_loop(0, fields, one_field, 0)
    near = sources_of(shifted, members, around(scale, cells))
    rest, mean = gather(block, [*near, (block, *center)], block)
    mean_ref[fields] = gmean[:, :cells] + mean
    means = pltpu.make_async_copy(mean_ref, mean_out, out_sem.at[1])
    means.start()
    held[fields] = rest
    save(fields).start()
    means.wait()
    pltpu.make_async_copy(held, anom_ref, out_sem.at[0]).wait()


def local(
    atm_members, ocean_members, remap_weights, pair_src, obs_cell, obs_value, obs_error,
    obs_live, obs_order,
):
    members, fields, cells = atm_members.shape[2:]
    slots = obs_cell.shape[2]
    sources, depth = remap_weights.shape[2:4]
    vmem = pl.BlockSpec(memory_space=pltpu.VMEM)
    anywhere = pl.BlockSpec(memory_space=pl.ANY)
    table = tables()
    results = (
        pltpu.VMEM((members, cells), jnp.float32),
        pltpu.VMEM((cells, 128), jnp.float32),
        pltpu.VMEM((NB, 4, OB, 2 * cells), jnp.float32),
        pltpu.VMEM((fields, members, cells), jnp.float32),
        pltpu.VMEM((fields + 1, members, cells), jnp.float32),
        pltpu.VMEM((16, cells), jnp.float32),
        pltpu.VMEM((members + 8, 8 * cells), jnp.float32),
        pltpu.VMEM(table.shape, jnp.bfloat16),
    )
    state = pl.pallas_call(
        exchange_kernel,
        out_shape=results,
        in_specs=[anywhere] * 10,
        out_specs=(vmem,) * len(results),
        scratch_shapes=[
            pltpu.VMEM((9, members, depth), jnp.bfloat16),
            pltpu.VMEM((2, members, depth), jnp.bfloat16),
            pltpu.VMEM((sources + 1, depth, cells), jnp.bfloat16),
            pltpu.VMEM((16, 8, 128), jnp.float32),
            pltpu.SMEM((1, sources), jnp.int32),
            pltpu.VMEM((3, 1, slots), jnp.int32),
            pltpu.VMEM((2, 1, slots), jnp.float32),
            pltpu.VMEM((cells, 128), jnp.float32),
            pltpu.VMEM((members + 8, 8 * cells), jnp.float32),
            pltpu.SemaphoreType.DMA((7,)),
            pltpu.SemaphoreType.DMA((1,)),
            pltpu.SemaphoreType.DMA((3 * (members // PIECE) + 3,)),
            pltpu.SemaphoreType.DMA((2,)),
        ],
        compiler_params=pltpu.CompilerParams(
            collective_id=0, has_side_effects=True, vmem_limit_bytes=LIMIT
        ),
        name="exchange",
    )(
        *(
            pltpu.with_memory_space_constraint(x, pltpu.HBM)
            for x in (
                pair_src[0], obs_order[0], obs_cell[0], obs_live[0], obs_value[0], obs_error[0],
                ocean_members[0, 0], remap_weights[0, 0],
                jnp.transpose(atm_members[0, 0], (1, 0, 2)),
                jnp.asarray(table, jnp.bfloat16),
            )
        )
    )
    post_mean, post_anom = pl.pallas_call(
        analysis_kernel,
        out_shape=(
            jax.ShapeDtypeStruct((fields + 1, 1, cells), jnp.float32),
            jax.ShapeDtypeStruct((fields + 1, members, cells), jnp.float32),
        ),
        in_specs=[vmem] * len(results),
        out_specs=(anywhere, anywhere),
        scratch_shapes=[
            pltpu.VMEM((fields + 1, members, cells), jnp.float32),
            pltpu.VMEM((fields + 1, 1, cells), jnp.float32),
            pltpu.VMEM((members + 8, SLOTS * cells), jnp.float32),
            pltpu.VMEM((members + 8, 8 * cells), jnp.float32),
            pltpu.SemaphoreType.DMA((2,)),
        ],
        compiler_params=pltpu.CompilerParams(vmem_limit_bytes=LIMIT),
        name="analysis",
    )(*state)
    return (post_mean.reshape(1, 1, fields + 1, cells), jnp.transpose(post_anom, (1, 0, 2))[None, None])


def solution(mesh):
    in_specs = (
        P("gx", "gy", None, None, None),
        P("gx", "gy", None, None),
        P("gx", "gy", None, None, None),
        P("gx", "gy", None),
        P("gx", "gy", None),
        P("gx", "gy", None),
        P("gx", "gy", None),
        P("gx", "gy", None),
        P("gx", "gy", None),
    )
    out_specs = (P("gx", "gy", None, None), P("gx", "gy", None, None, None))
    return jax.shard_map(local, mesh=mesh, in_specs=in_specs, out_specs=out_specs, check_vma=False)
```
